32 devices in a mesh: groups: 2 (over y), rows: 4 (over z), cols: 4 (over x, core).
Axes of the slice: x: 2, y: 2, z: 4, core: 2. Of those that a mesh axis runs over, the one named last changes fastest.
Arguments:
- alignment_features: float32 [128, 32, 64], P(('groups', 'rows'), 'cols'), parts along dimension 0, may hold values from -6 to 6
- affine_factor: float32 [64], replicated, may hold values from 0.25 to 1.75
- affine_offset: float32 [64], replicated, may hold values from -3 to 3
- first_projector: bfloat16 [64, 32], replicated, may hold values from -0.75 to 0.75
- second_projector: bfloat16 [64, 32], replicated, may hold values from -0.75 to 0.75
- final_projector: bfloat16 [1024, 128], replicated, may hold values from -0.75 to 0.75
- additive_term: float32 [128], replicated, may hold values from -3 to 3
- adjoint_update: bfloat16 [128, 64, 128], P(('groups', 'rows'), 'cols'), parts along dimension 0, may hold values from -6 to 6
Outputs:
- residue_update: bfloat16 [128, 64, 128], P(('groups', 'rows'), 'cols'), parts along dimension 0
- alignment_slope: float32 [128, 32, 64], P(('groups', 'rows'), 'cols'), parts along dimension 0
- final_projector_slope: float32 [2048, 128], P(('groups', 'rows', 'cols')), parts along dimension 0
- first_projector_slope: float32 [128, 32], P('groups'), parts along dimension 0
- second_projector_slope: float32 [128, 32], P('groups'), parts along dimension 0
The draws below stay inside these ranges and needn't reach their ends.
There are 2 independent parts, one for each index of `groups`. The reference program is written for one: setup_inputs(seed, part) draws one part's arguments, and reference() takes and returns one part's arrays. A program takes and returns all parts, laid end to end along the dimension named above; an argument that names none is the same for every part. Nothing has to cross between parts.
All inputs are finite; a program needn't handle non-finite values.
Results may differ from the reference program's by a relative error of at most 0.0061.
Values may be sent and summed in bfloat16 or wider, within the bound.
No kernel may reach another device: no remote copies, remote signals or barrier semaphores. Data moves between devices by JAX's collectives and lax.ppermute only.
A program may use at most 64 MiB of HBM per device.

```python
import jax
import jax.numpy as jnp
from jax import lax

ALIGNMENT_DEPTH = 64
PROJECTION_WIDTH = 32
FEATURE_DEPTH = 128
ALIGNMENT_ROWS = 32
RESIDUES_EACH = 16
WINDOW_RESIDUES = 64


def levels(rng, shape, pieces, smallest, high):
    factor_of, own = 1.0, jax.random.fold_in(rng, 6)
    for axis_at, parts in pieces:
        draws = jnp.exp(jax.random.uniform(jax.random.fold_in(own, axis_at), (parts,), jnp.float32, smallest / len(pieces), high / len(pieces)))
        factor_of = factor_of * jnp.repeat(draws, shape[axis_at] // parts).reshape([-1 if axis == axis_at else 1 for axis in range(len(shape))])
    return factor_of


def bell_draw(key, extent, scale, bound, pieces=(), held_as=jnp.bfloat16):
    entries = scale * jax.random.normal(key, extent, jnp.float32)
    if pieces:
        entries = entries * levels(key, extent, pieces, -0.22, 0.18)
    return jnp.clip(entries, -bound, bound).astype(held_as)


def setup_inputs(seed: int = 0, part: int = 0) -> dict:
    arg_keys = jax.random.split(jax.random.key(seed), 9)
    own_keys = jax.random.split(jax.random.fold_in(arg_keys[8], part), 9)
    alignment_features = bell_draw(own_keys[0], (WINDOW_RESIDUES, ALIGNMENT_ROWS, ALIGNMENT_DEPTH), 1.0, 6.0, ((0, 4), (1, 4)), jnp.float32)
    affine_factor = jnp.clip(1.0 + 0.15 * jax.random.normal(arg_keys[1], (ALIGNMENT_DEPTH,), jnp.float32), 0.25, 1.75)
    affine_offset = bell_draw(arg_keys[2], (ALIGNMENT_DEPTH,), 0.5, 3.0, (), jnp.float32)
    first_projector = bell_draw(arg_keys[3], (ALIGNMENT_DEPTH, PROJECTION_WIDTH), ALIGNMENT_DEPTH ** -0.5, 0.75)
    second_projector = bell_draw(arg_keys[4], (ALIGNMENT_DEPTH, PROJECTION_WIDTH), ALIGNMENT_DEPTH ** -0.5, 0.75)
    final_projector = bell_draw(arg_keys[5], (PROJECTION_WIDTH * PROJECTION_WIDTH, FEATURE_DEPTH), (PROJECTION_WIDTH * 2) ** -0.5, 0.75)
    additive_term = bell_draw(arg_keys[6], (FEATURE_DEPTH,), 0.5, 3.0, (), jnp.float32)
    adjoint_update = bell_draw(own_keys[7], (WINDOW_RESIDUES, WINDOW_RESIDUES, FEATURE_DEPTH), 1.0, 6.0, ((0, 4), (1, 4)))
    return dict(alignment_features=alignment_features, affine_factor=affine_factor, affine_offset=affine_offset, first_projector=first_projector, second_projector=second_projector, final_projector=final_projector, additive_term=additive_term, adjoint_update=adjoint_update)


def layernorm_parts(alignment_features, affine_factor, affine_offset):
    centered_alignment = alignment_features - lax.optimization_barrier(jnp.mean(alignment_features, axis=-1, keepdims=True))
    reciprocal_spread = lax.rsqrt(lax.optimization_barrier(jnp.mean(centered_alignment * centered_alignment, axis=-1, keepdims=True)) + 1e-05)
    zscored_alignment = centered_alignment * reciprocal_spread
    return (zscored_alignment, reciprocal_spread, (zscored_alignment * affine_factor + affine_offset).astype(jnp.bfloat16))

def reference(alignment_features, affine_factor, affine_offset, first_projector, second_projector, final_projector, additive_term, adjoint_update):
    zscored_alignment, reciprocal_spread, unit_alignment = layernorm_parts(alignment_features, affine_factor, affine_offset)
    first_factor = jnp.dot(unit_alignment, first_projector, preferred_element_type=jnp.float32).astype(jnp.bfloat16)
    second_factor = jnp.dot(unit_alignment, second_projector, preferred_element_type=jnp.float32).astype(jnp.bfloat16)
    multiplier = 1.0 / ALIGNMENT_ROWS
    right_wide = second_factor.astype(jnp.float32)
    tile_list = WINDOW_RESIDUES // RESIDUES_EACH
    first_tile_list = first_factor.reshape(tile_list, RESIDUES_EACH, ALIGNMENT_ROWS, PROJECTION_WIDTH)
    cot_blocks = adjoint_update.reshape(tile_list, RESIDUES_EACH, WINDOW_RESIDUES, FEATURE_DEPTH)

    def step(carry, inputs):
        right_acc, out_acc = carry
        left_part, cot_part = inputs
        outer = (jnp.einsum('isc,jsd->ijcd', left_part.astype(jnp.float32), right_wide) * multiplier).astype(jnp.bfloat16)
        flat = outer.reshape(RESIDUES_EACH * WINDOW_RESIDUES, PROJECTION_WIDTH * PROJECTION_WIDTH)
        cot_flat = cot_part.reshape(RESIDUES_EACH * WINDOW_RESIDUES, FEATURE_DEPTH)
        update = (jnp.dot(flat, final_projector, preferred_element_type=jnp.float32) + additive_term).astype(jnp.bfloat16)
        outer_grad = jnp.dot(cot_flat, final_projector.T, preferred_element_type=jnp.float32).astype(jnp.bfloat16)
        outer_grad = outer_grad.reshape(RESIDUES_EACH, WINDOW_RESIDUES, PROJECTION_WIDTH, PROJECTION_WIDTH).astype(jnp.float32)
        out_acc = out_acc + jnp.dot(flat.T, cot_flat, preferred_element_type=jnp.float32)
        first_adjoint = jnp.einsum('ijcd,jsd->isc', outer_grad, right_wide) * multiplier
        right_acc = right_acc + jnp.einsum('ijcd,isc->jsd', outer_grad, left_part.astype(jnp.float32)) * multiplier
        return ((right_acc, out_acc), (update.reshape(RESIDUES_EACH, WINDOW_RESIDUES, FEATURE_DEPTH), first_adjoint))
    beginning_position = (jnp.zeros((WINDOW_RESIDUES, ALIGNMENT_ROWS, PROJECTION_WIDTH), jnp.float32), jnp.zeros((PROJECTION_WIDTH * PROJECTION_WIDTH, FEATURE_DEPTH), jnp.float32))
    (right_back, final_projector_slope), (updates, first_adjoint_list) = lax.scan(step, beginning_position, (first_tile_list, cot_blocks))
    residue_update = updates.reshape(WINDOW_RESIDUES, WINDOW_RESIDUES, FEATURE_DEPTH)
    first_adjoint = first_adjoint_list.reshape(WINDOW_RESIDUES, ALIGNMENT_ROWS, PROJECTION_WIDTH)
    unit_broadcast = unit_alignment.astype(jnp.float32)
    high = lax.Precision.HIGHEST
    first_projector_slope = jnp.einsum('tsk,tsc->kc', unit_broadcast, first_adjoint, precision=high)
    second_projector_slope = jnp.einsum('tsk,tsc->kc', unit_broadcast, right_back, precision=high)
    unit_adjoint = jnp.einsum('tsc,kc->tsk', first_adjoint, first_projector.astype(jnp.float32), precision=high)
    unit_adjoint = unit_adjoint + jnp.einsum('tsc,kc->tsk', right_back, second_projector.astype(jnp.float32), precision=high)
    scaled_alignment = unit_adjoint * affine_factor
    alignment_slope = reciprocal_spread * (scaled_alignment - lax.optimization_barrier(jnp.mean(scaled_alignment, axis=-1, keepdims=True)) - zscored_alignment * lax.optimization_barrier(jnp.mean(scaled_alignment * zscored_alignment, axis=-1, keepdims=True)))
    return (residue_update, alignment_slope, final_projector_slope, first_projector_slope, second_projector_slope)
```

```python
import jax
import jax.numpy as jnp
from jax import lax
from jax.sharding import PartitionSpec as P


def layernorm_parts(alignment_features, affine_factor, affine_offset):
    centered_alignment = alignment_features - jnp.mean(alignment_features, axis=-1, keepdims=True)
    reciprocal_spread = lax.rsqrt(
        jnp.mean(centered_alignment * centered_alignment, axis=-1, keepdims=True) + 1e-05
    )
    zscored_alignment = centered_alignment * reciprocal_spread
    return (
        zscored_alignment,
        reciprocal_spread,
        (zscored_alignment * affine_factor + affine_offset).astype(jnp.bfloat16),
    )


def local_general(
    alignment_features,
    affine_factor,
    affine_offset,
    first_projector,
    second_projector,
    final_projector,
    additive_term,
    adjoint_update,
):
    zscored_alignment, reciprocal_spread, unit_alignment = layernorm_parts(
        alignment_features, affine_factor, affine_offset
    )
    first_factor_here = jnp.dot(
        unit_alignment, first_projector, preferred_element_type=jnp.float32
    ).astype(jnp.bfloat16)
    second_factor_here = jnp.dot(
        unit_alignment, second_projector, preferred_element_type=jnp.float32
    ).astype(jnp.bfloat16)
    tokens, quarter, chans = first_factor_here.shape
    left_flat = first_factor_here.reshape(tokens, quarter * chans)
    right_flat = second_factor_here.reshape(tokens, quarter * chans)
    left_wide, right_wide = (
        lax.all_gather(left_flat, "cols", axis=1, tiled=True),
        lax.all_gather(right_flat, "cols", axis=1, tiled=True),
    )
    left_rows = left_wide.reshape(tokens, -1, chans)
    right_all = lax.all_gather(right_wide, "rows", axis=0, tiled=True)
    block = right_all.shape[0] // lax.axis_size("cols")
    right_cols = lax.dynamic_slice_in_dim(
        right_all, lax.axis_index("cols") * block, block, 0
    ).reshape(block, -1, chans)
    seqs = left_rows.shape[1]
    multiplier = 1.0 / seqs
    pair_ch = adjoint_update.shape[2]
    step_rows = 4
    rounds = tokens // step_rows
    first_tile_list = left_rows.reshape(rounds, step_rows, seqs, chans)
    cot_blocks = adjoint_update.reshape(rounds, step_rows, block, pair_ch)

    def advance(carry, inputs):
        right_acc, out_acc = carry
        left_slab, cot_slab = inputs
        outer = (
            jnp.einsum("isc,jsd->ijcd", left_slab, right_cols, preferred_element_type=jnp.float32)
            * multiplier
        ).astype(jnp.bfloat16)
        flat = outer.reshape(step_rows * block, chans * chans)
        cot_flat = cot_slab.reshape(step_rows * block, pair_ch)
        update = (
            jnp.dot(flat, final_projector, preferred_element_type=jnp.float32) + additive_term
        ).astype(jnp.bfloat16)
        outer_grad = jnp.dot(
            cot_flat, final_projector.T, preferred_element_type=jnp.float32
        ).astype(jnp.bfloat16)
        outer_grad = outer_grad.reshape(step_rows, block, chans, chans)
        left_piece = (
            jnp.einsum("ijcd,jsd->isc", outer_grad, right_cols, preferred_element_type=jnp.float32)
            * multiplier
        )
        right_acc = (
            right_acc
            + jnp.einsum("ijcd,isc->jsd", outer_grad, left_slab, preferred_element_type=jnp.float32)
            * multiplier
        )
        out_acc = out_acc + jnp.einsum(
            "fk,fe->ke", flat, cot_flat, preferred_element_type=jnp.float32
        )
        return ((right_acc, out_acc), (update.reshape(step_rows, block, pair_ch), left_piece))

    beginning_position = (
        jnp.zeros((block, seqs, chans), jnp.float32),
        jnp.zeros((chans * chans, pair_ch), jnp.float32),
    )
    (right_part, out_term), (updates, left_pieces) = lax.scan(
        advance, beginning_position, (first_tile_list, cot_blocks)
    )
    residue_update = updates.reshape(tokens, block, pair_ch)
    left_part = left_pieces.reshape(tokens, seqs * chans)
    first_adjoint = lax.psum_scatter(left_part, "cols", scatter_dimension=1, tiled=True).reshape(
        tokens, quarter, chans
    )
    moved = lax.all_to_all(
        right_part.reshape(block, seqs * chans), "cols", split_axis=1, concat_axis=0, tiled=True
    )
    right_back = lax.psum_scatter(moved, "rows", scatter_dimension=0, tiled=True).reshape(
        tokens, quarter, chans
    )
    final_projector_slope = lax.psum_scatter(
        out_term, ("rows", "cols"), scatter_dimension=0, tiled=True
    )
    unit_broadcast = unit_alignment.astype(jnp.float32)
    high = lax.Precision.HIGHEST
    left_term = jnp.einsum("tsk,tsc->kc", unit_broadcast, first_adjoint, precision=high)
    right_term = jnp.einsum("tsk,tsc->kc", unit_broadcast, right_back, precision=high)
    first_projector_slope, second_projector_slope = lax.psum(
        (left_term, right_term), ("rows", "cols")
    )
    unit_adjoint = jnp.einsum(
        "tsc,kc->tsk", first_adjoint, first_projector.astype(jnp.float32), precision=high
    )
    unit_adjoint = unit_adjoint + jnp.einsum(
        "tsc,kc->tsk", right_back, second_projector.astype(jnp.float32), precision=high
    )
    scaled_alignment = unit_adjoint * affine_factor
    alignment_slope = reciprocal_spread * (
        scaled_alignment
        - jnp.mean(scaled_alignment, axis=-1, keepdims=True)
        - zscored_alignment * jnp.mean(scaled_alignment * zscored_alignment, axis=-1, keepdims=True)
    )
    return (
        residue_update,
        alignment_slope,
        final_projector_slope,
        first_projector_slope,
        second_projector_slope,
    )


def local_square(
    alignment_features,
    affine_factor,
    affine_offset,
    first_projector,
    second_projector,
    final_projector,
    additive_term,
    adjoint_update,
):
    rows, cols = lax.axis_size("rows"), lax.axis_size("cols")
    zscored_alignment, reciprocal_spread, unit_alignment = layernorm_parts(
        alignment_features, affine_factor, affine_offset
    )
    tokens, quarter, width = unit_alignment.shape
    chans = first_projector.shape[1]
    pair_ch = final_projector.shape[1]
    flip = [(r * cols + q, q * cols + r) for r in range(rows) for q in range(cols)]
    unit_rows = lax.all_gather(unit_alignment, "cols", axis=1, tiled=True)
    left_rows = jnp.dot(
        unit_rows, first_projector, preferred_element_type=jnp.float32
    ).astype(jnp.bfloat16)
    right_rows = jnp.dot(
        unit_rows, second_projector, preferred_element_type=jnp.float32
    ).astype(jnp.bfloat16)
    seqs = left_rows.shape[1]
    multiplier = 1.0 / seqs
    right_cols = lax.ppermute(
        right_rows.reshape(tokens, seqs * chans), ("rows", "cols"), flip
    ).reshape(tokens, seqs, chans)
    cot_flat = adjoint_update.reshape(tokens * tokens, pair_ch)
    outer_grad = (
        jnp.dot(cot_flat, final_projector.T, preferred_element_type=jnp.float32)
        .astype(jnp.bfloat16)
        .reshape(tokens, tokens, chans, chans)
    )
    right_part = (
        jnp.einsum("ijcd,isc->jsd", outer_grad, left_rows, preferred_element_type=jnp.float32)
        * multiplier
    ).astype(jnp.bfloat16)
    right_term = lax.ppermute(
        right_part.reshape(tokens, seqs * chans), ("rows", "cols"), flip
    ).reshape(tokens, seqs, chans)
    outer = (
        jnp.einsum("isc,jsd->ijcd", left_rows, right_cols, preferred_element_type=jnp.float32)
        * multiplier
    ).astype(jnp.bfloat16)
    flat = outer.reshape(tokens * tokens, chans * chans)
    residue_update = (
        (jnp.dot(flat, final_projector, preferred_element_type=jnp.float32) + additive_term)
        .astype(jnp.bfloat16)
        .reshape(tokens, tokens, pair_ch)
    )
    out_term = jnp.einsum("fk,fe->ke", flat, cot_flat, preferred_element_type=jnp.float32)
    left_term = (
        jnp.einsum("ijcd,jsd->isc", outer_grad, right_cols, preferred_element_type=jnp.float32)
        * multiplier
    ).astype(jnp.bfloat16)
    both = jnp.concatenate([left_term, right_term], axis=2)
    slopes = jnp.einsum(
        "tsk,tsc->kc", unit_rows, both, preferred_element_type=jnp.float32
    ).astype(jnp.bfloat16)
    share = out_term.shape[0] // (rows * cols)
    out_blocks = (
        out_term.astype(jnp.bfloat16)
        .reshape(rows, cols, share * pair_ch)
        .transpose(1, 0, 2)
        .reshape(cols, rows * share, pair_ch)
    )
    both_blocks = (
        both.reshape(tokens, cols, quarter * 2 * chans)
        .transpose(1, 0, 2)
        .reshape(cols, -1, pair_ch)
    )
    slope_rows = slopes.reshape(-1, pair_ch)
    message = jnp.concatenate(
        [
            out_blocks,
            both_blocks,
            jnp.broadcast_to(slope_rows, (cols,) + slope_rows.shape),
        ],
        axis=1,
    )
    got = lax.all_to_all(message, "cols", 0, 0, tiled=True)
    summed = jnp.sum(got.astype(jnp.float32), axis=0)
    first_cut, second_cut = rows * share, rows * share + both_blocks.shape[1]
    back = summed[first_cut:second_cut].reshape(tokens, quarter, 2 * chans)
    message = jnp.concatenate(
        [
            summed[:first_cut].reshape(rows, share, pair_ch),
            jnp.broadcast_to(summed[second_cut:], (rows,) + slope_rows.shape),
        ],
        axis=1,
    ).astype(jnp.bfloat16)
    got = jnp.sum(
        lax.all_to_all(message, "rows", 0, 0, tiled=True).astype(jnp.float32), axis=0
    )
    final_projector_slope = got[:share]
    slopes = got[share:].reshape(width, 2 * chans)
    high = lax.Precision.HIGHEST
    both_projectors = jnp.concatenate([first_projector, second_projector], axis=1)
    unit_adjoint = jnp.einsum(
        "tsc,kc->tsk", back, both_projectors.astype(jnp.float32), precision=high
    )
    scaled_alignment = unit_adjoint * affine_factor
    alignment_slope = reciprocal_spread * (
        scaled_alignment
        - jnp.mean(scaled_alignment, axis=-1, keepdims=True)
        - zscored_alignment * jnp.mean(scaled_alignment * zscored_alignment, axis=-1, keepdims=True)
    )
    return (
        residue_update,
        alignment_slope,
        final_projector_slope,
        slopes[:, :chans],
        slopes[:, chans:],
    )


def solution(mesh):
    rows, cols = mesh.shape["rows"], mesh.shape["cols"]
    local = local_square if rows == cols else local_general
    in_specs = (
        P(("groups", "rows"), "cols", None),
        P(),
        P(),
        P(),
        P(),
        P(),
        P(),
        P(("groups", "rows"), "cols", None),
    )
    out_specs = (
        P(("groups", "rows"), "cols", None),
        P(("groups", "rows"), "cols", None),
        P(("groups", "rows", "cols"), None),
        P("groups", None),
        P("groups", None),
    )
    return jax.shard_map(local, mesh=mesh, in_specs=in_specs, out_specs=out_specs, check_vma=False)
```

```python
import functools

import jax
import jax.numpy as jnp
from jax import lax
from jax.experimental import pallas as pl
from jax.experimental.pallas import tpu as pltpu
from jax.sharding import PartitionSpec as P


def layernorm_parts(alignment_features, affine_factor, affine_offset):
    centered_alignment = alignment_features - jnp.mean(alignment_features, axis=-1, keepdims=True)
    reciprocal_spread = lax.rsqrt(
        jnp.mean(centered_alignment * centered_alignment, axis=-1, keepdims=True) + 1e-05
    )
    zscored_alignment = centered_alignment * reciprocal_spread
    return (
        zscored_alignment,
        reciprocal_spread,
        (zscored_alignment * affine_factor + affine_offset).astype(jnp.bfloat16),
    )


def local_general(
    alignment_features,
    affine_factor,
    affine_offset,
    first_projector,
    second_projector,
    final_projector,
    additive_term,
    adjoint_update,
):
    zscored_alignment, reciprocal_spread, unit_alignment = layernorm_parts(
        alignment_features, affine_factor, affine_offset
    )
    first_factor_here = jnp.dot(
        unit_alignment, first_projector, preferred_element_type=jnp.float32
    ).astype(jnp.bfloat16)
    second_factor_here = jnp.dot(
        unit_alignment, second_projector, preferred_element_type=jnp.float32
    ).astype(jnp.bfloat16)
    tokens, quarter, chans = first_factor_here.shape
    left_flat = first_factor_here.reshape(tokens, quarter * chans)
    right_flat = second_factor_here.reshape(tokens, quarter * chans)
    left_wide, right_wide = (
        lax.all_gather(left_flat, "cols", axis=1, tiled=True),
        lax.all_gather(right_flat, "cols", axis=1, tiled=True),
    )
    left_rows = left_wide.reshape(tokens, -1, chans)
    right_all = lax.all_gather(right_wide, "rows", axis=0, tiled=True)
    block = right_all.shape[0] // lax.axis_size("cols")
    right_cols = lax.dynamic_slice_in_dim(
        right_all, lax.axis_index("cols") * block, block, 0
    ).reshape(block, -1, chans)
    seqs = left_rows.shape[1]
    multiplier = 1.0 / seqs
    pair_ch = adjoint_update.shape[2]
    step_rows = 4
    rounds = tokens // step_rows
    first_tile_list = left_rows.reshape(rounds, step_rows, seqs, chans)
    cot_blocks = adjoint_update.reshape(rounds, step_rows, block, pair_ch)

    def advance(carry, inputs):
        right_acc, out_acc = carry
        left_slab, cot_slab = inputs
        outer = (
            jnp.einsum("isc,jsd->ijcd", left_slab, right_cols, preferred_element_type=jnp.float32)
            * multiplier
        ).astype(jnp.bfloat16)
        flat = outer.reshape(step_rows * block, chans * chans)
        cot_flat = cot_slab.reshape(step_rows * block, pair_ch)
        update = (
            jnp.dot(flat, final_projector, preferred_element_type=jnp.float32) + additive_term
        ).astype(jnp.bfloat16)
        outer_grad = jnp.dot(
            cot_flat, final_projector.T, preferred_element_type=jnp.float32
        ).astype(jnp.bfloat16)
        outer_grad = outer_grad.reshape(step_rows, block, chans, chans)
        left_piece = (
            jnp.einsum("ijcd,jsd->isc", outer_grad, right_cols, preferred_element_type=jnp.float32)
            * multiplier
        )
        right_acc = (
            right_acc
            + jnp.einsum("ijcd,isc->jsd", outer_grad, left_slab, preferred_element_type=jnp.float32)
            * multiplier
        )
        out_acc = out_acc + jnp.einsum(
            "fk,fe->ke", flat, cot_flat, preferred_element_type=jnp.float32
        )
        return ((right_acc, out_acc), (update.reshape(step_rows, block, pair_ch), left_piece))

    beginning_position = (
        jnp.zeros((block, seqs, chans), jnp.float32),
        jnp.zeros((chans * chans, pair_ch), jnp.float32),
    )
    (right_part, out_term), (updates, left_pieces) = lax.scan(
        advance, beginning_position, (first_tile_list, cot_blocks)
    )
    residue_update = updates.reshape(tokens, block, pair_ch)
    left_part = left_pieces.reshape(tokens, seqs * chans)
    first_adjoint = lax.psum_scatter(left_part, "cols", scatter_dimension=1, tiled=True).reshape(
        tokens, quarter, chans
    )
    moved = lax.all_to_all(
        right_part.reshape(block, seqs * chans), "cols", split_axis=1, concat_axis=0, tiled=True
    )
    right_back = lax.psum_scatter(moved, "rows", scatter_dimension=0, tiled=True).reshape(
        tokens, quarter, chans
    )
    final_projector_slope = lax.psum_scatter(
        out_term, ("rows", "cols"), scatter_dimension=0, tiled=True
    )
    unit_broadcast = unit_alignment.astype(jnp.float32)
    high = lax.Precision.HIGHEST
    left_term = jnp.einsum("tsk,tsc->kc", unit_broadcast, first_adjoint, precision=high)
    right_term = jnp.einsum("tsk,tsc->kc", unit_broadcast, right_back, precision=high)
    first_projector_slope, second_projector_slope = lax.psum(
        (left_term, right_term), ("rows", "cols")
    )
    unit_adjoint = jnp.einsum(
        "tsc,kc->tsk", first_adjoint, first_projector.astype(jnp.float32), precision=high
    )
    unit_adjoint = unit_adjoint + jnp.einsum(
        "tsc,kc->tsk", right_back, second_projector.astype(jnp.float32), precision=high
    )
    scaled_alignment = unit_adjoint * affine_factor
    alignment_slope = reciprocal_spread * (
        scaled_alignment
        - jnp.mean(scaled_alignment, axis=-1, keepdims=True)
        - zscored_alignment * jnp.mean(scaled_alignment * zscored_alignment, axis=-1, keepdims=True)
    )
    return (
        residue_update,
        alignment_slope,
        final_projector_slope,
        first_projector_slope,
        second_projector_slope,
    )


F32, BF16 = jnp.float32, jnp.bfloat16
LANES, SUBLANES = 128, 8


def dot(a, b, at=1, bt=0):
    return lax.dot_general(a, b, (((at,), (bt,)), ((), ())), preferred_element_type=F32)


def lane_group(shape, chans):
    return lax.broadcasted_iota(jnp.int32, shape, len(shape) - 1) // chans


def pick(parts, group):
    out = parts[-1]
    for b in range(len(parts) - 2, -1, -1):
        out = jnp.where(group == b, parts[b], out)
    return out


def normalise(x):
    centered = x - jnp.mean(x, axis=-1, keepdims=True)
    spread = lax.rsqrt(jnp.mean(centered * centered, axis=-1, keepdims=True) + 1e-05)
    return centered * spread, spread


def call(kernel, out_shape, scratch=(), flops=0, **kw):
    return pl.pallas_call(
        kernel,
        out_shape=out_shape,
        scratch_shapes=list(scratch),
        cost_estimate=pl.CostEstimate(flops=flops, bytes_accessed=0, transcendentals=0),
        **kw,
    )


def norm_kernel(x_ref, gain_ref, offset_ref, out_ref):
    tokens, quarter, width = x_ref.shape
    xhat, _ = normalise(x_ref[...].reshape(tokens * quarter, width))
    unit = xhat * gain_ref[...] + offset_ref[...]
    half = tokens * quarter // 2
    out_ref[...] = jnp.concatenate([unit[:half], unit[half:]], axis=1).astype(BF16)


def grad_kernel(
    cot_ref, final_ref, by_col_ref, by_row_ref, cot_cols_ref, cot_f, final_f, *, chans
):
    tokens, block, _ = cot_ref.shape
    steps = by_col_ref.shape[0] // tokens
    cot = cot_ref[...]
    final = final_ref[...]
    cot_f[...] = cot.astype(F32)
    final_f[...] = final.astype(F32)
    for j in range(block):
        cot_cols_ref[j * tokens : (j + 1) * tokens, :] = cot_f[:, j, :].astype(BF16)
    cot_cols = cot_cols_ref[...]
    cot_rows = cot.reshape(tokens * block, cot.shape[2])
    per = LANES // chans
    for a in range(steps):
        lanes_cd = final[a * LANES : (a + 1) * LANES]
        got = dot(cot_cols, lanes_cd, 1, 1).astype(BF16)
        for j in range(block):
            by_col_ref[a * tokens : (a + 1) * tokens, j * LANES : (j + 1) * LANES] = got[
                j * tokens : (j + 1) * tokens
            ]
        lanes_dc = jnp.concatenate(
            [final_f[pl.ds(a * per + b, chans, stride=chans), :] for b in range(per)], axis=0
        ).astype(BF16)
        got = dot(cot_rows, lanes_dc, 1, 1).astype(BF16)
        for i in range(tokens):
            by_row_ref[a * block : (a + 1) * block, i * LANES : (i + 1) * LANES] = got[
                i * block : (i + 1) * block
            ]


def fold(spread_ref, seqs, chans, tokens):
    per = LANES // chans
    group = lane_group((seqs, LANES), chans)
    out = []
    for p in range(tokens // per):
        total = None
        for shift in range(per):
            parts = []
            for b in range(per):
                t = p * per + (b + shift) % per
                parts.append(spread_ref[b * seqs : (b + 1) * seqs, t * LANES : (t + 1) * LANES])
            part = pick(parts, group)
            if shift:
                part = pltpu.roll(part, shift * chans, 1)
            total = part if total is None else total + part
        out.append(total)
    return out


def padded_projectors(first, second, b, per):
    zero = jnp.zeros_like(first)
    return jnp.concatenate(
        [x if i == b else zero for x in (first, second) for i in range(per)], axis=0
    )


def project_kernel(
    n0, n1, n2, n3, first_ref, second_ref, by_col_ref, send_ref, left_ref, unit_ref, unit_f, proj_f, wide_f, spread_f,
):
    blocks = (n0, n1, n2, n3)
    seqs, width = unit_f.shape[1], unit_f.shape[2]
    tokens = unit_f.shape[0]
    quarter = seqs // len(blocks)
    chans = first_ref.shape[0]
    per, steps = LANES // chans, chans // (LANES // chans)
    mine = lax.axis_index("cols")
    half = tokens // 2
    for k, ref in enumerate(blocks):
        at = pl.multiple_of((mine ^ k) * quarter, quarter)
        got = ref[...].astype(F32)
        for h in range(2):
            unit_f[h * half : (h + 1) * half, pl.ds(at, quarter), :] = got[
                :, h * width : (h + 1) * width
            ].reshape(half, quarter, width)
    unit = unit_f[...].astype(BF16)
    first, second = first_ref[...], second_ref[...]
    total = None
    by_group = unit.reshape(tokens // per, per, seqs, width)
    for b in range(per):
        part = by_group[:, b].reshape(tokens // per * seqs, width)
        unit_ref[b] = part
        got = dot(part, padded_projectors(first, second, b, per), 1, 1)
        total = got if total is None else total + got
    rows = tokens // per * seqs
    send_ref[0:rows, :] = total[:, LANES:].astype(BF16)
    proj_f[0] = first.astype(F32)
    proj_f[1] = second.astype(F32)
    permuted = jnp.concatenate(
        [proj_f[x, pl.ds(b, steps, stride=per), :] for x in range(2) for b in range(per)], axis=0
    ).astype(BF16)
    tall = dot(permuted, unit.reshape(tokens * seqs, width), 1, 1).astype(BF16).astype(F32)
    group = lane_group((steps, LANES), chans)
    for x in range(2):
        for p in range(tokens // per):
            tiles = [
                tall[
                    (x * per + b) * steps : (x * per + b + 1) * steps, p * LANES : (p + 1) * LANES
                ]
                for b in range(per)
            ]
            for own in range(per):
                parts = [
                    pltpu.roll(tile, (b - own) % per * chans, 1) if b != own else tile
                    for b, tile in enumerate(tiles)
                ]
                wide_f[x, :, p * per + own, :] = pick(parts, group)
    left = wide_f[0].reshape(steps * tokens, LANES)
    left_ref[...] = left.astype(BF16)
    send_ref[2 * rows : 2 * rows + steps * tokens, :] = (
        wide_f[1].reshape(steps * tokens, LANES).astype(BF16)
    )
    spread_f[...] = dot(left.T.astype(BF16), by_col_ref[...])
    for p, tile in enumerate(fold(spread_f, seqs, chans, tokens)):
        send_ref[rows + p * seqs : rows + (p + 1) * seqs, :] = (tile * (1.0 / seqs)).astype(BF16)


def pair_kernel(
    right_ref, left_ref, unit_ref, by_row_ref, final_ref, cot_cols_ref, bias_ref,
    update_ref, own_ref, m1, m2, m3,
    outer_ref, update_f, slope_f, spread_f, both_f,
    *, chans, rows_axis, cols_axis,
):
    per, steps = LANES // chans, chans // (LANES // chans)
    tokens = update_ref.shape[0]
    groups = tokens // per
    seqs = both_f.shape[2]
    rows = groups * seqs
    quarter = seqs // cols_axis
    share = slope_f.shape[0] // (rows_axis * cols_axis)
    mine = lax.axis_index("cols")
    group = lane_group((seqs, LANES), chans)
    left = left_ref[...]
    for p in range(groups):
        tile = right_ref[p * seqs : (p + 1) * seqs, :].astype(F32)
        rolled = [pltpu.roll(tile, s * chans, 1) if s else tile for s in range(per)]
        for own in range(per):
            j = p * per + own
            blocks = jnp.concatenate(
                [jnp.where(group == b, rolled[(b - own) % per], 0.0) for b in range(per)], axis=0
            ).astype(BF16)
            got = (dot(left, blocks) * (1.0 / seqs)).astype(BF16)
            for a in range(steps):
                outer_ref[j * tokens : (j + 1) * tokens, a * LANES : (a + 1) * LANES] = got[
                    a * tokens : (a + 1) * tokens
                ]
    outer = outer_ref[...]
    slope_f[...] = dot(outer, cot_cols_ref[...], 0, 0)
    update = dot(outer, final_ref[...]) + bias_ref[...]
    for j in range(tokens):
        update_f[:, j, :] = update[j * tokens : (j + 1) * tokens]
    update_ref[...] = update_f[...].astype(BF16)
    wide = right_ref[2 * rows : 2 * rows + steps * tokens, :].astype(F32)
    spread_f[...] = dot(wide.T.astype(BF16), by_row_ref[...])
    for p, tile in enumerate(fold(spread_f, seqs, chans, tokens)):
        both_f[p, 0] = tile * (1.0 / seqs)
        both_f[p, 1] = right_ref[rows + p * seqs : rows + (p + 1) * seqs, :].astype(F32)
    both = jnp.concatenate(
        [both_f[:, x].reshape(rows, LANES).astype(BF16) for x in range(2)], axis=1
    )
    width = unit_ref.shape[2]
    slopes = pick(
        [dot(unit_ref[b], both, 0, 0) for b in range(per)],
        lane_group((width, 2 * LANES), chans) % per,
    )
    sides = [slopes[:, x * LANES : (x + 1) * LANES] for x in range(2)]
    sides = [s + pltpu.roll(s, LANES // 2, 1) for s in sides]
    slopes = jnp.where(lane_group((width, LANES), LANES // 2) == 0, sides[0], sides[1])
    for k, ref in enumerate((own_ref, m1, m2, m3)):
        peer = mine ^ k
        kind = ref.dtype
        for r in range(rows_axis):
            at = pl.multiple_of((r * cols_axis + peer) * share, share)
            ref[r * share : (r + 1) * share, :] = slope_f[pl.ds(at, share), :].astype(kind)
        base = rows_axis * share
        at = pl.multiple_of(peer * quarter, quarter)
        span = 2 * quarter
        for p in range(groups):
            ref[base + p * span : base + (p + 1) * span, :] = (
                both_f[p, :, pl.ds(at, quarter), :].reshape(span, LANES).astype(kind)
            )
        base += groups * span
        ref[base : base + width, :] = slopes.astype(kind)


def between_kernel(own_ref, r1, r2, r3, back_ref, next_ref, m1, m2, m3, total_f, *, rows_axis, share):
    total_f[...] = (
        own_ref[...] + r1[...].astype(F32) + r2[...].astype(F32) + r3[...].astype(F32)
    )
    mine = lax.axis_index("rows")
    first = rows_axis * share
    last = first + back_ref.shape[0]
    back_ref[...] = total_f[first:last, :]
    slopes = total_f[last:, :]
    for k, ref in enumerate((next_ref, m1, m2, m3)):
        at = pl.multiple_of((mine ^ k) * share, share)
        ref[0:share, :] = total_f[pl.ds(at, share), :].astype(ref.dtype)
        ref[share:, :] = slopes.astype(ref.dtype)


def back_kernel(back_ref, x_ref, gain_ref, first_ref, second_ref, out_ref, unit_f):
    tokens, quarter, width = x_ref.shape
    chans = first_ref.shape[0]
    per = LANES // chans
    groups = tokens // per
    back = back_ref[...].reshape(groups, 2, quarter, LANES)
    wide = jnp.concatenate([back[:, x].reshape(groups * quarter, LANES) for x in range(2)], axis=1)
    high = wide.astype(BF16)
    low = (wide - high.astype(F32)).astype(BF16)
    first, second = first_ref[...], second_ref[...]
    for b in range(per):
        weights = padded_projectors(first, second, b, per)
        got = dot(high, weights) + dot(low, weights)
        for p in range(groups):
            unit_f[p * per + b] = got[p * quarter : (p + 1) * quarter]
    xhat, spread = normalise(x_ref[...].reshape(tokens * quarter, width))
    g = unit_f[...].reshape(tokens * quarter, width) * gain_ref[...]
    out = spread * (
        g
        - jnp.mean(g, axis=-1, keepdims=True)
        - xhat * jnp.mean(g * xhat, axis=-1, keepdims=True)
    )
    out_ref[...] = out.reshape(tokens, quarter, width)


def last_kernel(own_ref, r1, r2, r3, final_ref, first_ref, second_ref):
    total = own_ref[...] + r1[...].astype(F32) + r2[...].astype(F32) + r3[...].astype(F32)
    share = final_ref.shape[0]
    final_ref[...] = total[:share]
    slopes = total[share:].T
    chans = first_ref.shape[0]
    for x, ref in enumerate((first_ref, second_ref)):
        side = slopes[x * LANES // 2 : (x + 1) * LANES // 2]
        out = side[:chans]
        for b in range(1, LANES // 2 // chans):
            out = out + side[b * chans : (b + 1) * chans]
        ref[...] = out


def exchange(messages, axis):
    size = lax.axis_size(axis)
    return [
        lax.ppermute(m, axis, [(p, p ^ k) for p in range(size)])
        for k, m in enumerate(messages, 1)
    ]


def local_square(
    alignment_features,
    affine_factor,
    affine_offset,
    first_projector,
    second_projector,
    final_projector,
    additive_term,
    adjoint_update,
):
    rows, cols = lax.axis_size("rows"), lax.axis_size("cols")
    tokens, quarter, width = alignment_features.shape
    chans = first_projector.shape[1]
    total, pair_ch = final_projector.shape
    seqs = quarter * cols
    per, steps = LANES // chans, chans // (LANES // chans)
    share = total // (rows * cols)
    flip = [(r * cols + q, q * cols + r) for r in range(rows) for q in range(cols)]
    shape = jax.ShapeDtypeStruct
    gain = affine_factor.reshape(1, width)
    offset = affine_offset.reshape(1, width)
    first, second = first_projector.T, second_projector.T
    wide = tokens * LANES
    tall = steps * tokens
    packed = tokens // per * seqs
    unit = call(norm_kernel, shape((tokens * quarter // 2, 2 * width), BF16))(
        alignment_features, gain, offset
    )
    units = [unit] + exchange([unit] * (cols - 1), "cols")
    by_col, by_row, cot_cols = call(
        functools.partial(grad_kernel, chans=chans),
        (
            shape((tall, wide), BF16),
            shape((tall, wide), BF16),
            shape((tokens * tokens, pair_ch), BF16),
        ),
        [pltpu.VMEM(adjoint_update.shape, F32), pltpu.VMEM((total, pair_ch), F32)],
        flops=8 * tokens * tokens * total * pair_ch,
    )(adjoint_update, final_projector)
    send, left, unit_rows = call(
        project_kernel,
        (
            shape((2 * packed + tall, LANES), BF16),
            shape((tall, LANES), BF16),
            shape((per, packed, width), BF16),
        ),
        [
            pltpu.VMEM((tokens, seqs, width), F32),
            pltpu.VMEM((2, chans, width), F32),
            pltpu.VMEM((2, steps, tokens, LANES), F32),
            pltpu.VMEM((LANES, wide), F32),
        ],
    )(*units, first, second, by_col)
    right = lax.ppermute(send, ("rows", "cols"), flip)
    message = rows * share + 2 * quarter * tokens // per + width
    update, own, *messages = call(
        functools.partial(pair_kernel, chans=chans, rows_axis=rows, cols_axis=cols),
        (
            shape((tokens, tokens, pair_ch), BF16),
            shape((message, LANES), F32),
            *[shape((message, LANES), BF16)] * (cols - 1),
        ),
        [
            pltpu.VMEM((tokens * tokens, total), BF16),
            pltpu.VMEM((tokens, tokens, pair_ch), F32),
            pltpu.VMEM((total, pair_ch), F32),
            pltpu.VMEM((LANES, wide), F32),
            pltpu.VMEM((tokens // per, 2, seqs, LANES), F32),
        ],
    )(right, left, unit_rows, by_row, final_projector, cot_cols, additive_term.reshape(1, pair_ch))
    got = exchange(messages, "cols")
    back, own, *messages = call(
        functools.partial(between_kernel, rows_axis=rows, share=share),
        (
            shape((2 * quarter * tokens // per, LANES), F32),
            shape((share + width, LANES), F32),
            *[shape((share + width, LANES), BF16)] * (rows - 1),
        ),
        [pltpu.VMEM((message, LANES), F32)],
    )(own, *got)
    got = exchange(messages, "rows")
    alignment_slope = call(
        back_kernel,
        shape((tokens, quarter, width), F32),
        [pltpu.VMEM((tokens, quarter, width), F32)],
        flops=10**8,
    )(back, alignment_features, gain, first, second)
    final_slope, first_slope, second_slope = call(
        last_kernel,
        (shape((share, pair_ch), F32), shape((chans, width), F32), shape((chans, width), F32)),
    )(own, *got)
    return update, alignment_slope, final_slope, first_slope.T, second_slope.T


def fits(mesh, alignment_features, first_projector, final_projector):
    rows, cols = mesh.shape["rows"], mesh.shape["cols"]
    tokens = alignment_features.shape[0] // (mesh.shape["groups"] * rows)
    quarter = alignment_features.shape[1] // cols
    width, chans = first_projector.shape
    per = LANES // chans
    return (
        rows == cols == 4
        and chans * per == LANES
        and chans % per == 0
        and chans // per == SUBLANES
        and 2 * width == LANES
        and final_projector.shape[1] == LANES
        and quarter == SUBLANES
        and tokens % (2 * SUBLANES) == 0
        and quarter * cols == chans
        and chans // per * tokens == LANES
    )


def solution(mesh):
    in_specs = (
        P(("groups", "rows"), "cols", None),
        P(),
        P(),
        P(),
        P(),
        P(),
        P(),
        P(("groups", "rows"), "cols", None),
    )
    out_specs = (
        P(("groups", "rows"), "cols", None),
        P(("groups", "rows"), "cols", None),
        P(("groups", "rows", "cols"), None),
        P("groups", None),
        P("groups", None),
    )

    def whole(*args):
        square = fits(mesh, args[0], args[3], args[5])
        return jax.shard_map(
            local_square if square else local_general,
            mesh=mesh,
            in_specs=in_specs,
            out_specs=out_specs,
            check_vma=False,
        )(*args)

    return whole
```

```python
import functools

import jax
import jax.numpy as jnp
from jax import lax
from jax.experimental import pallas as pl
from jax.experimental.pallas import tpu as pltpu
from jax.sharding import PartitionSpec as P


def layernorm_parts(alignment_features, affine_factor, affine_offset):
    centered_alignment = alignment_features - jnp.mean(alignment_features, axis=-1, keepdims=True)
    reciprocal_spread = lax.rsqrt(
        jnp.mean(centered_alignment * centered_alignment, axis=-1, keepdims=True) + 1e-05
    )
    zscored_alignment = centered_alignment * reciprocal_spread
    return (
        zscored_alignment,
        reciprocal_spread,
        (zscored_alignment * affine_factor + affine_offset).astype(jnp.bfloat16),
    )


def local_general(
    alignment_features,
    affine_factor,
    affine_offset,
    first_projector,
    second_projector,
    final_projector,
    additive_term,
    adjoint_update,
):
    zscored_alignment, reciprocal_spread, unit_alignment = layernorm_parts(
        alignment_features, affine_factor, affine_offset
    )
    first_factor_here = jnp.dot(
        unit_alignment, first_projector, preferred_element_type=jnp.float32
    ).astype(jnp.bfloat16)
    second_factor_here = jnp.dot(
        unit_alignment, second_projector, preferred_element_type=jnp.float32
    ).astype(jnp.bfloat16)
    tokens, quarter, chans = first_factor_here.shape
    left_flat = first_factor_here.reshape(tokens, quarter * chans)
    right_flat = second_factor_here.reshape(tokens, quarter * chans)
    left_wide, right_wide = (
        lax.all_gather(left_flat, "cols", axis=1, tiled=True),
        lax.all_gather(right_flat, "cols", axis=1, tiled=True),
    )
    left_rows = left_wide.reshape(tokens, -1, chans)
    right_all = lax.all_gather(right_wide, "rows", axis=0, tiled=True)
    block = right_all.shape[0] // lax.axis_size("cols")
    right_cols = lax.dynamic_slice_in_dim(
        right_all, lax.axis_index("cols") * block, block, 0
    ).reshape(block, -1, chans)
    seqs = left_rows.shape[1]
    multiplier = 1.0 / seqs
    pair_ch = adjoint_update.shape[2]
    step_rows = 4
    rounds = tokens // step_rows
    first_tile_list = left_rows.reshape(rounds, step_rows, seqs, chans)
    cot_blocks = adjoint_update.reshape(rounds, step_rows, block, pair_ch)

    def advance(carry, inputs):
        right_acc, out_acc = carry
        left_slab, cot_slab = inputs
        outer = (
            jnp.einsum("isc,jsd->ijcd", left_slab, right_cols, preferred_element_type=jnp.float32)
            * multiplier
        ).astype(jnp.bfloat16)
        flat = outer.reshape(step_rows * block, chans * chans)
        cot_flat = cot_slab.reshape(step_rows * block, pair_ch)
        update = (
            jnp.dot(flat, final_projector, preferred_element_type=jnp.float32) + additive_term
        ).astype(jnp.bfloat16)
        outer_grad = jnp.dot(
            cot_flat, final_projector.T, preferred_element_type=jnp.float32
        ).astype(jnp.bfloat16)
        outer_grad = outer_grad.reshape(step_rows, block, chans, chans)
        left_piece = (
            jnp.einsum("ijcd,jsd->isc", outer_grad, right_cols, preferred_element_type=jnp.float32)
            * multiplier
        )
        right_acc = (
            right_acc
            + jnp.einsum("ijcd,isc->jsd", outer_grad, left_slab, preferred_element_type=jnp.float32)
            * multiplier
        )
        out_acc = out_acc + jnp.einsum(
            "fk,fe->ke", flat, cot_flat, preferred_element_type=jnp.float32
        )
        return ((right_acc, out_acc), (update.reshape(step_rows, block, pair_ch), left_piece))

    beginning_position = (
        jnp.zeros((block, seqs, chans), jnp.float32),
        jnp.zeros((chans * chans, pair_ch), jnp.float32),
    )
    (right_part, out_term), (updates, left_pieces) = lax.scan(
        advance, beginning_position, (first_tile_list, cot_blocks)
    )
    residue_update = updates.reshape(tokens, block, pair_ch)
    left_part = left_pieces.reshape(tokens, seqs * chans)
    first_adjoint = lax.psum_scatter(left_part, "cols", scatter_dimension=1, tiled=True).reshape(
        tokens, quarter, chans
    )
    moved = lax.all_to_all(
        right_part.reshape(block, seqs * chans), "cols", split_axis=1, concat_axis=0, tiled=True
    )
    right_back = lax.psum_scatter(moved, "rows", scatter_dimension=0, tiled=True).reshape(
        tokens, quarter, chans
    )
    final_projector_slope = lax.psum_scatter(
        out_term, ("rows", "cols"), scatter_dimension=0, tiled=True
    )
    unit_broadcast = unit_alignment.astype(jnp.float32)
    high = lax.Precision.HIGHEST
    left_term = jnp.einsum("tsk,tsc->kc", unit_broadcast, first_adjoint, precision=high)
    right_term = jnp.einsum("tsk,tsc->kc", unit_broadcast, right_back, precision=high)
    first_projector_slope, second_projector_slope = lax.psum(
        (left_term, right_term), ("rows", "cols")
    )
    unit_adjoint = jnp.einsum(
        "tsc,kc->tsk", first_adjoint, first_projector.astype(jnp.float32), precision=high
    )
    unit_adjoint = unit_adjoint + jnp.einsum(
        "tsc,kc->tsk", right_back, second_projector.astype(jnp.float32), precision=high
    )
    scaled_alignment = unit_adjoint * affine_factor
    alignment_slope = reciprocal_spread * (
        scaled_alignment
        - jnp.mean(scaled_alignment, axis=-1, keepdims=True)
        - zscored_alignment * jnp.mean(scaled_alignment * zscored_alignment, axis=-1, keepdims=True)
    )
    return (
        residue_update,
        alignment_slope,
        final_projector_slope,
        first_projector_slope,
        second_projector_slope,
    )


F32, BF16 = jnp.float32, jnp.bfloat16
LANES, SUBLANES = 128, 8


def dot(a, b, at=1, bt=0):
    return lax.dot_general(a, b, (((at,), (bt,)), ((), ())), preferred_element_type=F32)


def lane_group(shape, chans):
    return lax.broadcasted_iota(jnp.int32, shape, len(shape) - 1) // chans


def pick(parts, group):
    out = parts[-1]
    for b in range(len(parts) - 2, -1, -1):
        out = jnp.where(group == b, parts[b], out)
    return out


def normalise(x):
    centered = x - jnp.mean(x, axis=-1, keepdims=True)
    spread = lax.rsqrt(jnp.mean(centered * centered, axis=-1, keepdims=True) + 1e-05)
    return centered * spread, spread


def call(kernel, out_shape, scratch=(), flops=0):
    on_chip = pl.BlockSpec(memory_space=pltpu.VMEM)

    def run(*args):
        return pl.pallas_call(
            kernel,
            out_shape=out_shape,
            in_specs=[on_chip] * len(args),
            out_specs=jax.tree.map(lambda _: on_chip, out_shape),
            scratch_shapes=list(scratch),
            cost_estimate=pl.CostEstimate(flops=flops, bytes_accessed=0, transcendentals=0),
            compiler_params=pltpu.CompilerParams(vmem_limit_bytes=16 * 2**20),
        )(*args)

    return run


def norm_kernel(x_ref, gain_ref, offset_ref, out_ref):
    tokens, quarter, width = x_ref.shape
    xhat, _ = normalise(x_ref[...].reshape(tokens * quarter, width))
    unit = xhat * gain_ref[...] + offset_ref[...]
    half = tokens * quarter // 2
    out_ref[...] = jnp.concatenate([unit[:half], unit[half:]], axis=1).astype(BF16)


def grad_kernel(
    cot_ref, final_ref, by_col_ref, by_row_ref, cot_cols_ref, cot_f, final_f, *, chans
):
    tokens, block, _ = cot_ref.shape
    steps = by_col_ref.shape[0] // tokens
    cot = cot_ref[...]
    final = final_ref[...]
    cot_f[...] = cot.astype(F32)
    final_f[...] = final.astype(F32)
    for j in range(block):
        cot_cols_ref[j * tokens : (j + 1) * tokens, :] = cot_f[:, j, :].astype(BF16)
    cot_cols = cot_cols_ref[...]
    cot_rows = cot.reshape(tokens * block, cot.shape[2])
    per = LANES // chans
    for a in range(steps):
        lanes_cd = final[a * LANES : (a + 1) * LANES]
        got = dot(cot_cols, lanes_cd, 1, 1).astype(BF16)
        for j in range(block):
            by_col_ref[a * tokens : (a + 1) * tokens, j * LANES : (j + 1) * LANES] = got[
                j * tokens : (j + 1) * tokens
            ]
        lanes_dc = jnp.concatenate(
            [final_f[pl.ds(a * per + b, chans, stride=chans), :] for b in range(per)], axis=0
        ).astype(BF16)
        got = dot(cot_rows, lanes_dc, 1, 1).astype(BF16)
        for i in range(tokens):
            by_row_ref[a * block : (a + 1) * block, i * LANES : (i + 1) * LANES] = got[
                i * block : (i + 1) * block
            ]


def fold(spread_ref, seqs, chans, tokens):
    per = LANES // chans
    group = lane_group((seqs, LANES), chans)
    out = []
    for p in range(tokens // per):
        total = None
        for shift in range(per):
            parts = []
            for b in range(per):
                t = p * per + (b + shift) % per
                parts.append(spread_ref[b * seqs : (b + 1) * seqs, t * LANES : (t + 1) * LANES])
            part = pick(parts, group)
            if shift:
                part = pltpu.roll(part, shift * chans, 1)
            total = part if total is None else total + part
        out.append(total)
    return out


def padded_projectors(first, second, b, per):
    zero = jnp.zeros_like(first)
    return jnp.concatenate(
        [x if i == b else zero for x in (first, second) for i in range(per)], axis=0
    )


def project_kernel(
    n0, n1, n2, n3, first_ref, second_ref, by_col_ref, send_ref, left_ref, unit_ref, unit_f, proj_f, wide_f, spread_f,
):
    blocks = (n0, n1, n2, n3)
    seqs, width = unit_f.shape[1], unit_f.shape[2]
    tokens = unit_f.shape[0]
    quarter = seqs // len(blocks)
    chans = first_ref.shape[0]
    per, steps = LANES // chans, chans // (LANES // chans)
    mine = lax.axis_index("cols")
    half = tokens // 2
    for k, ref in enumerate(blocks):
        at = pl.multiple_of((mine ^ k) * quarter, quarter)
        got = ref[...].astype(F32)
        for h in range(2):
            unit_f[h * half : (h + 1) * half, pl.ds(at, quarter), :] = got[
                :, h * width : (h + 1) * width
            ].reshape(half, quarter, width)
    unit = unit_f[...].astype(BF16)
    first, second = first_ref[...], second_ref[...]
    total = None
    by_group = unit.reshape(tokens // per, per, seqs, width)
    for b in range(per):
        part = by_group[:, b].reshape(tokens // per * seqs, width)
        unit_ref[b] = part
        got = dot(part, padded_projectors(first, second, b, per), 1, 1)
        total = got if total is None else total + got
    rows = tokens // per * seqs
    send_ref[0:rows, :] = total[:, LANES:].astype(BF16)
    proj_f[0] = first.astype(F32)
    proj_f[1] = second.astype(F32)
    permuted = jnp.concatenate(
        [proj_f[x, pl.ds(b, steps, stride=per), :] for x in range(2) for b in range(per)], axis=0
    ).astype(BF16)
    tall = dot(permuted, unit.reshape(tokens * seqs, width), 1, 1).astype(BF16).astype(F32)
    group = lane_group((steps, LANES), chans)
    for x in range(2):
        for p in range(tokens // per):
            tiles = [
                tall[
                    (x * per + b) * steps : (x * per + b + 1) * steps, p * LANES : (p + 1) * LANES
                ]
                for b in range(per)
            ]
            for own in range(per):
                parts = [
                    pltpu.roll(tile, (b - own) % per * chans, 1) if b != own else tile
                    for b, tile in enumerate(tiles)
                ]
                wide_f[x, :, p * per + own, :] = pick(parts, group)
    left = wide_f[0].reshape(steps * tokens, LANES)
    left_ref[...] = left.astype(BF16)
    send_ref[2 * rows : 2 * rows + steps * tokens, :] = (
        wide_f[1].reshape(steps * tokens, LANES).astype(BF16)
    )
    spread_f[...] = dot(left.T.astype(BF16), by_col_ref[...])
    for p, tile in enumerate(fold(spread_f, seqs, chans, tokens)):
        send_ref[rows + p * seqs : rows + (p + 1) * seqs, :] = (tile * (1.0 / seqs)).astype(BF16)


def pair_kernel(
    right_ref, left_ref, unit_ref, by_row_ref, final_ref, cot_cols_ref, bias_ref,
    update_ref, own_ref, m1, m2, m3,
    outer_ref, update_f, slope_f, spread_f, both_f,
    *, chans, rows_axis, cols_axis,
):
    per, steps = LANES // chans, chans // (LANES // chans)
    tokens = update_ref.shape[0]
    groups = tokens // per
    seqs = both_f.shape[2]
    rows = groups * seqs
    quarter = seqs // cols_axis
    share = slope_f.shape[0] // (rows_axis * cols_axis)
    mine = lax.axis_index("cols")
    group = lane_group((seqs, LANES), chans)
    left = left_ref[...]
    for p in range(groups):
        tile = right_ref[p * seqs : (p + 1) * seqs, :].astype(F32)
        rolled = [pltpu.roll(tile, s * chans, 1) if s else tile for s in range(per)]
        for own in range(per):
            j = p * per + own
            blocks = jnp.concatenate(
                [jnp.where(group == b, rolled[(b - own) % per], 0.0) for b in range(per)], axis=0
            ).astype(BF16)
            got = (dot(left, blocks) * (1.0 / seqs)).astype(BF16)
            for a in range(steps):
                outer_ref[j * tokens : (j + 1) * tokens, a * LANES : (a + 1) * LANES] = got[
                    a * tokens : (a + 1) * tokens
                ]
    outer = outer_ref[...]
    slope_f[...] = dot(outer, cot_cols_ref[...], 0, 0)
    update = dot(outer, final_ref[...]) + bias_ref[...]
    for j in range(tokens):
        update_f[:, j, :] = update[j * tokens : (j + 1) * tokens]
    update_ref[...] = update_f[...].astype(BF16)
    wide = right_ref[2 * rows : 2 * rows + steps * tokens, :].astype(F32)
    spread_f[...] = dot(wide.T.astype(BF16), by_row_ref[...])
    for p, tile in enumerate(fold(spread_f, seqs, chans, tokens)):
        both_f[p, 0] = tile * (1.0 / seqs)
        both_f[p, 1] = right_ref[rows + p * seqs : rows + (p + 1) * seqs, :].astype(F32)
    both = jnp.concatenate(
        [both_f[:, x].reshape(rows, LANES).astype(BF16) for x in range(2)], axis=1
    )
    width = unit_ref.shape[2]
    slopes = pick(
        [dot(unit_ref[b], both, 0, 0) for b in range(per)],
        lane_group((width, 2 * LANES), chans) % per,
    )
    sides = [slopes[:, x * LANES : (x + 1) * LANES] for x in range(2)]
    sides = [s + pltpu.roll(s, LANES // 2, 1) for s in sides]
    slopes = jnp.where(lane_group((width, LANES), LANES // 2) == 0, sides[0], sides[1])
    for k, ref in enumerate((own_ref, m1, m2, m3)):
        peer = mine ^ k
        kind = ref.dtype
        for r in range(rows_axis):
            at = pl.multiple_of((r * cols_axis + peer) * share, share)
            ref[r * share : (r + 1) * share, :] = slope_f[pl.ds(at, share), :].astype(kind)
        base = rows_axis * share
        at = pl.multiple_of(peer * quarter, quarter)
        span = 2 * quarter
        for p in range(groups):
            ref[base + p * span : base + (p + 1) * span, :] = (
                both_f[p, :, pl.ds(at, quarter), :].reshape(span, LANES).astype(kind)
            )
        base += groups * span
        ref[base : base + width, :] = slopes.astype(kind)


def between_kernel(own_ref, r1, r2, r3, back_ref, next_ref, m1, m2, m3, total_f, *, rows_axis, share):
    total_f[...] = (
        own_ref[...] + r1[...].astype(F32) + r2[...].astype(F32) + r3[...].astype(F32)
    )
    mine = lax.axis_index("rows")
    first = rows_axis * share
    last = first + back_ref.shape[0]
    back_ref[...] = total_f[first:last, :]
    slopes = total_f[last:, :]
    for k, ref in enumerate((next_ref, m1, m2, m3)):
        at = pl.multiple_of((mine ^ k) * share, share)
        ref[0:share, :] = total_f[pl.ds(at, share), :].astype(ref.dtype)
        ref[share:, :] = slopes.astype(ref.dtype)


def back_kernel(back_ref, x_ref, gain_ref, first_ref, second_ref, out_ref, unit_f):
    tokens, quarter, width = x_ref.shape
    chans = first_ref.shape[0]
    per = LANES // chans
    groups = tokens // per
    back = back_ref[...].reshape(groups, 2, quarter, LANES)
    wide = jnp.concatenate([back[:, x].reshape(groups * quarter, LANES) for x in range(2)], axis=1)
    high = wide.astype(BF16)
    low = (wide - high.astype(F32)).astype(BF16)
    first, second = first_ref[...], second_ref[...]
    for b in range(per):
        weights = padded_projectors(first, second, b, per)
        got = dot(high, weights) + dot(low, weights)
        for p in range(groups):
            unit_f[p * per + b] = got[p * quarter : (p + 1) * quarter]
    xhat, spread = normalise(x_ref[...].reshape(tokens * quarter, width))
    g = unit_f[...].reshape(tokens * quarter, width) * gain_ref[...]
    out = spread * (
        g
        - jnp.mean(g, axis=-1, keepdims=True)
        - xhat * jnp.mean(g * xhat, axis=-1, keepdims=True)
    )
    out_ref[...] = out.reshape(tokens, quarter, width)


def last_kernel(own_ref, r1, r2, r3, final_ref, first_ref, second_ref):
    total = own_ref[...] + r1[...].astype(F32) + r2[...].astype(F32) + r3[...].astype(F32)
    share = final_ref.shape[0]
    final_ref[...] = total[:share]
    slopes = total[share:].T
    chans = first_ref.shape[0]
    for x, ref in enumerate((first_ref, second_ref)):
        side = slopes[x * LANES // 2 : (x + 1) * LANES // 2]
        out = side[:chans]
        for b in range(1, LANES // 2 // chans):
            out = out + side[b * chans : (b + 1) * chans]
        ref[...] = out


def exchange(messages, axis):
    size = lax.axis_size(axis)
    return [
        lax.ppermute(m, axis, [(p, p ^ k) for p in range(size)])
        for k, m in enumerate(messages, 1)
    ]


def local_square(
    alignment_features,
    affine_factor,
    affine_offset,
    first_projector,
    second_projector,
    final_projector,
    additive_term,
    adjoint_update,
):
    rows, cols = lax.axis_size("rows"), lax.axis_size("cols")
    tokens, quarter, width = alignment_features.shape
    chans = first_projector.shape[1]
    total, pair_ch = final_projector.shape
    seqs = quarter * cols
    per, steps = LANES // chans, chans // (LANES // chans)
    share = total // (rows * cols)
    flip = [(r * cols + q, q * cols + r) for r in range(rows) for q in range(cols)]
    shape = jax.ShapeDtypeStruct
    gain = affine_factor.reshape(1, width)
    offset = affine_offset.reshape(1, width)
    first, second = first_projector.T, second_projector.T
    wide = tokens * LANES
    tall = steps * tokens
    packed = tokens // per * seqs
    unit = call(norm_kernel, shape((tokens * quarter // 2, 2 * width), BF16))(
        alignment_features, gain, offset
    )
    units = [unit] + exchange([unit] * (cols - 1), "cols")
    by_col, by_row, cot_cols = call(
        functools.partial(grad_kernel, chans=chans),
        (
            shape((tall, wide), BF16),
            shape((tall, wide), BF16),
            shape((tokens * tokens, pair_ch), BF16),
        ),
        [pltpu.VMEM(adjoint_update.shape, F32), pltpu.VMEM((total, pair_ch), F32)],
        flops=8 * tokens * tokens * total * pair_ch,
    )(adjoint_update, final_projector)
    send, left, unit_rows = call(
        project_kernel,
        (
            shape((2 * packed + tall, LANES), BF16),
            shape((tall, LANES), BF16),
            shape((per, packed, width), BF16),
        ),
        [
            pltpu.VMEM((tokens, seqs, width), F32),
            pltpu.VMEM((2, chans, width), F32),
            pltpu.VMEM((2, steps, tokens, LANES), F32),
            pltpu.VMEM((LANES, wide), F32),
        ],
    )(*units, first, second, by_col)
    right = lax.ppermute(send, ("rows", "cols"), flip)
    message = rows * share + 2 * quarter * tokens // per + width
    update, own, *messages = call(
        functools.partial(pair_kernel, chans=chans, rows_axis=rows, cols_axis=cols),
        (
            shape((tokens, tokens, pair_ch), BF16),
            shape((message, LANES), F32),
            *[shape((message, LANES), BF16)] * (cols - 1),
        ),
        [
            pltpu.VMEM((tokens * tokens, total), BF16),
            pltpu.VMEM((tokens, tokens, pair_ch), F32),
            pltpu.VMEM((total, pair_ch), F32),
            pltpu.VMEM((LANES, wide), F32),
            pltpu.VMEM((tokens // per, 2, seqs, LANES), F32),
        ],
    )(right, left, unit_rows, by_row, final_projector, cot_cols, additive_term.reshape(1, pair_ch))
    got = exchange(messages, "cols")
    back, own, *messages = call(
        functools.partial(between_kernel, rows_axis=rows, share=share),
        (
            shape((2 * quarter * tokens // per, LANES), F32),
            shape((share + width, LANES), F32),
            *[shape((share + width, LANES), BF16)] * (rows - 1),
        ),
        [pltpu.VMEM((message, LANES), F32)],
    )(own, *got)
    got = exchange(messages, "rows")
    alignment_slope = call(
        back_kernel,
        shape((tokens, quarter, width), F32),
        [pltpu.VMEM((tokens, quarter, width), F32)],
        flops=10**8,
    )(back, alignment_features, gain, first, second)
    final_slope, first_slope, second_slope = call(
        last_kernel,
        (shape((share, pair_ch), F32), shape((chans, width), F32), shape((chans, width), F32)),
    )(own, *got)
    return update, alignment_slope, final_slope, first_slope.T, second_slope.T


def fits(mesh, alignment_features, first_projector, final_projector):
    rows, cols = mesh.shape["rows"], mesh.shape["cols"]
    tokens = alignment_features.shape[0] // (mesh.shape["groups"] * rows)
    quarter = alignment_features.shape[1] // cols
    width, chans = first_projector.shape
    per = LANES // chans
    return (
        rows == cols == 4
        and chans * per == LANES
        and chans % per == 0
        and chans // per == SUBLANES
        and 2 * width == LANES
        and final_projector.shape[1] == LANES
        and quarter == SUBLANES
        and tokens % (2 * SUBLANES) == 0
        and quarter * cols == chans
        and chans // per * tokens == LANES
    )


def solution(mesh):
    in_specs = (
        P(("groups", "rows"), "cols", None),
        P(),
        P(),
        P(),
        P(),
        P(),
        P(),
        P(("groups", "rows"), "cols", None),
    )
    out_specs = (
        P(("groups", "rows"), "cols", None),
        P(("groups", "rows"), "cols", None),
        P(("groups", "rows", "cols"), None),
        P("groups", None),
        P("groups", None),
    )

    def whole(*args):
        square = fits(mesh, args[0], args[3], args[5])
        return jax.shard_map(
            local_square if square else local_general,
            mesh=mesh,
            in_specs=in_specs,
            out_specs=out_specs,
            check_vma=False,
        )(*args)

    return whole
```

```python
import functools

import jax
import jax.numpy as jnp
from jax import lax
from jax.experimental import pallas as pl
from jax.experimental.pallas import tpu as pltpu
from jax.sharding import PartitionSpec as P


def layernorm_parts(alignment_features, affine_factor, affine_offset):
    centered_alignment = alignment_features - jnp.mean(alignment_features, axis=-1, keepdims=True)
    reciprocal_spread = lax.rsqrt(
        jnp.mean(centered_alignment * centered_alignment, axis=-1, keepdims=True) + 1e-05
    )
    zscored_alignment = centered_alignment * reciprocal_spread
    return (
        zscored_alignment,
        reciprocal_spread,
        (zscored_alignment * affine_factor + affine_offset).astype(jnp.bfloat16),
    )


def local_general(
    alignment_features,
    affine_factor,
    affine_offset,
    first_projector,
    second_projector,
    final_projector,
    additive_term,
    adjoint_update,
):
    zscored_alignment, reciprocal_spread, unit_alignment = layernorm_parts(
        alignment_features, affine_factor, affine_offset
    )
    first_factor_here = jnp.dot(
        unit_alignment, first_projector, preferred_element_type=jnp.float32
    ).astype(jnp.bfloat16)
    second_factor_here = jnp.dot(
        unit_alignment, second_projector, preferred_element_type=jnp.float32
    ).astype(jnp.bfloat16)
    tokens, quarter, chans = first_factor_here.shape
    left_flat = first_factor_here.reshape(tokens, quarter * chans)
    right_flat = second_factor_here.reshape(tokens, quarter * chans)
    left_wide, right_wide = (
        lax.all_gather(left_flat, "cols", axis=1, tiled=True),
        lax.all_gather(right_flat, "cols", axis=1, tiled=True),
    )
    left_rows = left_wide.reshape(tokens, -1, chans)
    right_all = lax.all_gather(right_wide, "rows", axis=0, tiled=True)
    block = right_all.shape[0] // lax.axis_size("cols")
    right_cols = lax.dynamic_slice_in_dim(
        right_all, lax.axis_index("cols") * block, block, 0
    ).reshape(block, -1, chans)
    seqs = left_rows.shape[1]
    multiplier = 1.0 / seqs
    pair_ch = adjoint_update.shape[2]
    step_rows = 4
    rounds = tokens // step_rows
    first_tile_list = left_rows.reshape(rounds, step_rows, seqs, chans)
    cot_blocks = adjoint_update.reshape(rounds, step_rows, block, pair_ch)

    def advance(carry, inputs):
        right_acc, out_acc = carry
        left_slab, cot_slab = inputs
        outer = (
            jnp.einsum("isc,jsd->ijcd", left_slab, right_cols, preferred_element_type=jnp.float32)
            * multiplier
        ).astype(jnp.bfloat16)
        flat = outer.reshape(step_rows * block, chans * chans)
        cot_flat = cot_slab.reshape(step_rows * block, pair_ch)
        update = (
            jnp.dot(flat, final_projector, preferred_element_type=jnp.float32) + additive_term
        ).astype(jnp.bfloat16)
        outer_grad = jnp.dot(
            cot_flat, final_projector.T, preferred_element_type=jnp.float32
        ).astype(jnp.bfloat16)
        outer_grad = outer_grad.reshape(step_rows, block, chans, chans)
        left_piece = (
            jnp.einsum("ijcd,jsd->isc", outer_grad, right_cols, preferred_element_type=jnp.float32)
            * multiplier
        )
        right_acc = (
            right_acc
            + jnp.einsum("ijcd,isc->jsd", outer_grad, left_slab, preferred_element_type=jnp.float32)
            * multiplier
        )
        out_acc = out_acc + jnp.einsum(
            "fk,fe->ke", flat, cot_flat, preferred_element_type=jnp.float32
        )
        return ((right_acc, out_acc), (update.reshape(step_rows, block, pair_ch), left_piece))

    beginning_position = (
        jnp.zeros((block, seqs, chans), jnp.float32),
        jnp.zeros((chans * chans, pair_ch), jnp.float32),
    )
    (right_part, out_term), (updates, left_pieces) = lax.scan(
        advance, beginning_position, (first_tile_list, cot_blocks)
    )
    residue_update = updates.reshape(tokens, block, pair_ch)
    left_part = left_pieces.reshape(tokens, seqs * chans)
    first_adjoint = lax.psum_scatter(left_part, "cols", scatter_dimension=1, tiled=True).reshape(
        tokens, quarter, chans
    )
    moved = lax.all_to_all(
        right_part.reshape(block, seqs * chans), "cols", split_axis=1, concat_axis=0, tiled=True
    )
    right_back = lax.psum_scatter(moved, "rows", scatter_dimension=0, tiled=True).reshape(
        tokens, quarter, chans
    )
    final_projector_slope = lax.psum_scatter(
        out_term, ("rows", "cols"), scatter_dimension=0, tiled=True
    )
    unit_broadcast = unit_alignment.astype(jnp.float32)
    high = lax.Precision.HIGHEST
    left_term = jnp.einsum("tsk,tsc->kc", unit_broadcast, first_adjoint, precision=high)
    right_term = jnp.einsum("tsk,tsc->kc", unit_broadcast, right_back, precision=high)
    first_projector_slope, second_projector_slope = lax.psum(
        (left_term, right_term), ("rows", "cols")
    )
    unit_adjoint = jnp.einsum(
        "tsc,kc->tsk", first_adjoint, first_projector.astype(jnp.float32), precision=high
    )
    unit_adjoint = unit_adjoint + jnp.einsum(
        "tsc,kc->tsk", right_back, second_projector.astype(jnp.float32), precision=high
    )
    scaled_alignment = unit_adjoint * affine_factor
    alignment_slope = reciprocal_spread * (
        scaled_alignment
        - jnp.mean(scaled_alignment, axis=-1, keepdims=True)
        - zscored_alignment * jnp.mean(scaled_alignment * zscored_alignment, axis=-1, keepdims=True)
    )
    return (
        residue_update,
        alignment_slope,
        final_projector_slope,
        first_projector_slope,
        second_projector_slope,
    )


F32, BF16 = jnp.float32, jnp.bfloat16
LANES, SUBLANES = 128, 8


def dot(a, b, at=1, bt=0):
    return lax.dot_general(a, b, (((at,), (bt,)), ((), ())), preferred_element_type=F32)


def lane_group(shape, size):
    return lax.broadcasted_iota(jnp.int32, shape, len(shape) - 1) // size


def pick(parts, group):
    out = parts[-1]
    for b in range(len(parts) - 2, -1, -1):
        out = jnp.where(group == b, parts[b], out)
    return out


def normalise(x):
    centered = x - jnp.mean(x, axis=-1, keepdims=True)
    spread = lax.rsqrt(jnp.mean(centered * centered, axis=-1, keepdims=True) + 1e-05)
    return centered * spread, spread


def call(kernel, out_shape, scratch=(), flops=0, space=pltpu.VMEM):
    place = pl.BlockSpec(memory_space=space)
    on_chip = pl.BlockSpec(memory_space=pltpu.VMEM)

    def run(*args):
        return pl.pallas_call(
            kernel,
            out_shape=out_shape,
            in_specs=[place] * len(args),
            out_specs=jax.tree.map(lambda _: on_chip, out_shape),
            scratch_shapes=list(scratch),
            cost_estimate=pl.CostEstimate(flops=flops, bytes_accessed=0, transcendentals=0),
            compiler_params=pltpu.CompilerParams(vmem_limit_bytes=16 * 2**20),
        )(*args)

    return run


def norm_kernel(*refs):
    x_ref, offset_ref, sems = refs[-3:]
    count = sems.shape[0]
    sources, (out_ref, xhat_ref, spread_ref) = refs[:count], refs[count : count + 3]
    kept = (x_ref, offset_ref) + refs[count + 3 : -3]
    copies = [
        pltpu.make_async_copy(source, ref, sems.at[n])
        for n, (source, ref) in enumerate(zip(sources, kept))
    ]
    for copy in copies:
        copy.start()
    for copy in copies[:3]:
        copy.wait()
    tokens, quarter, width = x_ref.shape
    xhat, spread = normalise(x_ref[...].reshape(tokens * quarter, width))
    xhat_ref[...] = xhat
    spread_ref[...] = jnp.broadcast_to(spread, xhat.shape)
    unit = xhat * kept[2][...] + offset_ref[...]
    half = tokens * quarter // 2
    out_ref[...] = jnp.concatenate([unit[:half], unit[half:]], axis=1).astype(BF16)
    for copy in copies[3:]:
        copy.wait()


def grad_kernel(
    cot_ref, final_ref, first_ref, second_ref,
    by_col_ref, by_row_ref, cot_cols_ref, weight_ref, order_ref,
    cot_f, final_f,
    *, chans,
):
    tokens, block, _ = cot_ref.shape
    steps = by_col_ref.shape[0] // tokens
    per = LANES // chans
    cot = cot_ref[...]
    final = final_ref[...]
    cot_f[...] = cot.astype(F32)
    final_f[...] = final.astype(F32)
    for j in range(block):
        cot_cols_ref[j * tokens : (j + 1) * tokens, :] = cot_f[:, j, :].astype(BF16)
    cot_cols = cot_cols_ref[...]
    cot_rows = cot.reshape(tokens * block, cot.shape[2])
    for a in range(steps):
        got = dot(cot_cols, final[a * LANES : (a + 1) * LANES], 1, 1).astype(BF16)
        for j in range(block):
            by_col_ref[a * tokens : (a + 1) * tokens, j * LANES : (j + 1) * LANES] = got[
                j * tokens : (j + 1) * tokens
            ]
        lanes_dc = jnp.concatenate(
            [final_f[pl.ds(a * per + b, chans, stride=chans), :] for b in range(per)], axis=0
        ).astype(BF16)
        got = dot(cot_rows, lanes_dc, 1, 1).astype(BF16)
        for i in range(tokens):
            by_row_ref[a * block : (a + 1) * block, i * LANES : (i + 1) * LANES] = got[
                i * block : (i + 1) * block
            ]
    for x, ref in enumerate((first_ref, second_ref)):
        projector = ref[...]
        zero = jnp.zeros_like(projector)
        halves = [
            jnp.concatenate([projector, zero], axis=1),
            jnp.concatenate([zero, projector], axis=1),
        ]
        empty = jnp.concatenate([zero, zero], axis=1)
        for b in range(per):
            for h in range(2):
                for other in range(per):
                    at = (((x * 2) + h) * per + other) * chans
                    weight_ref[b, at : at + chans, :] = halves[h] if other == b else empty
    size = tokens * chans
    for b in range(per):
        row = lax.broadcasted_iota(jnp.int32, (size, LANES), 0)
        lane = lax.broadcasted_iota(jnp.int32, (size, LANES), 1)
        wanted = lane % tokens * chans + lane // tokens * per + b
        order_ref[:, b * LANES : (b + 1) * LANES] = jnp.where(row == wanted, 1.0, 0.0).astype(BF16)


def joint_kernel(n0, n1, n2, n3, out_ref, unit_f):
    blocks = (n0, n1, n2, n3)
    mine = lax.axis_index("cols")
    half, seqs, lanes = unit_f.shape
    quarter = seqs // len(blocks)
    for k, ref in enumerate(blocks):
        at = pl.multiple_of((mine ^ k) * quarter, quarter)
        unit_f[:, pl.ds(at, quarter), :] = ref[...].astype(F32).reshape(half, quarter, lanes)
    out_ref[...] = unit_f[...].reshape(half * seqs, lanes).astype(BF16)


def project(unit, weight_ref, x, seqs, per):
    half = unit.shape[0] // seqs
    by_group = unit.reshape(half // per, per, seqs, unit.shape[1])
    size = weight_ref.shape[1] // 2
    total = None
    for b in range(per):
        part = by_group[:, b].reshape(half // per * seqs, unit.shape[1])
        got = dot(part, weight_ref[b, x * size : (x + 1) * size, :], 1, 1)
        total = got if total is None else total + got
    total = total.astype(BF16)
    count = half // per
    return [
        total[p % count * seqs : (p % count + 1) * seqs, p // count * LANES : (p // count + 1) * LANES]
        for p in range(2 * count)
    ]


def reorder(tiles, order_ref):
    wide = dot(jnp.concatenate(tiles, axis=1), order_ref[...])
    count = wide.shape[1] // LANES
    return jnp.concatenate([wide[:, b * LANES : (b + 1) * LANES] for b in range(count)], axis=0)


def fold(spread_ref, seqs, chans, tokens):
    per = LANES // chans
    group = lane_group((seqs, LANES), chans)
    out = []
    for p in range(tokens // per):
        total = None
        for shift in range(per):
            parts = []
            for b in range(per):
                t = p * per + (b + shift) % per
                parts.append(spread_ref[b * seqs : (b + 1) * seqs, t * LANES : (t + 1) * LANES])
            part = pick(parts, group)
            if shift:
                part = pltpu.roll(part, shift * chans, 1)
            total = part if total is None else total + part
        out.append(total)
    return out


def slope(unit_turned, tiles, per, chans):
    seqs = tiles[0].shape[0]
    count = len(tiles) // 2
    group = lane_group((seqs, LANES), chans)
    rows = []
    for p in range(count):
        for b in range(per):
            rows.append(
                jnp.concatenate(
                    [jnp.where(group == b, tiles[h * count + p], 0.0) for h in range(2)], axis=1
                )
            )
    got = dot(unit_turned, jnp.concatenate(rows, axis=0).astype(BF16))
    width = unit_turned.shape[0] // 2
    return got[:width, :LANES] + got[width:, LANES:]


def left_kernel(
    unit_ref, weight_ref, order_ref, by_col_ref, left_ref, turned_ref, part_ref, spread_f, *, chans, seqs
):
    per = LANES // chans
    tokens = unit_ref.shape[0] // seqs * 2
    unit = unit_ref[...]
    turned_ref[...] = unit.astype(F32).T.astype(BF16)
    turned = reorder(project(unit, weight_ref, 0, seqs, per), order_ref)
    left_ref[...] = turned.T.astype(BF16)
    spread_f[...] = dot(turned.astype(BF16), by_col_ref[...])
    for p, tile in enumerate(fold(spread_f, seqs, chans, tokens)):
        part_ref[p] = tile * (1.0 / seqs)


def pair_kernel(
    unit_ref, left_ref, turned_ref, part_ref, weight_ref, order_ref, by_row_ref, cot_cols_ref,
    outer_ref, own_ref, m1, m2, m3,
    block_ref, slope_f, spread_f, both_f,
    *, chans, seqs, sizes,
):
    per, steps = LANES // chans, chans // (LANES // chans)
    rows, cols = sizes
    tokens = unit_ref.shape[0] // seqs * 2
    groups = tokens // per
    quarter = seqs // cols
    share = slope_f.shape[0] // (rows * cols)
    mine = lax.axis_index("cols")
    group = lane_group((seqs, LANES), chans)
    unit = unit_ref[...]
    right = project(unit, weight_ref, 1, seqs, per)
    for p, tile in enumerate(right):
        tile = tile.astype(F32)
        rolled = [pltpu.roll(tile, s * chans, 1) if s else tile for s in range(per)]
        for own in range(per):
            j = p * per + own
            for b in range(per):
                block_ref[b * seqs : (b + 1) * seqs, j * LANES : (j + 1) * LANES] = jnp.where(
                    group == b, rolled[(b - own) % per], 0.0
                ).astype(BF16)
    left = left_ref[...]
    for p in range(groups):
        span = per * LANES
        got = dot(left, block_ref[:, p * span : (p + 1) * span])
        got = (got * (1.0 / seqs)).astype(BF16)
        for own in range(per):
            j = p * per + own
            for a in range(steps):
                outer_ref[j * tokens : (j + 1) * tokens, a * LANES : (a + 1) * LANES] = got[
                    a * tokens : (a + 1) * tokens, own * LANES : (own + 1) * LANES
                ]
    spread_f[...] = dot(reorder(right, order_ref).astype(BF16), by_row_ref[...])
    slope_f[...] = dot(outer_ref[...], cot_cols_ref[...], 0, 0)
    lefts = [tile * (1.0 / seqs) for tile in fold(spread_f, seqs, chans, tokens)]
    rights = [part_ref[p] for p in range(groups)]
    for p in range(groups):
        both_f[p, 0] = lefts[p]
        both_f[p, 1] = rights[p]
    sides = [
        slope(turned_ref[...], lefts, per, chans),
        slope(unit.astype(F32).T.astype(BF16), rights, per, chans),
    ]
    width = sides[0].shape[0]
    sides = [s + pltpu.roll(s, LANES // 2, 1) for s in sides]
    slopes = jnp.where(lane_group((width, LANES), LANES // 2) == 0, sides[0], sides[1])
    for k, ref in enumerate((own_ref, m1, m2, m3)):
        peer = mine ^ k
        kind = ref.dtype
        for r in range(rows):
            at = pl.multiple_of((r * cols + peer) * share, share)
            ref[r * share : (r + 1) * share, :] = slope_f[pl.ds(at, share), :].astype(kind)
        base = rows * share
        at = pl.multiple_of(peer * quarter, quarter)
        span = groups * quarter
        for x in range(2):
            ref[base + x * span : base + (x + 1) * span, :] = (
                both_f[:, x, pl.ds(at, quarter), :].reshape(span, LANES).astype(kind)
            )
        base += 2 * span
        ref[base : base + width, :] = slopes.astype(kind)


def update_kernel(outer_ref, final_ref, bias_ref, update_ref, update_f):
    tokens = update_ref.shape[0]
    update = dot(outer_ref[...], final_ref[...]) + bias_ref[...]
    for j in range(update_ref.shape[1]):
        update_f[:, j, :] = update[j * tokens : (j + 1) * tokens]
    update_ref[...] = update_f[...].astype(BF16)


def between_kernel(
    own_ref, r1, r2, r3, left_ref, next_ref, m1, m2, m3, total_f, right_f, *, rows, share
):
    refs = (own_ref, r1, r2, r3)
    span = left_ref.shape[0]
    first = rows * share
    last = first + 2 * span
    mine, column = lax.axis_index("rows"), lax.axis_index("cols")
    for k, ref in enumerate(refs):
        right_f[column ^ k] = ref[first + span : last, :].astype(F32)
    for start, stop in ((0, first + span), (last, total_f.shape[0])):
        total = own_ref[start:stop, :]
        for ref in refs[1:]:
            total = total + ref[start:stop, :].astype(F32)
        total_f[start:stop, :] = total
    left_ref[...] = total_f[first : first + span, :]
    slopes = total_f[last:, :]
    for k, ref in enumerate((next_ref, m1, m2, m3)):
        peer = mine ^ k
        at = pl.multiple_of(peer * share, share)
        ref[0:share, :] = total_f[pl.ds(at, share), :].astype(ref.dtype)
        ref[share : share + span, :] = right_f[peer].astype(ref.dtype)
        ref[share + span :, :] = slopes.astype(ref.dtype)


def to_unit(back, projector_ref, unit_ref, quarter):
    back = back[...]
    projector = projector_ref[...]
    chans = projector.shape[0]
    high = back.astype(BF16)
    low = (back - high.astype(F32)).astype(BF16)
    zero = jnp.zeros_like(projector)
    per = LANES // chans
    for b in range(per):
        weights = jnp.concatenate([projector if i == b else zero for i in range(per)], axis=0)
        got = dot(high, weights) + dot(low, weights)
        for p in range(back.shape[0] // quarter):
            unit_ref[p * per + b] = got[p * quarter : (p + 1) * quarter]


def last_kernel(
    own_ref, r1, r2, r3, unit_ref, xhat_ref, spread_ref, gain_ref, second_ref,
    final_ref, first_slope_ref, second_slope_ref, out_ref, unit_f,
):
    total = own_ref[...] + r1[...].astype(F32) + r2[...].astype(F32) + r3[...].astype(F32)
    share = final_ref.shape[0]
    final_ref[...] = total[:share]
    tokens, quarter, width = out_ref.shape
    span = tokens * quarter * second_ref.shape[0] // LANES
    to_unit(total[share : share + span], second_ref, unit_f, quarter)
    g = (unit_ref[...] + unit_f[...]).reshape(tokens * quarter, width) * gain_ref[...]
    xhat = xhat_ref[...]
    out = spread_ref[...] * (
        g
        - jnp.mean(g, axis=-1, keepdims=True)
        - xhat * jnp.mean(g * xhat, axis=-1, keepdims=True)
    )
    out_ref[...] = out.reshape(tokens, quarter, width)
    slopes = total[share + span :].T
    chans = second_ref.shape[0]
    for x, ref in enumerate((first_slope_ref, second_slope_ref)):
        side = slopes[x * LANES // 2 : (x + 1) * LANES // 2]
        out = side[:chans]
        for b in range(1, LANES // 2 // chans):
            out = out + side[b * chans : (b + 1) * chans]
        ref[...] = out


def exchange(messages, axis):
    size = lax.axis_size(axis)
    return [
        lax.ppermute(m, axis, [(p, p ^ k) for p in range(size)])
        for k, m in enumerate(messages, 1)
    ]


def local_square(
    alignment_features,
    affine_factor,
    affine_offset,
    first_projector,
    second_projector,
    final_projector,
    additive_term,
    adjoint_update,
):
    rows, cols = lax.axis_size("rows"), lax.axis_size("cols")
    tokens, quarter, width = alignment_features.shape
    chans = first_projector.shape[1]
    total, pair_ch = final_projector.shape
    seqs = quarter * cols
    per, steps = LANES // chans, chans // (LANES // chans)
    share = total // (rows * cols)
    flip = [(r * cols + q, q * cols + r) for r in range(rows) for q in range(cols)]
    shape = jax.ShapeDtypeStruct
    wide, tall = tokens * LANES, steps * tokens
    groups = tokens // per
    half = tokens // 2
    aligned = shape((tokens, quarter, width), F32)
    flat = shape((tokens * quarter, width), F32)
    inputs = [
        alignment_features,
        affine_offset.reshape(1, width),
        affine_factor.reshape(1, width),
        adjoint_update,
        final_projector,
        first_projector.T,
        second_projector.T,
        additive_term.reshape(1, pair_ch),
    ]
    unit, xhat, spread, gain, cot, final, first, second, bias = call(
        norm_kernel,
        [shape((half * quarter, 2 * width), BF16), flat, flat]
        + [shape(i.shape, i.dtype) for i in inputs[2:]],
        [pltpu.VMEM(i.shape, i.dtype) for i in inputs[:2]]
        + [pltpu.SemaphoreType.DMA((len(inputs),))],
        space=pltpu.HBM,
    )(*[pltpu.with_memory_space_constraint(i, pltpu.HBM) for i in inputs])
    units = [unit] + exchange([unit] * (cols - 1), "cols")
    by_col, by_row, cot_cols, weight, order = call(
        functools.partial(grad_kernel, chans=chans),
        (
            shape((tall, wide), BF16),
            shape((tall, wide), BF16),
            shape((tokens * tokens, pair_ch), BF16),
            shape((per, 4 * LANES, 2 * width), BF16),
            shape((tokens * chans, per * LANES), BF16),
        ),
        [pltpu.VMEM(adjoint_update.shape, F32), pltpu.VMEM((total, pair_ch), F32)],
        flops=8 * tokens * tokens * total * pair_ch,
    )(cot, final, first, second)
    unit_rows = call(
        joint_kernel,
        shape((half * seqs, 2 * width), BF16),
        [pltpu.VMEM((half, seqs, 2 * width), F32)],
    )(*units)
    unit_cols = lax.ppermute(unit_rows, ("rows", "cols"), flip)
    left, turned, part = call(
        functools.partial(left_kernel, chans=chans, seqs=seqs),
        (
            shape((tall, LANES), BF16),
            shape((2 * width, half * seqs), BF16),
            shape((groups, seqs, LANES), F32),
        ),
        [pltpu.VMEM((LANES, wide), F32)],
        flops=10**8,
    )(unit_rows, weight, order, by_col)
    span = groups * quarter
    message = rows * share + 2 * span + width
    outer, own, *messages = call(
        functools.partial(pair_kernel, chans=chans, seqs=seqs, sizes=(rows, cols)),
        (
            shape((tokens * tokens, total), BF16),
            shape((message, LANES), F32),
            *[shape((message, LANES), BF16)] * (cols - 1),
        ),
        [
            pltpu.VMEM((LANES, wide), BF16),
            pltpu.VMEM((total, pair_ch), F32),
            pltpu.VMEM((LANES, wide), F32),
            pltpu.VMEM((groups, 2, seqs, LANES), F32),
        ],
    )(unit_cols, left, turned, part, weight, order, by_row, cot_cols)
    got = exchange(messages, "cols")
    update = call(
        update_kernel,
        shape((tokens, tokens, pair_ch), BF16),
        [pltpu.VMEM((tokens, tokens, pair_ch), F32)],
        flops=10**8,
    )(outer, final, bias)
    message = share + span + width
    back, own, *messages = call(
        functools.partial(between_kernel, rows=rows, share=share),
        (
            shape((span, LANES), F32),
            shape((message, LANES), F32),
            *[shape((message, LANES), BF16)] * (rows - 1),
        ),
        [
            pltpu.VMEM((rows * share + 2 * span + width, LANES), F32),
            pltpu.VMEM((cols, span, LANES), F32),
        ],
    )(own, *got)
    got = exchange(messages, "rows")
    from_left = call(functools.partial(to_unit, quarter=quarter), aligned, flops=10**8)(back, first)
    final_slope, first_slope, second_slope, alignment_slope = call(
        last_kernel,
        (
            shape((share, pair_ch), F32),
            shape((chans, width), F32),
            shape((chans, width), F32),
            aligned,
        ),
        [pltpu.VMEM((tokens, quarter, width), F32)],
    )(own, *got, from_left, xhat, spread, gain, second)
    return update, alignment_slope, final_slope, first_slope.T, second_slope.T


def fits(mesh, alignment_features, first_projector, final_projector):
    rows, cols = mesh.shape["rows"], mesh.shape["cols"]
    tokens = alignment_features.shape[0] // (mesh.shape["groups"] * rows)
    quarter = alignment_features.shape[1] // cols
    width, chans = first_projector.shape
    per = LANES // chans
    return (
        rows == cols == 4
        and chans * per == LANES
        and chans % per == 0
        and chans // per == SUBLANES
        and 2 * width == LANES
        and final_projector.shape[1] == LANES
        and quarter == SUBLANES
        and tokens % (2 * SUBLANES) == 0
        and quarter * cols == chans
        and chans // per * tokens == LANES
    )


def solution(mesh):
    in_specs = (
        P(("groups", "rows"), "cols", None),
        P(),
        P(),
        P(),
        P(),
        P(),
        P(),
        P(("groups", "rows"), "cols", None),
    )
    out_specs = (
        P(("groups", "rows"), "cols", None),
        P(("groups", "rows"), "cols", None),
        P(("groups", "rows", "cols"), None),
        P("groups", None),
        P("groups", None),
    )

    def whole(*args):
        square = fits(mesh, args[0], args[3], args[5])
        return jax.shard_map(
            local_square if square else local_general,
            mesh=mesh,
            in_specs=in_specs,
            out_specs=out_specs,
            check_vma=False,
        )(*args)

    return whole
```

```python
import functools

import jax
import jax.numpy as jnp
from jax import lax
from jax.experimental import pallas as pl
from jax.experimental.pallas import tpu as pltpu
from jax.sharding import PartitionSpec as P


def layernorm_parts(alignment_features, affine_factor, affine_offset):
    centered_alignment = alignment_features - jnp.mean(alignment_features, axis=-1, keepdims=True)
    reciprocal_spread = lax.rsqrt(
        jnp.mean(centered_alignment * centered_alignment, axis=-1, keepdims=True) + 1e-05
    )
    zscored_alignment = centered_alignment * reciprocal_spread
    return (
        zscored_alignment,
        reciprocal_spread,
        (zscored_alignment * affine_factor + affine_offset).astype(jnp.bfloat16),
    )


def local_general(
    alignment_features,
    affine_factor,
    affine_offset,
    first_projector,
    second_projector,
    final_projector,
    additive_term,
    adjoint_update,
):
    zscored_alignment, reciprocal_spread, unit_alignment = layernorm_parts(
        alignment_features, affine_factor, affine_offset
    )
    first_factor_here = jnp.dot(
        unit_alignment, first_projector, preferred_element_type=jnp.float32
    ).astype(jnp.bfloat16)
    second_factor_here = jnp.dot(
        unit_alignment, second_projector, preferred_element_type=jnp.float32
    ).astype(jnp.bfloat16)
    tokens, quarter, chans = first_factor_here.shape
    left_flat = first_factor_here.reshape(tokens, quarter * chans)
    right_flat = second_factor_here.reshape(tokens, quarter * chans)
    left_wide, right_wide = (
        lax.all_gather(left_flat, "cols", axis=1, tiled=True),
        lax.all_gather(right_flat, "cols", axis=1, tiled=True),
    )
    left_rows = left_wide.reshape(tokens, -1, chans)
    right_all = lax.all_gather(right_wide, "rows", axis=0, tiled=True)
    block = right_all.shape[0] // lax.axis_size("cols")
    right_cols = lax.dynamic_slice_in_dim(
        right_all, lax.axis_index("cols") * block, block, 0
    ).reshape(block, -1, chans)
    seqs = left_rows.shape[1]
    multiplier = 1.0 / seqs
    pair_ch = adjoint_update.shape[2]
    step_rows = 4
    rounds = tokens // step_rows
    first_tile_list = left_rows.reshape(rounds, step_rows, seqs, chans)
    cot_blocks = adjoint_update.reshape(rounds, step_rows, block, pair_ch)

    def advance(carry, inputs):
        right_acc, out_acc = carry
        left_slab, cot_slab = inputs
        outer = (
            jnp.einsum("isc,jsd->ijcd", left_slab, right_cols, preferred_element_type=jnp.float32)
            * multiplier
        ).astype(jnp.bfloat16)
        flat = outer.reshape(step_rows * block, chans * chans)
        cot_flat = cot_slab.reshape(step_rows * block, pair_ch)
        update = (
            jnp.dot(flat, final_projector, preferred_element_type=jnp.float32) + additive_term
        ).astype(jnp.bfloat16)
        outer_grad = jnp.dot(
            cot_flat, final_projector.T, preferred_element_type=jnp.float32
        ).astype(jnp.bfloat16)
        outer_grad = outer_grad.reshape(step_rows, block, chans, chans)
        left_piece = (
            jnp.einsum("ijcd,jsd->isc", outer_grad, right_cols, preferred_element_type=jnp.float32)
            * multiplier
        )
        right_acc = (
            right_acc
            + jnp.einsum("ijcd,isc->jsd", outer_grad, left_slab, preferred_element_type=jnp.float32)
            * multiplier
        )
        out_acc = out_acc + jnp.einsum(
            "fk,fe->ke", flat, cot_flat, preferred_element_type=jnp.float32
        )
        return ((right_acc, out_acc), (update.reshape(step_rows, block, pair_ch), left_piece))

    beginning_position = (
        jnp.zeros((block, seqs, chans), jnp.float32),
        jnp.zeros((chans * chans, pair_ch), jnp.float32),
    )
    (right_part, out_term), (updates, left_pieces) = lax.scan(
        advance, beginning_position, (first_tile_list, cot_blocks)
    )
    residue_update = updates.reshape(tokens, block, pair_ch)
    left_part = left_pieces.reshape(tokens, seqs * chans)
    first_adjoint = lax.psum_scatter(left_part, "cols", scatter_dimension=1, tiled=True).reshape(
        tokens, quarter, chans
    )
    moved = lax.all_to_all(
        right_part.reshape(block, seqs * chans), "cols", split_axis=1, concat_axis=0, tiled=True
    )
    right_back = lax.psum_scatter(moved, "rows", scatter_dimension=0, tiled=True).reshape(
        tokens, quarter, chans
    )
    final_projector_slope = lax.psum_scatter(
        out_term, ("rows", "cols"), scatter_dimension=0, tiled=True
    )
    unit_broadcast = unit_alignment.astype(jnp.float32)
    high = lax.Precision.HIGHEST
    left_term = jnp.einsum("tsk,tsc->kc", unit_broadcast, first_adjoint, precision=high)
    right_term = jnp.einsum("tsk,tsc->kc", unit_broadcast, right_back, precision=high)
    first_projector_slope, second_projector_slope = lax.psum(
        (left_term, right_term), ("rows", "cols")
    )
    unit_adjoint = jnp.einsum(
        "tsc,kc->tsk", first_adjoint, first_projector.astype(jnp.float32), precision=high
    )
    unit_adjoint = unit_adjoint + jnp.einsum(
        "tsc,kc->tsk", right_back, second_projector.astype(jnp.float32), precision=high
    )
    scaled_alignment = unit_adjoint * affine_factor
    alignment_slope = reciprocal_spread * (
        scaled_alignment
        - jnp.mean(scaled_alignment, axis=-1, keepdims=True)
        - zscored_alignment * jnp.mean(scaled_alignment * zscored_alignment, axis=-1, keepdims=True)
    )
    return (
        residue_update,
        alignment_slope,
        final_projector_slope,
        first_projector_slope,
        second_projector_slope,
    )


F32, BF16 = jnp.float32, jnp.bfloat16
LANES, SUBLANES = 128, 8


def dot(a, b, at=1, bt=0):
    return lax.dot_general(a, b, (((at,), (bt,)), ((), ())), preferred_element_type=F32)


def lane_group(shape, size):
    return lax.broadcasted_iota(jnp.int32, shape, len(shape) - 1) // size


def pick(parts, group):
    out = parts[-1]
    for b in range(len(parts) - 2, -1, -1):
        out = jnp.where(group == b, parts[b], out)
    return out


def normalise(x):
    centered = x - jnp.mean(x, axis=-1, keepdims=True)
    spread = lax.rsqrt(jnp.mean(centered * centered, axis=-1, keepdims=True) + 1e-05)
    return centered * spread, spread


def call(kernel, out_shape, scratch=(), flops=0, space=pltpu.VMEM):
    place = pl.BlockSpec(memory_space=space)
    on_chip = pl.BlockSpec(memory_space=pltpu.VMEM)

    def run(*args):
        return pl.pallas_call(
            kernel,
            out_shape=out_shape,
            in_specs=[place] * len(args),
            out_specs=jax.tree.map(lambda _: on_chip, out_shape),
            scratch_shapes=list(scratch),
            cost_estimate=pl.CostEstimate(flops=flops, bytes_accessed=0, transcendentals=0),
            compiler_params=pltpu.CompilerParams(vmem_limit_bytes=16 * 2**20),
        )(*args)

    return run


def norm_kernel(*refs):
    x_ref, offset_ref, sems = refs[-3:]
    count = sems.shape[0]
    sources, (out_ref, xhat_ref, spread_ref) = refs[:count], refs[count : count + 3]
    kept = (x_ref, offset_ref) + refs[count + 3 : -3]
    copies = [
        pltpu.make_async_copy(source, ref, sems.at[n])
        for n, (source, ref) in enumerate(zip(sources, kept))
    ]
    for copy in copies:
        copy.start()
    for copy in copies[:3]:
        copy.wait()
    tokens, quarter, width = x_ref.shape
    xhat, spread = normalise(x_ref[...].reshape(tokens * quarter, width))
    xhat_ref[...] = xhat
    spread_ref[...] = jnp.broadcast_to(spread, xhat.shape)
    unit = xhat * kept[2][...] + offset_ref[...]
    half = tokens * quarter // 2
    out_ref[...] = jnp.concatenate([unit[:half], unit[half:]], axis=1).astype(BF16)
    for copy in copies[3:]:
        copy.wait()


def grad_kernel(
    cot_ref, final_ref, first_ref, second_ref,
    by_col_ref, by_row_ref, cot_cols_ref, weight_ref, order_ref,
    cot_f, final_f,
    *, chans,
):
    tokens, block, _ = cot_ref.shape
    steps = by_col_ref.shape[0] // tokens
    per = LANES // chans
    cot = cot_ref[...]
    final = final_ref[...]
    cot_f[...] = cot.astype(F32)
    final_f[...] = final.astype(F32)
    for j in range(block):
        cot_cols_ref[j * tokens : (j + 1) * tokens, :] = cot_f[:, j, :].astype(BF16)
    cot_cols = cot_cols_ref[...]
    cot_rows = cot.reshape(tokens * block, cot.shape[2])
    for a in range(steps):
        got = dot(cot_cols, final[a * LANES : (a + 1) * LANES], 1, 1).astype(BF16)
        for j in range(block):
            by_col_ref[a * tokens : (a + 1) * tokens, j * LANES : (j + 1) * LANES] = got[
                j * tokens : (j + 1) * tokens
            ]
        lanes_dc = jnp.concatenate(
            [final_f[pl.ds(a * per + b, chans, stride=chans), :] for b in range(per)], axis=0
        ).astype(BF16)
        got = dot(cot_rows, lanes_dc, 1, 1).astype(BF16)
        for i in range(tokens):
            by_row_ref[a * block : (a + 1) * block, i * LANES : (i + 1) * LANES] = got[
                i * block : (i + 1) * block
            ]
    for x, ref in enumerate((first_ref, second_ref)):
        projector = ref[...]
        zero = jnp.zeros_like(projector)
        halves = [
            jnp.concatenate([projector, zero], axis=1),
            jnp.concatenate([zero, projector], axis=1),
        ]
        empty = jnp.concatenate([zero, zero], axis=1)
        for b in range(per):
            for h in range(2):
                for other in range(per):
                    at = (((x * 2) + h) * per + other) * chans
                    weight_ref[b, at : at + chans, :] = halves[h] if other == b else empty
    size = tokens * chans
    for b in range(per):
        row = lax.broadcasted_iota(jnp.int32, (size, LANES), 0)
        lane = lax.broadcasted_iota(jnp.int32, (size, LANES), 1)
        wanted = lane % tokens * chans + lane // tokens * per + b
        order_ref[:, b * LANES : (b + 1) * LANES] = jnp.where(row == wanted, 1.0, 0.0).astype(BF16)


def joint_kernel(n0, n1, n2, n3, out_ref, unit_f):
    blocks = (n0, n1, n2, n3)
    mine = lax.axis_index("cols")
    half, seqs, lanes = unit_f.shape
    quarter = seqs // len(blocks)
    for k, ref in enumerate(blocks):
        at = pl.multiple_of((mine ^ k) * quarter, quarter)
        unit_f[:, pl.ds(at, quarter), :] = ref[...].astype(F32).reshape(half, quarter, lanes)
    out_ref[...] = unit_f[...].reshape(half * seqs, lanes).astype(BF16)


def project(unit, weight_ref, x, seqs, per):
    half = unit.shape[0] // seqs
    by_group = unit.reshape(half // per, per, seqs, unit.shape[1])
    size = weight_ref.shape[1] // 2
    total = None
    for b in range(per):
        part = by_group[:, b].reshape(half // per * seqs, unit.shape[1])
        got = dot(part, weight_ref[b, x * size : (x + 1) * size, :], 1, 1)
        total = got if total is None else total + got
    total = total.astype(BF16)
    count = half // per
    return [
        total[p % count * seqs : (p % count + 1) * seqs, p // count * LANES : (p // count + 1) * LANES]
        for p in range(2 * count)
    ]


def reorder(tiles, order_ref):
    wide = dot(jnp.concatenate(tiles, axis=1), order_ref[...])
    count = wide.shape[1] // LANES
    return jnp.concatenate([wide[:, b * LANES : (b + 1) * LANES] for b in range(count)], axis=0)


def fold(spread_ref, seqs, chans, tokens):
    per = LANES // chans
    group = lane_group((seqs, LANES), chans)
    out = []
    for p in range(tokens // per):
        total = None
        for shift in range(per):
            parts = []
            for b in range(per):
                t = p * per + (b + shift) % per
                parts.append(spread_ref[b * seqs : (b + 1) * seqs, t * LANES : (t + 1) * LANES])
            part = pick(parts, group)
            if shift:
                part = pltpu.roll(part, shift * chans, 1)
            total = part if total is None else total + part
        out.append(total)
    return out


def slope(unit_turned, tiles, per, chans):
    seqs = tiles[0].shape[0]
    count = len(tiles) // 2
    group = lane_group((seqs, LANES), chans)
    rows = []
    for p in range(count):
        for b in range(per):
            rows.append(
                jnp.concatenate(
                    [jnp.where(group == b, tiles[h * count + p], 0.0) for h in range(2)], axis=1
                )
            )
    got = dot(unit_turned, jnp.concatenate(rows, axis=0).astype(BF16))
    width = unit_turned.shape[0] // 2
    return got[:width, :LANES] + got[width:, LANES:]


def left_kernel(
    unit_ref, weight_ref, order_ref, by_col_ref, left_ref, turned_ref, part_ref, spread_f, *, chans, seqs
):
    per = LANES // chans
    tokens = unit_ref.shape[0] // seqs * 2
    unit = unit_ref[...]
    turned_ref[...] = unit.astype(F32).T.astype(BF16)
    turned = reorder(project(unit, weight_ref, 0, seqs, per), order_ref)
    left_ref[...] = turned.T.astype(BF16)
    spread_f[...] = dot(turned.astype(BF16), by_col_ref[...])
    for p, tile in enumerate(fold(spread_f, seqs, chans, tokens)):
        part_ref[p] = tile * (1.0 / seqs)


def pair_kernel(
    unit_ref, left_ref, turned_ref, part_ref, weight_ref, order_ref, by_row_ref, cot_cols_ref,
    outer_ref, own_ref, m3, m2, m1,
    block_ref, slope_f, spread_f, both_f,
    *, chans, seqs, sizes,
):
    per, steps = LANES // chans, chans // (LANES // chans)
    rows, cols = sizes
    tokens = unit_ref.shape[0] // seqs * 2
    groups = tokens // per
    quarter = seqs // cols
    share = slope_f.shape[0] // (rows * cols)
    mine = lax.axis_index("cols")
    group = lane_group((seqs, LANES), chans)
    unit = unit_ref[...]
    right = project(unit, weight_ref, 1, seqs, per)
    for p, tile in enumerate(right):
        tile = tile.astype(F32)
        rolled = [pltpu.roll(tile, s * chans, 1) if s else tile for s in range(per)]
        for own in range(per):
            j = p * per + own
            for b in range(per):
                block_ref[b * seqs : (b + 1) * seqs, j * LANES : (j + 1) * LANES] = jnp.where(
                    group == b, rolled[(b - own) % per], 0.0
                ).astype(BF16)
    left = left_ref[...]
    for p in range(groups):
        span = per * LANES
        got = dot(left, block_ref[:, p * span : (p + 1) * span])
        got = (got * (1.0 / seqs)).astype(BF16)
        for own in range(per):
            j = p * per + own
            for a in range(steps):
                outer_ref[j * tokens : (j + 1) * tokens, a * LANES : (a + 1) * LANES] = got[
                    a * tokens : (a + 1) * tokens, own * LANES : (own + 1) * LANES
                ]
    spread_f[...] = dot(reorder(right, order_ref).astype(BF16), by_row_ref[...])
    slope_f[...] = dot(outer_ref[...], cot_cols_ref[...], 0, 0)
    lefts = [tile * (1.0 / seqs) for tile in fold(spread_f, seqs, chans, tokens)]
    rights = [part_ref[p] for p in range(groups)]
    for p in range(groups):
        both_f[p, 0] = lefts[p]
        both_f[p, 1] = rights[p]
    sides = [
        slope(turned_ref[...], lefts, per, chans),
        slope(unit.astype(F32).T.astype(BF16), rights, per, chans),
    ]
    width = sides[0].shape[0]
    sides = [s + pltpu.roll(s, LANES // 2, 1) for s in sides]
    slopes = jnp.where(lane_group((width, LANES), LANES // 2) == 0, sides[0], sides[1])
    for k, ref in enumerate((own_ref, m1, m2, m3)):
        peer = mine ^ k
        kind = ref.dtype
        for r in range(rows):
            at = pl.multiple_of((r * cols + peer) * share, share)
            ref[r * share : (r + 1) * share, :] = slope_f[pl.ds(at, share), :].astype(kind)
        base = rows * share
        at = pl.multiple_of(peer * quarter, quarter)
        span = groups * quarter
        for x in range(2):
            ref[base + x * span : base + (x + 1) * span, :] = (
                both_f[:, x, pl.ds(at, quarter), :].reshape(span, LANES).astype(kind)
            )
        base += 2 * span
        ref[base : base + width, :] = slopes.astype(kind)


def update_kernel(outer_ref, final_ref, bias_ref, update_ref, update_f):
    tokens = update_ref.shape[0]
    update = dot(outer_ref[...], final_ref[...]) + bias_ref[...]
    for j in range(update_ref.shape[1]):
        update_f[:, j, :] = update[j * tokens : (j + 1) * tokens]
    update_ref[...] = update_f[...].astype(BF16)


def between_kernel(
    own_ref, r3, r2, r1, left_ref, next_ref, m3, m2, m1, total_f, right_f, *, rows, share
):
    refs = (own_ref, r1, r2, r3)
    span = left_ref.shape[0]
    first = rows * share
    last = first + 2 * span
    mine, column = lax.axis_index("rows"), lax.axis_index("cols")
    for k, ref in enumerate(refs):
        right_f[column ^ k] = ref[first + span : last, :].astype(F32)
    for start, stop in ((0, first + span), (last, total_f.shape[0])):
        total = own_ref[start:stop, :]
        for ref in refs[1:]:
            total = total + ref[start:stop, :].astype(F32)
        total_f[start:stop, :] = total
    left_ref[...] = total_f[first : first + span, :]
    slopes = total_f[last:, :]
    for k, ref in enumerate((next_ref, m1, m2, m3)):
        peer = mine ^ k
        at = pl.multiple_of(peer * share, share)
        ref[0:share, :] = total_f[pl.ds(at, share), :].astype(ref.dtype)
        ref[share : share + span, :] = right_f[peer].astype(ref.dtype)
        ref[share + span :, :] = slopes.astype(ref.dtype)


def to_unit(back, projector_ref, unit_ref, quarter):
    back = back[...]
    projector = projector_ref[...]
    chans = projector.shape[0]
    high = back.astype(BF16)
    low = (back - high.astype(F32)).astype(BF16)
    zero = jnp.zeros_like(projector)
    per = LANES // chans
    for b in range(per):
        weights = jnp.concatenate([projector if i == b else zero for i in range(per)], axis=0)
        got = dot(high, weights) + dot(low, weights)
        for p in range(back.shape[0] // quarter):
            unit_ref[p * per + b] = got[p * quarter : (p + 1) * quarter]


def last_kernel(
    own_ref, r3, r2, r1, unit_ref, xhat_ref, spread_ref, gain_ref, second_ref,
    final_ref, first_slope_ref, second_slope_ref, out_ref, unit_f,
):
    total = own_ref[...] + r1[...].astype(F32) + r2[...].astype(F32) + r3[...].astype(F32)
    share = final_ref.shape[0]
    final_ref[...] = total[:share]
    tokens, quarter, width = out_ref.shape
    span = tokens * quarter * second_ref.shape[0] // LANES
    to_unit(total[share : share + span], second_ref, unit_f, quarter)
    g = (unit_ref[...] + unit_f[...]).reshape(tokens * quarter, width) * gain_ref[...]
    xhat = xhat_ref[...]
    out = spread_ref[...] * (
        g
        - jnp.mean(g, axis=-1, keepdims=True)
        - xhat * jnp.mean(g * xhat, axis=-1, keepdims=True)
    )
    out_ref[...] = out.reshape(tokens, quarter, width)
    slopes = total[share + span :].T
    chans = second_ref.shape[0]
    for x, ref in enumerate((first_slope_ref, second_slope_ref)):
        side = slopes[x * LANES // 2 : (x + 1) * LANES // 2]
        out = side[:chans]
        for b in range(1, LANES // 2 // chans):
            out = out + side[b * chans : (b + 1) * chans]
        ref[...] = out


def exchange(messages, axis, order):
    size = lax.axis_size(axis)
    got = {}
    for k in order:
        got[k] = lax.ppermute(messages[k], axis, [(p, p ^ k) for p in range(size)])
    return [got[k] for k in sorted(got)]


def holders(rows, cols):
    pairs = []
    for r in range(rows):
        far = sorted((z for z in range(rows) if z != r), key=lambda z: (-abs(z - r), z))
        near = sorted((q for q in range(cols) if q != r), key=lambda q: (q // 2 != r // 2, q))
        pairs += [(r * cols + r, r * cols + r)]
        pairs += [(r * cols + q, z * cols + r) for q, z in zip(near, far)]
    return sorted(pairs)


def local_square(
    alignment_features,
    affine_factor,
    affine_offset,
    first_projector,
    second_projector,
    final_projector,
    additive_term,
    adjoint_update,
):
    rows, cols = lax.axis_size("rows"), lax.axis_size("cols")
    tokens, quarter, width = alignment_features.shape
    chans = first_projector.shape[1]
    total, pair_ch = final_projector.shape
    seqs = quarter * cols
    per, steps = LANES // chans, chans // (LANES // chans)
    share = total // (rows * cols)
    shape = jax.ShapeDtypeStruct
    wide, tall = tokens * LANES, steps * tokens
    groups = tokens // per
    half = tokens // 2
    aligned = shape((tokens, quarter, width), F32)
    flat = shape((tokens * quarter, width), F32)
    inputs = [
        alignment_features,
        affine_offset.reshape(1, width),
        affine_factor.reshape(1, width),
        adjoint_update,
        final_projector,
        first_projector.T,
        second_projector.T,
        additive_term.reshape(1, pair_ch),
    ]
    unit, xhat, spread, gain, cot, final, first, second, bias = call(
        norm_kernel,
        [shape((half * quarter, 2 * width), BF16), flat, flat]
        + [shape(i.shape, i.dtype) for i in inputs[2:]],
        [pltpu.VMEM(i.shape, i.dtype) for i in inputs[:2]]
        + [pltpu.SemaphoreType.DMA((len(inputs),))],
        space=pltpu.HBM,
    )(*[pltpu.with_memory_space_constraint(i, pltpu.HBM) for i in inputs])
    units = [unit] + exchange([unit] * cols, "cols", (1, 2, 3))
    by_col, by_row, cot_cols, weight, order = call(
        functools.partial(grad_kernel, chans=chans),
        (
            shape((tall, wide), BF16),
            shape((tall, wide), BF16),
            shape((tokens * tokens, pair_ch), BF16),
            shape((per, 4 * LANES, 2 * width), BF16),
            shape((tokens * chans, per * LANES), BF16),
        ),
        [pltpu.VMEM(adjoint_update.shape, F32), pltpu.VMEM((total, pair_ch), F32)],
        flops=8 * tokens * tokens * total * pair_ch,
    )(cot, final, first, second)
    unit_rows = call(
        joint_kernel,
        shape((half * seqs, 2 * width), BF16),
        [pltpu.VMEM((half, seqs, 2 * width), F32)],
    )(*units)
    unit_cols = lax.ppermute(unit_rows, ("rows", "cols"), holders(rows, cols))
    left, turned, part = call(
        functools.partial(left_kernel, chans=chans, seqs=seqs),
        (
            shape((tall, LANES), BF16),
            shape((2 * width, half * seqs), BF16),
            shape((groups, seqs, LANES), F32),
        ),
        [pltpu.VMEM((LANES, wide), F32)],
        flops=10**8,
    )(unit_rows, weight, order, by_col)
    span = groups * quarter
    message = rows * share + 2 * span + width
    outer, own, *messages = call(
        functools.partial(pair_kernel, chans=chans, seqs=seqs, sizes=(rows, cols)),
        (
            shape((tokens * tokens, total), BF16),
            shape((message, LANES), F32),
            *[shape((message, LANES), BF16)] * (cols - 1),
        ),
        [
            pltpu.VMEM((LANES, wide), BF16),
            pltpu.VMEM((total, pair_ch), F32),
            pltpu.VMEM((LANES, wide), F32),
            pltpu.VMEM((groups, 2, seqs, LANES), F32),
        ],
    )(unit_cols, left, turned, part, weight, order, by_row, cot_cols)
    got = exchange([own] + messages[::-1], "cols", (1, 2, 3))
    update = call(
        update_kernel,
        shape((tokens, tokens, pair_ch), BF16),
        [pltpu.VMEM((tokens, tokens, pair_ch), F32)],
        flops=10**8,
    )(outer, final, bias)
    message = share + span + width
    back, own, *messages = call(
        functools.partial(between_kernel, rows=rows, share=share),
        (
            shape((span, LANES), F32),
            shape((message, LANES), F32),
            *[shape((message, LANES), BF16)] * (rows - 1),
        ),
        [
            pltpu.VMEM((rows * share + 2 * span + width, LANES), F32),
            pltpu.VMEM((cols, span, LANES), F32),
        ],
    )(own, *got[::-1])
    got = exchange([own] + messages[::-1], "rows", (1, 2, 3))
    from_left = call(functools.partial(to_unit, quarter=quarter), aligned, flops=10**8)(back, first)
    final_slope, first_slope, second_slope, alignment_slope = call(
        last_kernel,
        (
            shape((share, pair_ch), F32),
            shape((chans, width), F32),
            shape((chans, width), F32),
            aligned,
        ),
        [pltpu.VMEM((tokens, quarter, width), F32)],
    )(own, *got[::-1], from_left, xhat, spread, gain, second)
    return update, alignment_slope, final_slope, first_slope.T, second_slope.T


def fits(mesh, alignment_features, first_projector, final_projector):
    rows, cols = mesh.shape["rows"], mesh.shape["cols"]
    tokens = alignment_features.shape[0] // (mesh.shape["groups"] * rows)
    quarter = alignment_features.shape[1] // cols
    width, chans = first_projector.shape
    per = LANES // chans
    return (
        rows == cols == 4
        and chans * per == LANES
        and chans % per == 0
        and chans // per == SUBLANES
        and 2 * width == LANES
        and final_projector.shape[1] == LANES
        and quarter == SUBLANES
        and tokens % (2 * SUBLANES) == 0
        and quarter * cols == chans
        and chans // per * tokens == LANES
    )


def solution(mesh):
    in_specs = (
        P(("groups", "rows"), "cols", None),
        P(),
        P(),
        P(),
        P(),
        P(),
        P(),
        P(("groups", "rows"), "cols", None),
    )
    out_specs = (
        P(("groups", "rows"), "cols", None),
        P(("groups", "rows"), "cols", None),
        P(("groups", "rows", "cols"), None),
        P("groups", None),
        P("groups", None),
    )

    def whole(*args):
        square = fits(mesh, args[0], args[3], args[5])
        return jax.shard_map(
            local_square if square else local_general,
            mesh=mesh,
            in_specs=in_specs,
            out_specs=out_specs,
            check_vma=False,
        )(*args)

    return whole
```

```python
import functools
import itertools

import jax
import jax.numpy as jnp
from jax import lax
from jax.experimental import pallas as pl
from jax.experimental.pallas import tpu as pltpu
from jax.sharding import PartitionSpec as P


def layernorm_parts(alignment_features, affine_factor, affine_offset):
    centered_alignment = alignment_features - jnp.mean(alignment_features, axis=-1, keepdims=True)
    reciprocal_spread = lax.rsqrt(
        jnp.mean(centered_alignment * centered_alignment, axis=-1, keepdims=True) + 1e-05
    )
    zscored_alignment = centered_alignment * reciprocal_spread
    return (
        zscored_alignment,
        reciprocal_spread,
        (zscored_alignment * affine_factor + affine_offset).astype(jnp.bfloat16),
    )


def local_general(
    alignment_features,
    affine_factor,
    affine_offset,
    first_projector,
    second_projector,
    final_projector,
    additive_term,
    adjoint_update,
):
    zscored_alignment, reciprocal_spread, unit_alignment = layernorm_parts(
        alignment_features, affine_factor, affine_offset
    )
    first_factor_here = jnp.dot(
        unit_alignment, first_projector, preferred_element_type=jnp.float32
    ).astype(jnp.bfloat16)
    second_factor_here = jnp.dot(
        unit_alignment, second_projector, preferred_element_type=jnp.float32
    ).astype(jnp.bfloat16)
    tokens, quarter, chans = first_factor_here.shape
    left_flat = first_factor_here.reshape(tokens, quarter * chans)
    right_flat = second_factor_here.reshape(tokens, quarter * chans)
    left_wide, right_wide = (
        lax.all_gather(left_flat, "cols", axis=1, tiled=True),
        lax.all_gather(right_flat, "cols", axis=1, tiled=True),
    )
    left_rows = left_wide.reshape(tokens, -1, chans)
    right_all = lax.all_gather(right_wide, "rows", axis=0, tiled=True)
    block = right_all.shape[0] // lax.axis_size("cols")
    right_cols = lax.dynamic_slice_in_dim(
        right_all, lax.axis_index("cols") * block, block, 0
    ).reshape(block, -1, chans)
    seqs = left_rows.shape[1]
    multiplier = 1.0 / seqs
    pair_ch = adjoint_update.shape[2]
    step_rows = 4
    rounds = tokens // step_rows
    first_tile_list = left_rows.reshape(rounds, step_rows, seqs, chans)
    cot_blocks = adjoint_update.reshape(rounds, step_rows, block, pair_ch)

    def advance(carry, inputs):
        right_acc, out_acc = carry
        left_slab, cot_slab = inputs
        outer = (
            jnp.einsum("isc,jsd->ijcd", left_slab, right_cols, preferred_element_type=jnp.float32)
            * multiplier
        ).astype(jnp.bfloat16)
        flat = outer.reshape(step_rows * block, chans * chans)
        cot_flat = cot_slab.reshape(step_rows * block, pair_ch)
        update = (
            jnp.dot(flat, final_projector, preferred_element_type=jnp.float32) + additive_term
        ).astype(jnp.bfloat16)
        outer_grad = jnp.dot(
            cot_flat, final_projector.T, preferred_element_type=jnp.float32
        ).astype(jnp.bfloat16)
        outer_grad = outer_grad.reshape(step_rows, block, chans, chans)
        left_piece = (
            jnp.einsum("ijcd,jsd->isc", outer_grad, right_cols, preferred_element_type=jnp.float32)
            * multiplier
        )
        right_acc = (
            right_acc
            + jnp.einsum("ijcd,isc->jsd", outer_grad, left_slab, preferred_element_type=jnp.float32)
            * multiplier
        )
        out_acc = out_acc + jnp.einsum(
            "fk,fe->ke", flat, cot_flat, preferred_element_type=jnp.float32
        )
        return ((right_acc, out_acc), (update.reshape(step_rows, block, pair_ch), left_piece))

    beginning_position = (
        jnp.zeros((block, seqs, chans), jnp.float32),
        jnp.zeros((chans * chans, pair_ch), jnp.float32),
    )
    (right_part, out_term), (updates, left_pieces) = lax.scan(
        advance, beginning_position, (first_tile_list, cot_blocks)
    )
    residue_update = updates.reshape(tokens, block, pair_ch)
    left_part = left_pieces.reshape(tokens, seqs * chans)
    first_adjoint = lax.psum_scatter(left_part, "cols", scatter_dimension=1, tiled=True).reshape(
        tokens, quarter, chans
    )
    moved = lax.all_to_all(
        right_part.reshape(block, seqs * chans), "cols", split_axis=1, concat_axis=0, tiled=True
    )
    right_back = lax.psum_scatter(moved, "rows", scatter_dimension=0, tiled=True).reshape(
        tokens, quarter, chans
    )
    final_projector_slope = lax.psum_scatter(
        out_term, ("rows", "cols"), scatter_dimension=0, tiled=True
    )
    unit_broadcast = unit_alignment.astype(jnp.float32)
    high = lax.Precision.HIGHEST
    left_term = jnp.einsum("tsk,tsc->kc", unit_broadcast, first_adjoint, precision=high)
    right_term = jnp.einsum("tsk,tsc->kc", unit_broadcast, right_back, precision=high)
    first_projector_slope, second_projector_slope = lax.psum(
        (left_term, right_term), ("rows", "cols")
    )
    unit_adjoint = jnp.einsum(
        "tsc,kc->tsk", first_adjoint, first_projector.astype(jnp.float32), precision=high
    )
    unit_adjoint = unit_adjoint + jnp.einsum(
        "tsc,kc->tsk", right_back, second_projector.astype(jnp.float32), precision=high
    )
    scaled_alignment = unit_adjoint * affine_factor
    alignment_slope = reciprocal_spread * (
        scaled_alignment
        - jnp.mean(scaled_alignment, axis=-1, keepdims=True)
        - zscored_alignment * jnp.mean(scaled_alignment * zscored_alignment, axis=-1, keepdims=True)
    )
    return (
        residue_update,
        alignment_slope,
        final_projector_slope,
        first_projector_slope,
        second_projector_slope,
    )


F32, BF16 = jnp.float32, jnp.bfloat16
LANES, SUBLANES = 128, 8


def dot(a, b, at=1, bt=0):
    return lax.dot_general(a, b, (((at,), (bt,)), ((), ())), preferred_element_type=F32)


def lane_group(shape, size):
    return lax.broadcasted_iota(jnp.int32, shape, len(shape) - 1) // size


def pick(parts, group):
    out = parts[-1]
    for b in range(len(parts) - 2, -1, -1):
        out = jnp.where(group == b, parts[b], out)
    return out


def normalise(x):
    centered = x - jnp.mean(x, axis=-1, keepdims=True)
    spread = lax.rsqrt(jnp.mean(centered * centered, axis=-1, keepdims=True) + 1e-05)
    return centered * spread, spread


def call(kernel, out_shape, scratch=(), flops=0, space=pltpu.VMEM):
    place = pl.BlockSpec(memory_space=space)
    on_chip = pl.BlockSpec(memory_space=pltpu.VMEM)

    def run(*args):
        return pl.pallas_call(
            kernel,
            out_shape=out_shape,
            in_specs=[place] * len(args),
            out_specs=jax.tree.map(lambda _: on_chip, out_shape),
            scratch_shapes=list(scratch),
            cost_estimate=pl.CostEstimate(flops=flops, bytes_accessed=0, transcendentals=0),
            compiler_params=pltpu.CompilerParams(vmem_limit_bytes=16 * 2**20),
        )(*args)

    return run


def norm_kernel(*refs):
    x_ref, offset_ref, sems = refs[-3:]
    count = sems.shape[0]
    sources, (out_ref, xhat_ref, spread_ref) = refs[:count], refs[count : count + 3]
    kept = (x_ref, offset_ref) + refs[count + 3 : -3]
    copies = [
        pltpu.make_async_copy(source, ref, sems.at[n])
        for n, (source, ref) in enumerate(zip(sources, kept))
    ]
    for copy in copies:
        copy.start()
    for copy in copies[:3]:
        copy.wait()
    tokens, quarter, width = x_ref.shape
    xhat, spread = normalise(x_ref[...].reshape(tokens * quarter, width))
    xhat_ref[...] = xhat
    spread_ref[...] = jnp.broadcast_to(spread, xhat.shape)
    unit = xhat * kept[2][...] + offset_ref[...]
    half = tokens * quarter // 2
    out_ref[...] = jnp.concatenate([unit[:half], unit[half:]], axis=1).astype(BF16)
    for copy in copies[3:]:
        copy.wait()


def grad_kernel(
    cot_ref, final_ref, first_ref, second_ref,
    by_col_ref, by_row_ref, cot_cols_ref, weight_ref, order_ref,
    cot_f, final_f,
    *, chans,
):
    tokens, block, _ = cot_ref.shape
    steps = by_col_ref.shape[0] // tokens
    per = LANES // chans
    cot = cot_ref[...]
    final = final_ref[...]
    cot_f[...] = cot.astype(F32)
    final_f[...] = final.astype(F32)
    for j in range(block):
        cot_cols_ref[j * tokens : (j + 1) * tokens, :] = cot_f[:, j, :].astype(BF16)
    cot_cols = cot_cols_ref[...]
    cot_rows = cot.reshape(tokens * block, cot.shape[2])
    for a in range(steps):
        got = dot(cot_cols, final[a * LANES : (a + 1) * LANES], 1, 1).astype(BF16)
        for j in range(block):
            by_col_ref[a * tokens : (a + 1) * tokens, j * LANES : (j + 1) * LANES] = got[
                j * tokens : (j + 1) * tokens
            ]
        lanes_dc = jnp.concatenate(
            [final_f[pl.ds(a * per + b, chans, stride=chans), :] for b in range(per)], axis=0
        ).astype(BF16)
        got = dot(cot_rows, lanes_dc, 1, 1).astype(BF16)
        for i in range(tokens):
            by_row_ref[a * block : (a + 1) * block, i * LANES : (i + 1) * LANES] = got[
                i * block : (i + 1) * block
            ]
    for x, ref in enumerate((first_ref, second_ref)):
        projector = ref[...]
        zero = jnp.zeros_like(projector)
        halves = [
            jnp.concatenate([projector, zero], axis=1),
            jnp.concatenate([zero, projector], axis=1),
        ]
        empty = jnp.concatenate([zero, zero], axis=1)
        for b in range(per):
            for h in range(2):
                for other in range(per):
                    at = (((x * 2) + h) * per + other) * chans
                    weight_ref[b, at : at + chans, :] = halves[h] if other == b else empty
    size = tokens * chans
    for b in range(per):
        row = lax.broadcasted_iota(jnp.int32, (size, LANES), 0)
        lane = lax.broadcasted_iota(jnp.int32, (size, LANES), 1)
        wanted = lane % tokens * chans + lane // tokens * per + b
        order_ref[:, b * LANES : (b + 1) * LANES] = jnp.where(row == wanted, 1.0, 0.0).astype(BF16)


def half_kernel(own_ref, other_ref, out_ref, unit_f):
    low = lax.axis_index("cols") % 2
    half, seqs, lanes = unit_f.shape
    quarter = seqs // 2
    for k, ref in enumerate((own_ref, other_ref)):
        at = pl.multiple_of((low ^ k) * quarter, quarter)
        unit_f[:, pl.ds(at, quarter), :] = ref[...].astype(F32).reshape(half, quarter, lanes)
    out_ref[...] = unit_f[...].reshape(half * seqs, lanes).astype(BF16)


def join(first_half, refs, unit_ref):
    half, seqs, lanes = unit_ref.shape
    for k, ref in enumerate(refs):
        at = pl.multiple_of((first_half ^ k) * (seqs // 2), seqs // 2)
        unit_ref[:, pl.ds(at, seqs // 2), :] = ref[...].reshape(half, seqs // 2, lanes)
    return unit_ref[...].reshape(half * seqs, lanes)


def project(unit, weight_ref, x, seqs, per):
    half = unit.shape[0] // seqs
    by_group = unit.reshape(half // per, per, seqs, unit.shape[1])
    size = weight_ref.shape[1] // 2
    total = None
    for b in range(per):
        part = by_group[:, b].reshape(half // per * seqs, unit.shape[1])
        got = dot(part, weight_ref[b, x * size : (x + 1) * size, :], 1, 1)
        total = got if total is None else total + got
    total = total.astype(BF16)
    count = half // per
    return [
        total[p % count * seqs : (p % count + 1) * seqs, p // count * LANES : (p // count + 1) * LANES]
        for p in range(2 * count)
    ]


def reorder(tiles, order_ref):
    wide = dot(jnp.concatenate(tiles, axis=1), order_ref[...])
    count = wide.shape[1] // LANES
    return jnp.concatenate([wide[:, b * LANES : (b + 1) * LANES] for b in range(count)], axis=0)


def fold(spread_ref, seqs, chans, tokens):
    per = LANES // chans
    group = lane_group((seqs, LANES), chans)
    out = []
    for p in range(tokens // per):
        total = None
        for shift in range(per):
            parts = []
            for b in range(per):
                t = p * per + (b + shift) % per
                parts.append(spread_ref[b * seqs : (b + 1) * seqs, t * LANES : (t + 1) * LANES])
            part = pick(parts, group)
            if shift:
                part = pltpu.roll(part, shift * chans, 1)
            total = part if total is None else total + part
        out.append(total)
    return out


def slope(unit_turned, tiles, per, chans):
    seqs = tiles[0].shape[0]
    count = len(tiles) // 2
    group = lane_group((seqs, LANES), chans)
    rows = []
    for p in range(count):
        for b in range(per):
            rows.append(
                jnp.concatenate(
                    [jnp.where(group == b, tiles[h * count + p], 0.0) for h in range(2)], axis=1
                )
            )
    got = dot(unit_turned, jnp.concatenate(rows, axis=0).astype(BF16))
    width = unit_turned.shape[0] // 2
    return got[:width, :LANES] + got[width:, LANES:]


def left_kernel(
    u0, u1, weight_ref, order_ref, by_col_ref, left_ref, turned_ref, part_ref, unit_ref, spread_f,
    *, chans,
):
    per = LANES // chans
    half, seqs, _ = unit_ref.shape
    tokens = 2 * half
    unit = join(lax.axis_index("cols") // 2, (u0, u1), unit_ref)
    turned_ref[...] = unit.astype(F32).T.astype(BF16)
    turned = reorder(project(unit, weight_ref, 0, seqs, per), order_ref)
    left_ref[...] = turned.T.astype(BF16)
    spread_f[...] = dot(turned.astype(BF16), by_col_ref[...])
    for p, tile in enumerate(fold(spread_f, seqs, chans, tokens)):
        part_ref[p] = tile * (1.0 / seqs)


def pair_kernel(
    u0, u1, left_ref, turned_ref, part_ref, weight_ref, order_ref, by_row_ref, cot_cols_ref,
    outer_ref, own_ref, m3, m2, m1,
    block_ref, slope_f, spread_f, both_f, unit_ref,
    *, chans, sizes, first_halves,
):
    per, steps = LANES // chans, chans // (LANES // chans)
    rows, cols = sizes
    half, seqs, _ = unit_ref.shape
    tokens = 2 * half
    groups = tokens // per
    quarter = seqs // cols
    share = slope_f.shape[0] // (rows * cols)
    mine = lax.axis_index("cols")
    group = lane_group((seqs, LANES), chans)
    place = lax.axis_index("rows") * cols + mine
    unit = join((first_halves >> place) & 1, (u0, u1), unit_ref)
    right = project(unit, weight_ref, 1, seqs, per)
    for p, tile in enumerate(right):
        tile = tile.astype(F32)
        rolled = [pltpu.roll(tile, s * chans, 1) if s else tile for s in range(per)]
        for own in range(per):
            j = p * per + own
            for b in range(per):
                block_ref[b * seqs : (b + 1) * seqs, j * LANES : (j + 1) * LANES] = jnp.where(
                    group == b, rolled[(b - own) % per], 0.0
                ).astype(BF16)
    left = left_ref[...]
    for p in range(groups):
        span = per * LANES
        got = dot(left, block_ref[:, p * span : (p + 1) * span])
        got = (got * (1.0 / seqs)).astype(BF16)
        for own in range(per):
            j = p * per + own
            for a in range(steps):
                outer_ref[j * tokens : (j + 1) * tokens, a * LANES : (a + 1) * LANES] = got[
                    a * tokens : (a + 1) * tokens, own * LANES : (own + 1) * LANES
                ]
    spread_f[...] = dot(reorder(right, order_ref).astype(BF16), by_row_ref[...])
    slope_f[...] = dot(outer_ref[...], cot_cols_ref[...], 0, 0)
    lefts = [tile * (1.0 / seqs) for tile in fold(spread_f, seqs, chans, tokens)]
    rights = [part_ref[p] for p in range(groups)]
    for p in range(groups):
        both_f[p, 0] = lefts[p]
        both_f[p, 1] = rights[p]
    sides = [
        slope(turned_ref[...], lefts, per, chans),
        slope(unit.astype(F32).T.astype(BF16), rights, per, chans),
    ]
    width = sides[0].shape[0]
    sides = [s + pltpu.roll(s, LANES // 2, 1) for s in sides]
    slopes = jnp.where(lane_group((width, LANES), LANES // 2) == 0, sides[0], sides[1])
    for k, ref in enumerate((own_ref, m1, m2, m3)):
        peer = mine ^ k
        kind = ref.dtype
        for r in range(rows):
            at = pl.multiple_of((r * cols + peer) * share, share)
            ref[r * share : (r + 1) * share, :] = slope_f[pl.ds(at, share), :].astype(kind)
        base = rows * share
        at = pl.multiple_of(peer * quarter, quarter)
        span = groups * quarter
        for x in range(2):
            ref[base + x * span : base + (x + 1) * span, :] = (
                both_f[:, x, pl.ds(at, quarter), :].reshape(span, LANES).astype(kind)
            )
        base += 2 * span
        ref[base : base + width, :] = slopes.astype(kind)


def update_kernel(outer_ref, final_ref, bias_ref, update_ref, update_f):
    tokens = update_ref.shape[0]
    update = dot(outer_ref[...], final_ref[...]) + bias_ref[...]
    for j in range(update_ref.shape[1]):
        update_f[:, j, :] = update[j * tokens : (j + 1) * tokens]
    update_ref[...] = update_f[...].astype(BF16)


def between_kernel(
    own_ref, r3, r2, r1, left_ref, next_ref, m3, m2, m1, total_f, right_f, *, rows, share
):
    refs = (own_ref, r1, r2, r3)
    span = left_ref.shape[0]
    first = rows * share
    last = first + 2 * span
    mine, column = lax.axis_index("rows"), lax.axis_index("cols")
    for k, ref in enumerate(refs):
        right_f[column ^ k] = ref[first + span : last, :].astype(F32)
    for start, stop in ((0, first + span), (last, total_f.shape[0])):
        total = own_ref[start:stop, :]
        for ref in refs[1:]:
            total = total + ref[start:stop, :].astype(F32)
        total_f[start:stop, :] = total
    left_ref[...] = total_f[first : first + span, :]
    slopes = total_f[last:, :]
    for k, ref in enumerate((next_ref, m1, m2, m3)):
        peer = mine ^ k
        at = pl.multiple_of(peer * share, share)
        ref[0:share, :] = total_f[pl.ds(at, share), :].astype(ref.dtype)
        ref[share : share + span, :] = right_f[peer].astype(ref.dtype)
        ref[share + span :, :] = slopes.astype(ref.dtype)


def to_unit(back, projector_ref, unit_ref, quarter):
    back = back[...]
    projector = projector_ref[...]
    chans = projector.shape[0]
    high = back.astype(BF16)
    low = (back - high.astype(F32)).astype(BF16)
    zero = jnp.zeros_like(projector)
    per = LANES // chans
    for b in range(per):
        weights = jnp.concatenate([projector if i == b else zero for i in range(per)], axis=0)
        got = dot(high, weights) + dot(low, weights)
        for p in range(back.shape[0] // quarter):
            unit_ref[p * per + b] = got[p * quarter : (p + 1) * quarter]


def last_kernel(
    own_ref, r3, r2, r1, unit_ref, xhat_ref, spread_ref, gain_ref, second_ref,
    final_ref, first_slope_ref, second_slope_ref, out_ref, unit_f,
):
    total = own_ref[...] + r1[...].astype(F32) + r2[...].astype(F32) + r3[...].astype(F32)
    share = final_ref.shape[0]
    final_ref[...] = total[:share]
    tokens, quarter, width = out_ref.shape
    span = tokens * quarter * second_ref.shape[0] // LANES
    to_unit(total[share : share + span], second_ref, unit_f, quarter)
    g = (unit_ref[...] + unit_f[...]).reshape(tokens * quarter, width) * gain_ref[...]
    xhat = xhat_ref[...]
    out = spread_ref[...] * (
        g
        - jnp.mean(g, axis=-1, keepdims=True)
        - xhat * jnp.mean(g * xhat, axis=-1, keepdims=True)
    )
    out_ref[...] = out.reshape(tokens, quarter, width)
    slopes = total[share + span :].T
    chans = second_ref.shape[0]
    for x, ref in enumerate((first_slope_ref, second_slope_ref)):
        side = slopes[x * LANES // 2 : (x + 1) * LANES // 2]
        out = side[:chans]
        for b in range(1, LANES // 2 // chans):
            out = out + side[b * chans : (b + 1) * chans]
        ref[...] = out


def exchange(messages, axis, order):
    size = lax.axis_size(axis)
    got = {}
    for k in order:
        got[k] = lax.ppermute(messages[k], axis, [(p, p ^ k) for p in range(size)])
    return [got[k] for k in sorted(got)]


def holders(rows, cols):
    first, second, mask = [], [], 0
    for r in range(rows):

        def hops(to):
            return [abs(z - r) + (q // 2 != r // 2) for q, z in enumerate(to) if z != r]

        best = None
        for a in itertools.permutations(range(rows)):
            for b in itertools.permutations(range(rows)):
                if any(a.index(z) // 2 == b.index(z) // 2 for z in range(rows)):
                    continue
                cost = (max(hops(a) + hops(b)), sum(hops(a) + hops(b)))
                if best is None or cost < best[0]:
                    best = cost, a, b
        _, a, b = best
        first += [(r * cols + q, z * cols + r) for q, z in enumerate(a)]
        second += [(r * cols + q, z * cols + r) for q, z in enumerate(b)]
        for q, z in enumerate(a):
            mask |= q // 2 << (z * cols + r)
    return first, second, mask


def local_square(
    alignment_features,
    affine_factor,
    affine_offset,
    first_projector,
    second_projector,
    final_projector,
    additive_term,
    adjoint_update,
):
    rows, cols = lax.axis_size("rows"), lax.axis_size("cols")
    tokens, quarter, width = alignment_features.shape
    chans = first_projector.shape[1]
    total, pair_ch = final_projector.shape
    seqs = quarter * cols
    per, steps = LANES // chans, chans // (LANES // chans)
    share = total // (rows * cols)
    shape = jax.ShapeDtypeStruct
    wide, tall = tokens * LANES, steps * tokens
    groups = tokens // per
    half = tokens // 2
    aligned = shape((tokens, quarter, width), F32)
    flat = shape((tokens * quarter, width), F32)
    inputs = [
        alignment_features,
        affine_offset.reshape(1, width),
        affine_factor.reshape(1, width),
        adjoint_update,
        final_projector,
        first_projector.T,
        second_projector.T,
        additive_term.reshape(1, pair_ch),
    ]
    unit, xhat, spread, gain, cot, final, first, second, bias = call(
        norm_kernel,
        [shape((half * quarter, 2 * width), BF16), flat, flat]
        + [shape(i.shape, i.dtype) for i in inputs[2:]],
        [pltpu.VMEM(i.shape, i.dtype) for i in inputs[:2]]
        + [pltpu.SemaphoreType.DMA((len(inputs),))],
        space=pltpu.HBM,
    )(*[pltpu.with_memory_space_constraint(i, pltpu.HBM) for i in inputs])
    pairs = [(p, p ^ 1) for p in range(cols)]
    halves = call(
        half_kernel,
        shape((half * seqs // 2, 2 * width), BF16),
        [pltpu.VMEM((half, seqs // 2, 2 * width), F32)],
    )(unit, lax.ppermute(unit, "cols", pairs))
    from_first, from_second, first_halves = holders(rows, cols)
    cols_a = lax.ppermute(halves, ("rows", "cols"), from_first)
    cols_b = lax.ppermute(halves, ("rows", "cols"), from_second)
    across = lax.ppermute(halves, "cols", [(p, p ^ 2) for p in range(cols)])
    by_col, by_row, cot_cols, weight, order = call(
        functools.partial(grad_kernel, chans=chans),
        (
            shape((tall, wide), BF16),
            shape((tall, wide), BF16),
            shape((tokens * tokens, pair_ch), BF16),
            shape((per, 4 * LANES, 2 * width), BF16),
            shape((tokens * chans, per * LANES), BF16),
        ),
        [pltpu.VMEM(adjoint_update.shape, F32), pltpu.VMEM((total, pair_ch), F32)],
        flops=8 * tokens * tokens * total * pair_ch,
    )(cot, final, first, second)
    left, turned, part = call(
        functools.partial(left_kernel, chans=chans),
        (
            shape((tall, LANES), BF16),
            shape((2 * width, half * seqs), BF16),
            shape((groups, seqs, LANES), F32),
        ),
        [pltpu.VMEM((half, seqs, 2 * width), BF16), pltpu.VMEM((LANES, wide), F32)],
        flops=10**8,
    )(halves, across, weight, order, by_col)
    span = groups * quarter
    message = rows * share + 2 * span + width
    outer, own, *messages = call(
        functools.partial(
            pair_kernel, chans=chans, sizes=(rows, cols), first_halves=first_halves
        ),
        (
            shape((tokens * tokens, total), BF16),
            shape((message, LANES), F32),
            *[shape((message, LANES), BF16)] * (cols - 1),
        ),
        [
            pltpu.VMEM((LANES, wide), BF16),
            pltpu.VMEM((total, pair_ch), F32),
            pltpu.VMEM((LANES, wide), F32),
            pltpu.VMEM((groups, 2, seqs, LANES), F32),
            pltpu.VMEM((half, seqs, 2 * width), BF16),
        ],
    )(cols_a, cols_b, left, turned, part, weight, order, by_row, cot_cols)
    got = exchange([own] + messages[::-1], "cols", (1, 2, 3))
    update = call(
        update_kernel,
        shape((tokens, tokens, pair_ch), BF16),
        [pltpu.VMEM((tokens, tokens, pair_ch), F32)],
        flops=10**8,
    )(outer, final, bias)
    message = share + span + width
    back, own, *messages = call(
        functools.partial(between_kernel, rows=rows, share=share),
        (
            shape((span, LANES), F32),
            shape((message, LANES), F32),
            *[shape((message, LANES), BF16)] * (rows - 1),
        ),
        [
            pltpu.VMEM((rows * share + 2 * span + width, LANES), F32),
            pltpu.VMEM((cols, span, LANES), F32),
        ],
    )(own, *got[::-1])
    got = exchange([own] + messages[::-1], "rows", (1, 2, 3))
    from_left = call(functools.partial(to_unit, quarter=quarter), aligned, flops=10**8)(back, first)
    final_slope, first_slope, second_slope, alignment_slope = call(
        last_kernel,
        (
            shape((share, pair_ch), F32),
            shape((chans, width), F32),
            shape((chans, width), F32),
            aligned,
        ),
        [pltpu.VMEM((tokens, quarter, width), F32)],
    )(own, *got[::-1], from_left, xhat, spread, gain, second)
    return update, alignment_slope, final_slope, first_slope.T, second_slope.T


def fits(mesh, alignment_features, first_projector, final_projector):
    rows, cols = mesh.shape["rows"], mesh.shape["cols"]
    tokens = alignment_features.shape[0] // (mesh.shape["groups"] * rows)
    quarter = alignment_features.shape[1] // cols
    width, chans = first_projector.shape
    per = LANES // chans
    return (
        rows == cols == 4
        and chans * per == LANES
        and chans % per == 0
        and chans // per == SUBLANES
        and 2 * width == LANES
        and final_projector.shape[1] == LANES
        and quarter == SUBLANES
        and tokens % (2 * SUBLANES) == 0
        and quarter * cols == chans
        and chans // per * tokens == LANES
    )


def solution(mesh):
    in_specs = (
        P(("groups", "rows"), "cols", None),
        P(),
        P(),
        P(),
        P(),
        P(),
        P(),
        P(("groups", "rows"), "cols", None),
    )
    out_specs = (
        P(("groups", "rows"), "cols", None),
        P(("groups", "rows"), "cols", None),
        P(("groups", "rows", "cols"), None),
        P("groups", None),
        P("groups", None),
    )

    def whole(*args):
        square = fits(mesh, args[0], args[3], args[5])
        step = jax.shard_map(
            local_square if square else local_general,
            mesh=mesh,
            in_specs=in_specs,
            out_specs=out_specs,
            check_vma=False,
        )
        return step(*args)

    return whole
```

```python
import functools
import itertools

import jax
import jax.numpy as jnp
from jax import lax
from jax.experimental import pallas as pl
from jax.experimental.pallas import tpu as pltpu
from jax.sharding import PartitionSpec as P


def layernorm_parts(alignment_features, affine_factor, affine_offset):
    centered_alignment = alignment_features - jnp.mean(alignment_features, axis=-1, keepdims=True)
    reciprocal_spread = lax.rsqrt(
        jnp.mean(centered_alignment * centered_alignment, axis=-1, keepdims=True) + 1e-05
    )
    zscored_alignment = centered_alignment * reciprocal_spread
    return (
        zscored_alignment,
        reciprocal_spread,
        (zscored_alignment * affine_factor + affine_offset).astype(jnp.bfloat16),
    )


def local_general(
    alignment_features,
    affine_factor,
    affine_offset,
    first_projector,
    second_projector,
    final_projector,
    additive_term,
    adjoint_update,
):
    zscored_alignment, reciprocal_spread, unit_alignment = layernorm_parts(
        alignment_features, affine_factor, affine_offset
    )
    first_factor_here = jnp.dot(
        unit_alignment, first_projector, preferred_element_type=jnp.float32
    ).astype(jnp.bfloat16)
    second_factor_here = jnp.dot(
        unit_alignment, second_projector, preferred_element_type=jnp.float32
    ).astype(jnp.bfloat16)
    tokens, quarter, chans = first_factor_here.shape
    left_flat = first_factor_here.reshape(tokens, quarter * chans)
    right_flat = second_factor_here.reshape(tokens, quarter * chans)
    left_wide, right_wide = (
        lax.all_gather(left_flat, "cols", axis=1, tiled=True),
        lax.all_gather(right_flat, "cols", axis=1, tiled=True),
    )
    left_rows = left_wide.reshape(tokens, -1, chans)
    right_all = lax.all_gather(right_wide, "rows", axis=0, tiled=True)
    block = right_all.shape[0] // lax.axis_size("cols")
    right_cols = lax.dynamic_slice_in_dim(
        right_all, lax.axis_index("cols") * block, block, 0
    ).reshape(block, -1, chans)
    seqs = left_rows.shape[1]
    multiplier = 1.0 / seqs
    pair_ch = adjoint_update.shape[2]
    step_rows = 4
    rounds = tokens // step_rows
    first_tile_list = left_rows.reshape(rounds, step_rows, seqs, chans)
    cot_blocks = adjoint_update.reshape(rounds, step_rows, block, pair_ch)

    def advance(carry, inputs):
        right_acc, out_acc = carry
        left_slab, cot_slab = inputs
        outer = (
            jnp.einsum("isc,jsd->ijcd", left_slab, right_cols, preferred_element_type=jnp.float32)
            * multiplier
        ).astype(jnp.bfloat16)
        flat = outer.reshape(step_rows * block, chans * chans)
        cot_flat = cot_slab.reshape(step_rows * block, pair_ch)
        update = (
            jnp.dot(flat, final_projector, preferred_element_type=jnp.float32) + additive_term
        ).astype(jnp.bfloat16)
        outer_grad = jnp.dot(
            cot_flat, final_projector.T, preferred_element_type=jnp.float32
        ).astype(jnp.bfloat16)
        outer_grad = outer_grad.reshape(step_rows, block, chans, chans)
        left_piece = (
            jnp.einsum("ijcd,jsd->isc", outer_grad, right_cols, preferred_element_type=jnp.float32)
            * multiplier
        )
        right_acc = (
            right_acc
            + jnp.einsum("ijcd,isc->jsd", outer_grad, left_slab, preferred_element_type=jnp.float32)
            * multiplier
        )
        out_acc = out_acc + jnp.einsum(
            "fk,fe->ke", flat, cot_flat, preferred_element_type=jnp.float32
        )
        return ((right_acc, out_acc), (update.reshape(step_rows, block, pair_ch), left_piece))

    beginning_position = (
        jnp.zeros((block, seqs, chans), jnp.float32),
        jnp.zeros((chans * chans, pair_ch), jnp.float32),
    )
    (right_part, out_term), (updates, left_pieces) = lax.scan(
        advance, beginning_position, (first_tile_list, cot_blocks)
    )
    residue_update = updates.reshape(tokens, block, pair_ch)
    left_part = left_pieces.reshape(tokens, seqs * chans)
    first_adjoint = lax.psum_scatter(left_part, "cols", scatter_dimension=1, tiled=True).reshape(
        tokens, quarter, chans
    )
    moved = lax.all_to_all(
        right_part.reshape(block, seqs * chans), "cols", split_axis=1, concat_axis=0, tiled=True
    )
    right_back = lax.psum_scatter(moved, "rows", scatter_dimension=0, tiled=True).reshape(
        tokens, quarter, chans
    )
    final_projector_slope = lax.psum_scatter(
        out_term, ("rows", "cols"), scatter_dimension=0, tiled=True
    )
    unit_broadcast = unit_alignment.astype(jnp.float32)
    high = lax.Precision.HIGHEST
    left_term = jnp.einsum("tsk,tsc->kc", unit_broadcast, first_adjoint, precision=high)
    right_term = jnp.einsum("tsk,tsc->kc", unit_broadcast, right_back, precision=high)
    first_projector_slope, second_projector_slope = lax.psum(
        (left_term, right_term), ("rows", "cols")
    )
    unit_adjoint = jnp.einsum(
        "tsc,kc->tsk", first_adjoint, first_projector.astype(jnp.float32), precision=high
    )
    unit_adjoint = unit_adjoint + jnp.einsum(
        "tsc,kc->tsk", right_back, second_projector.astype(jnp.float32), precision=high
    )
    scaled_alignment = unit_adjoint * affine_factor
    alignment_slope = reciprocal_spread * (
        scaled_alignment
        - jnp.mean(scaled_alignment, axis=-1, keepdims=True)
        - zscored_alignment * jnp.mean(scaled_alignment * zscored_alignment, axis=-1, keepdims=True)
    )
    return (
        residue_update,
        alignment_slope,
        final_projector_slope,
        first_projector_slope,
        second_projector_slope,
    )


F32, BF16 = jnp.float32, jnp.bfloat16
LANES, SUBLANES = 128, 8


def dot(a, b, at=1, bt=0):
    return lax.dot_general(a, b, (((at,), (bt,)), ((), ())), preferred_element_type=F32)


def lane_group(shape, size):
    return lax.broadcasted_iota(jnp.int32, shape, len(shape) - 1) // size


def pick(parts, group):
    out = parts[-1]
    for b in range(len(parts) - 2, -1, -1):
        out = jnp.where(group == b, parts[b], out)
    return out


def normalise(x):
    centered = x - jnp.mean(x, axis=-1, keepdims=True)
    spread = lax.rsqrt(jnp.mean(centered * centered, axis=-1, keepdims=True) + 1e-05)
    return centered * spread, spread


def call(kernel, out_shape, scratch=(), flops=0, space=pltpu.VMEM):
    place = pl.BlockSpec(memory_space=space)
    on_chip = pl.BlockSpec(memory_space=pltpu.VMEM)

    def run(*args):
        return pl.pallas_call(
            kernel,
            out_shape=out_shape,
            in_specs=[place] * len(args),
            out_specs=jax.tree.map(lambda _: on_chip, out_shape),
            scratch_shapes=list(scratch),
            cost_estimate=pl.CostEstimate(flops=flops, bytes_accessed=0, transcendentals=0),
            compiler_params=pltpu.CompilerParams(vmem_limit_bytes=16 * 2**20),
        )(*args)

    return run


def norm_kernel(*refs):
    x_ref, offset_ref, sems = refs[-3:]
    count = sems.shape[0]
    sources, (out_ref, xhat_ref, spread_ref) = refs[:count], refs[count : count + 3]
    kept = (x_ref, offset_ref) + refs[count + 3 : -3]
    copies = [
        pltpu.make_async_copy(source, ref, sems.at[n])
        for n, (source, ref) in enumerate(zip(sources, kept))
    ]
    for copy in copies:
        copy.start()
    for copy in copies[:3]:
        copy.wait()
    tokens, quarter, width = x_ref.shape
    xhat, spread = normalise(x_ref[...].reshape(tokens * quarter, width))
    xhat_ref[...] = xhat
    spread_ref[...] = jnp.broadcast_to(spread, xhat.shape)
    unit = xhat * kept[2][...] + offset_ref[...]
    half = tokens * quarter // 2
    out_ref[...] = jnp.concatenate([unit[:half], unit[half:]], axis=1).astype(BF16)
    for copy in copies[3:]:
        copy.wait()


def grad_kernel(
    cot_ref, final_ref, first_ref, second_ref,
    by_col_ref, by_row_ref, cot_cols_ref, weight_ref, order_ref,
    cot_f, final_f,
    *, chans,
):
    tokens, block, _ = cot_ref.shape
    steps = by_col_ref.shape[0] // tokens
    per = LANES // chans
    cot = cot_ref[...]
    final = final_ref[...]
    cot_f[...] = cot.astype(F32)
    final_f[...] = final.astype(F32)
    for j in range(block):
        cot_cols_ref[j * tokens : (j + 1) * tokens, :] = cot_f[:, j, :].astype(BF16)
    cot_cols = cot_cols_ref[...]
    cot_rows = cot.reshape(tokens * block, cot.shape[2])
    for a in range(steps):
        got = dot(cot_cols, final[a * LANES : (a + 1) * LANES], 1, 1).astype(BF16)
        for j in range(block):
            by_col_ref[a * tokens : (a + 1) * tokens, j * LANES : (j + 1) * LANES] = got[
                j * tokens : (j + 1) * tokens
            ]
        lanes_dc = jnp.concatenate(
            [final_f[pl.ds(a * per + b, chans, stride=chans), :] for b in range(per)], axis=0
        ).astype(BF16)
        got = dot(cot_rows, lanes_dc, 1, 1).astype(BF16)
        for i in range(tokens):
            by_row_ref[a * block : (a + 1) * block, i * LANES : (i + 1) * LANES] = got[
                i * block : (i + 1) * block
            ]
    for x, ref in enumerate((first_ref, second_ref)):
        projector = ref[...]
        zero = jnp.zeros_like(projector)
        halves = [
            jnp.concatenate([projector, zero], axis=1),
            jnp.concatenate([zero, projector], axis=1),
        ]
        empty = jnp.concatenate([zero, zero], axis=1)
        for b in range(per):
            for h in range(2):
                for other in range(per):
                    at = (((x * 2) + h) * per + other) * chans
                    weight_ref[b, at : at + chans, :] = halves[h] if other == b else empty
    size = tokens * chans
    for b in range(per):
        row = lax.broadcasted_iota(jnp.int32, (size, LANES), 0)
        lane = lax.broadcasted_iota(jnp.int32, (size, LANES), 1)
        wanted = lane % tokens * chans + lane // tokens * per + b
        order_ref[:, b * LANES : (b + 1) * LANES] = jnp.where(row == wanted, 1.0, 0.0).astype(BF16)


def half_kernel(own_ref, other_ref, out_ref, unit_f):
    low = lax.axis_index("cols") % 2
    half, seqs, lanes = unit_f.shape
    quarter = seqs // 2
    for k, ref in enumerate((own_ref, other_ref)):
        at = pl.multiple_of((low ^ k) * quarter, quarter)
        unit_f[:, pl.ds(at, quarter), :] = ref[...].astype(F32).reshape(half, quarter, lanes)
    out_ref[...] = unit_f[...].reshape(half * seqs, lanes).astype(BF16)


def join(first_half, refs, unit_ref):
    half, seqs, lanes = unit_ref.shape
    for k, ref in enumerate(refs):
        at = pl.multiple_of((first_half ^ k) * (seqs // 2), seqs // 2)
        unit_ref[:, pl.ds(at, seqs // 2), :] = ref[...].reshape(half, seqs // 2, lanes)
    return unit_ref[...].reshape(half * seqs, lanes)


def project(unit, weight_ref, x, seqs, per):
    half = unit.shape[0] // seqs
    by_group = unit.reshape(half // per, per, seqs, unit.shape[1])
    size = weight_ref.shape[1] // 2
    total = None
    for b in range(per):
        part = by_group[:, b].reshape(half // per * seqs, unit.shape[1])
        got = dot(part, weight_ref[b, x * size : (x + 1) * size, :], 1, 1)
        total = got if total is None else total + got
    total = total.astype(BF16)
    count = half // per
    return [
        total[p % count * seqs : (p % count + 1) * seqs, p // count * LANES : (p // count + 1) * LANES]
        for p in range(2 * count)
    ]


def reorder(tiles, order_ref):
    wide = dot(jnp.concatenate(tiles, axis=1), order_ref[...])
    count = wide.shape[1] // LANES
    return jnp.concatenate([wide[:, b * LANES : (b + 1) * LANES] for b in range(count)], axis=0)


def fold(spread_ref, seqs, chans, tokens):
    per = LANES // chans
    group = lane_group((seqs, LANES), chans)
    out = []
    for p in range(tokens // per):
        total = None
        for shift in range(per):
            parts = []
            for b in range(per):
                t = p * per + (b + shift) % per
                parts.append(spread_ref[b * seqs : (b + 1) * seqs, t * LANES : (t + 1) * LANES])
            part = pick(parts, group)
            if shift:
                part = pltpu.roll(part, shift * chans, 1)
            total = part if total is None else total + part
        out.append(total)
    return out


def slope(unit_turned, tiles, per, chans):
    seqs = tiles[0].shape[0]
    count = len(tiles) // 2
    group = lane_group((seqs, LANES), chans)
    rows = []
    for p in range(count):
        for b in range(per):
            rows.append(
                jnp.concatenate(
                    [jnp.where(group == b, tiles[h * count + p], 0.0) for h in range(2)], axis=1
                )
            )
    got = dot(unit_turned, jnp.concatenate(rows, axis=0).astype(BF16))
    width = unit_turned.shape[0] // 2
    return got[:width, :LANES] + got[width:, LANES:]


def left_kernel(
    u0, u1, weight_ref, order_ref, by_col_ref, left_ref, turned_ref, part_ref, unit_ref, spread_f,
    *, chans,
):
    per = LANES // chans
    half, seqs, _ = unit_ref.shape
    tokens = 2 * half
    unit = join(lax.axis_index("cols") // 2, (u0, u1), unit_ref)
    turned_ref[...] = unit.astype(F32).T.astype(BF16)
    turned = reorder(project(unit, weight_ref, 0, seqs, per), order_ref)
    left_ref[...] = turned.T.astype(BF16)
    spread_f[...] = dot(turned.astype(BF16), by_col_ref[...])
    for p, tile in enumerate(fold(spread_f, seqs, chans, tokens)):
        part_ref[p] = tile * (1.0 / seqs)


def pair_kernel(
    u0, u1, left_ref, turned_ref, part_ref, weight_ref, order_ref, by_row_ref, cot_cols_ref,
    outer_ref, own_ref, m3, m2, m1,
    block_ref, slope_f, spread_f, both_f, unit_ref,
    *, chans, sizes, first_halves,
):
    per, steps = LANES // chans, chans // (LANES // chans)
    rows, cols = sizes
    half, seqs, _ = unit_ref.shape
    tokens = 2 * half
    groups = tokens // per
    quarter = seqs // cols
    share = slope_f.shape[0] // (rows * cols)
    mine = lax.axis_index("cols")
    group = lane_group((seqs, LANES), chans)
    place = lax.axis_index("rows") * cols + mine
    unit = join((first_halves >> place) & 1, (u0, u1), unit_ref)
    right = project(unit, weight_ref, 1, seqs, per)
    for p, tile in enumerate(right):
        tile = tile.astype(F32)
        rolled = [pltpu.roll(tile, s * chans, 1) if s else tile for s in range(per)]
        for own in range(per):
            j = p * per + own
            for b in range(per):
                block_ref[b * seqs : (b + 1) * seqs, j * LANES : (j + 1) * LANES] = jnp.where(
                    group == b, rolled[(b - own) % per], 0.0
                ).astype(BF16)
    left = left_ref[...]
    for p in range(groups):
        span = per * LANES
        got = dot(left, block_ref[:, p * span : (p + 1) * span])
        got = (got * (1.0 / seqs)).astype(BF16)
        for own in range(per):
            j = p * per + own
            for a in range(steps):
                outer_ref[j * tokens : (j + 1) * tokens, a * LANES : (a + 1) * LANES] = got[
                    a * tokens : (a + 1) * tokens, own * LANES : (own + 1) * LANES
                ]
    spread_f[...] = dot(reorder(right, order_ref).astype(BF16), by_row_ref[...])
    slope_f[...] = dot(outer_ref[...], cot_cols_ref[...], 0, 0)
    lefts = [tile * (1.0 / seqs) for tile in fold(spread_f, seqs, chans, tokens)]
    rights = [part_ref[p] for p in range(groups)]
    for p in range(groups):
        both_f[p, 0] = lefts[p]
        both_f[p, 1] = rights[p]
    sides = [
        slope(turned_ref[...], lefts, per, chans),
        slope(unit.astype(F32).T.astype(BF16), rights, per, chans),
    ]
    sides = [s + pltpu.roll(s, LANES // 2, 1) for s in sides]
    sides = [s + pltpu.roll(s, LANES // 4, 1) for s in sides]
    width = sides[0].shape[0] // 2
    slopes = pick(
        [side[h * width : (h + 1) * width] for h in range(2) for side in sides],
        lane_group((width, LANES), chans),
    )
    for k, ref in enumerate((own_ref, m1, m2, m3)):
        peer = mine ^ k
        kind = ref.dtype
        for r in range(rows):
            at = pl.multiple_of((r * cols + peer) * share, share)
            ref[r * share : (r + 1) * share, :] = slope_f[pl.ds(at, share), :].astype(kind)
        base = rows * share
        at = pl.multiple_of(peer * quarter, quarter)
        span = groups * quarter
        for x in range(2):
            ref[base + x * span : base + (x + 1) * span, :] = (
                both_f[:, x, pl.ds(at, quarter), :].reshape(span, LANES).astype(kind)
            )
        base += 2 * span
        ref[base : base + width, :] = slopes.astype(kind)


def update_kernel(outer_ref, final_ref, bias_ref, update_ref, update_f):
    tokens = update_ref.shape[0]
    update = dot(outer_ref[...], final_ref[...]) + bias_ref[...]
    for j in range(update_ref.shape[1]):
        update_f[:, j, :] = update[j * tokens : (j + 1) * tokens]
    update_ref[...] = update_f[...].astype(BF16)


def between_kernel(
    own_ref, r3, r2, r1, left_ref, next_ref, m3, m2, m1, total_f, right_f, *, rows, share
):
    refs = (own_ref, r1, r2, r3)
    span = left_ref.shape[0]
    first = rows * share
    last = first + 2 * span
    mine, column = lax.axis_index("rows"), lax.axis_index("cols")
    for k, ref in enumerate(refs):
        right_f[column ^ k] = ref[first + span : last, :].astype(F32)
    for start, stop in ((0, first + span), (last, total_f.shape[0])):
        total = own_ref[start:stop, :]
        for ref in refs[1:]:
            total = total + ref[start:stop, :].astype(F32)
        total_f[start:stop, :] = total
    left_ref[...] = total_f[first : first + span, :]
    slopes = total_f[last:, :]
    for k, ref in enumerate((next_ref, m1, m2, m3)):
        peer = mine ^ k
        at = pl.multiple_of(peer * share, share)
        ref[0:share, :] = total_f[pl.ds(at, share), :].astype(ref.dtype)
        ref[share : share + span, :] = right_f[peer].astype(ref.dtype)
        ref[share + span :, :] = slopes.astype(ref.dtype)


def to_unit(back, projector_ref, unit_ref, quarter):
    back = back[...]
    projector = projector_ref[...]
    chans = projector.shape[0]
    high = back.astype(BF16)
    low = (back - high.astype(F32)).astype(BF16)
    zero = jnp.zeros_like(projector)
    per = LANES // chans
    for b in range(per):
        weights = jnp.concatenate([projector if i == b else zero for i in range(per)], axis=0)
        got = dot(high, weights) + dot(low, weights)
        for p in range(back.shape[0] // quarter):
            unit_ref[p * per + b] = got[p * quarter : (p + 1) * quarter]


def last_kernel(
    own_ref, r3, r2, r1, unit_ref, xhat_ref, spread_ref, gain_ref, second_ref,
    final_ref, first_slope_ref, second_slope_ref, out_ref, unit_f,
):
    total = own_ref[...] + r1[...].astype(F32) + r2[...].astype(F32) + r3[...].astype(F32)
    share = final_ref.shape[0]
    final_ref[...] = total[:share]
    tokens, quarter, width = out_ref.shape
    span = tokens * quarter * second_ref.shape[0] // LANES
    to_unit(total[share : share + span], second_ref, unit_f, quarter)
    g = (unit_ref[...] + unit_f[...]).reshape(tokens * quarter, width) * gain_ref[...]
    xhat = xhat_ref[...]
    out = spread_ref[...] * (
        g
        - jnp.mean(g, axis=-1, keepdims=True)
        - xhat * jnp.mean(g * xhat, axis=-1, keepdims=True)
    )
    out_ref[...] = out.reshape(tokens, quarter, width)
    slopes = total[share + span :].T
    chans = second_ref.shape[0]
    for x, ref in enumerate((first_slope_ref, second_slope_ref)):
        ref[...] = jnp.concatenate(
            [slopes[(2 * h + x) * chans : (2 * h + x + 1) * chans] for h in range(2)], axis=1
        )


def exchange(messages, axis, order):
    size = lax.axis_size(axis)
    got = {}
    for k in order:
        got[k] = lax.ppermute(messages[k], axis, [(p, p ^ k) for p in range(size)])
    return [got[k] for k in sorted(got)]


def holders(rows, cols):
    first, second, mask = [], [], 0
    for r in range(rows):

        def hops(to):
            return [abs(z - r) + (q // 2 != r // 2) for q, z in enumerate(to) if z != r]

        best = None
        for a in itertools.permutations(range(rows)):
            for b in itertools.permutations(range(rows)):
                if any(a.index(z) // 2 == b.index(z) // 2 for z in range(rows)):
                    continue
                cost = (max(hops(a) + hops(b)), sum(hops(a) + hops(b)))
                if best is None or cost < best[0]:
                    best = cost, a, b
        _, a, b = best
        first += [(r * cols + q, z * cols + r) for q, z in enumerate(a)]
        second += [(r * cols + q, z * cols + r) for q, z in enumerate(b)]
        for q, z in enumerate(a):
            mask |= q // 2 << (z * cols + r)
    return first, second, mask


def local_square(*args):
    return local_square_(*args)


def local_square_(
    alignment_features,
    affine_factor,
    affine_offset,
    first_projector,
    second_projector,
    final_projector,
    additive_term,
    adjoint_update,
):
    rows, cols = lax.axis_size("rows"), lax.axis_size("cols")
    tokens, quarter, width = alignment_features.shape
    chans = first_projector.shape[1]
    total, pair_ch = final_projector.shape
    seqs = quarter * cols
    per, steps = LANES // chans, chans // (LANES // chans)
    share = total // (rows * cols)
    shape = jax.ShapeDtypeStruct
    wide, tall = tokens * LANES, steps * tokens
    groups = tokens // per
    half = tokens // 2
    aligned = shape((tokens, quarter, width), F32)
    flat = shape((tokens * quarter, width), F32)
    inputs = [
        alignment_features,
        affine_offset.reshape(1, width),
        affine_factor.reshape(1, width),
        adjoint_update,
        final_projector,
        first_projector.T,
        second_projector.T,
        additive_term.reshape(1, pair_ch),
    ]
    unit, xhat, spread, gain, cot, final, first, second, bias = call(
        norm_kernel,
        [shape((half * quarter, 2 * width), BF16), flat, flat]
        + [shape(i.shape, i.dtype) for i in inputs[2:]],
        [pltpu.VMEM(i.shape, i.dtype) for i in inputs[:2]]
        + [pltpu.SemaphoreType.DMA((len(inputs),))],
        space=pltpu.HBM,
    )(*[pltpu.with_memory_space_constraint(i, pltpu.HBM) for i in inputs])
    partner = lax.ppermute(unit, "cols", [(p, p ^ 1) for p in range(cols)])
    halves = call(
        half_kernel,
        shape((half * seqs // 2, 2 * width), BF16),
        [pltpu.VMEM((half, seqs // 2, 2 * width), F32)],
    )(unit, partner)
    from_first, from_second, first_halves = holders(rows, cols)
    cols_a = lax.ppermute(halves, ("rows", "cols"), from_first)
    cols_b = lax.ppermute(halves, ("rows", "cols"), from_second)
    across = lax.ppermute(halves, "cols", [(p, p ^ 2) for p in range(cols)])
    grad = call(
        functools.partial(grad_kernel, chans=chans),
        (
            shape((tall, wide), BF16),
            shape((tall, wide), BF16),
            shape((tokens * tokens, pair_ch), BF16),
            shape((per, 4 * LANES, 2 * width), BF16),
            shape((tokens * chans, per * LANES), BF16),
        ),
        [pltpu.VMEM(adjoint_update.shape, F32), pltpu.VMEM((total, pair_ch), F32)],
        flops=8 * tokens * tokens * total * pair_ch,
    )
    by_col, by_row, cot_cols, weight, order = grad(cot, final, first, second)
    left, turned, part = call(
        functools.partial(left_kernel, chans=chans),
        (
            shape((tall, LANES), BF16),
            shape((2 * width, half * seqs), BF16),
            shape((groups, seqs, LANES), F32),
        ),
        [pltpu.VMEM((half, seqs, 2 * width), BF16), pltpu.VMEM((LANES, wide), F32)],
        flops=10**8,
    )(halves, across, weight, order, by_col)
    span = groups * quarter
    message = rows * share + 2 * span + width // 2
    outer, own, *messages = call(
        functools.partial(
            pair_kernel, chans=chans, sizes=(rows, cols), first_halves=first_halves
        ),
        (
            shape((tokens * tokens, total), BF16),
            shape((message, LANES), F32),
            *[shape((message, LANES), BF16)] * (cols - 1),
        ),
        [
            pltpu.VMEM((LANES, wide), BF16),
            pltpu.VMEM((total, pair_ch), F32),
            pltpu.VMEM((LANES, wide), F32),
            pltpu.VMEM((groups, 2, seqs, LANES), F32),
            pltpu.VMEM((half, seqs, 2 * width), BF16),
        ],
    )(cols_a, cols_b, left, turned, part, weight, order, by_row, cot_cols)
    got = exchange([own] + messages[::-1], "cols", (1, 2, 3))
    update = call(
        update_kernel,
        shape((tokens, tokens, pair_ch), BF16),
        [pltpu.VMEM((tokens, tokens, pair_ch), F32)],
        flops=10**8,
    )(outer, final, bias)
    message = share + span + width // 2
    back, own, *messages = call(
        functools.partial(between_kernel, rows=rows, share=share),
        (
            shape((span, LANES), F32),
            shape((message, LANES), F32),
            *[shape((message, LANES), BF16)] * (rows - 1),
        ),
        [
            pltpu.VMEM((rows * share + 2 * span + width // 2, LANES), F32),
            pltpu.VMEM((cols, span, LANES), F32),
        ],
    )(own, *got[::-1])
    got = exchange([own] + messages[::-1], "rows", (1, 2, 3))
    from_left = call(functools.partial(to_unit, quarter=quarter), aligned, flops=10**8)(back, first)
    final_slope, first_slope, second_slope, alignment_slope = call(
        last_kernel,
        (
            shape((share, pair_ch), F32),
            shape((chans, width), F32),
            shape((chans, width), F32),
            aligned,
        ),
        [pltpu.VMEM((tokens, quarter, width), F32)],
    )(own, *got[::-1], from_left, xhat, spread, gain, second)
    return update, alignment_slope, final_slope, first_slope.T, second_slope.T


def fits(mesh, alignment_features, first_projector, final_projector):
    rows, cols = mesh.shape["rows"], mesh.shape["cols"]
    tokens = alignment_features.shape[0] // (mesh.shape["groups"] * rows)
    quarter = alignment_features.shape[1] // cols
    width, chans = first_projector.shape
    per = LANES // chans
    return (
        rows == cols == 4
        and chans * per == LANES
        and chans % per == 0
        and chans // per == SUBLANES
        and 2 * width == LANES
        and final_projector.shape[1] == LANES
        and quarter == SUBLANES
        and tokens % (2 * SUBLANES) == 0
        and quarter * cols == chans
        and chans // per * tokens == LANES
    )


def solution(mesh):
    in_specs = (
        P(("groups", "rows"), "cols", None),
        P(),
        P(),
        P(),
        P(),
        P(),
        P(),
        P(("groups", "rows"), "cols", None),
    )
    out_specs = (
        P(("groups", "rows"), "cols", None),
        P(("groups", "rows"), "cols", None),
        P(("groups", "rows", "cols"), None),
        P("groups", None),
        P("groups", None),
    )

    def whole(*args):
        square = fits(mesh, args[0], args[3], args[5])
        step = jax.shard_map(
            local_square if square else local_general,
            mesh=mesh,
            in_specs=in_specs,
            out_specs=out_specs,
            check_vma=False,
        )
        return step(*args)

    return whole
```

```python
import functools

import jax
import jax.numpy as jnp
from jax import lax
from jax.experimental import pallas as pl
from jax.experimental.pallas import tpu as pltpu
from jax.sharding import PartitionSpec as P


def layernorm_parts(alignment_features, affine_factor, affine_offset):
    centered_alignment = alignment_features - jnp.mean(alignment_features, axis=-1, keepdims=True)
    reciprocal_spread = lax.rsqrt(
        jnp.mean(centered_alignment * centered_alignment, axis=-1, keepdims=True) + 1e-05
    )
    zscored_alignment = centered_alignment * reciprocal_spread
    return (
        zscored_alignment,
        reciprocal_spread,
        (zscored_alignment * affine_factor + affine_offset).astype(jnp.bfloat16),
    )


def local_general(
    alignment_features,
    affine_factor,
    affine_offset,
    first_projector,
    second_projector,
    final_projector,
    additive_term,
    adjoint_update,
):
    zscored_alignment, reciprocal_spread, unit_alignment = layernorm_parts(
        alignment_features, affine_factor, affine_offset
    )
    first_factor_here = jnp.dot(
        unit_alignment, first_projector, preferred_element_type=jnp.float32
    ).astype(jnp.bfloat16)
    second_factor_here = jnp.dot(
        unit_alignment, second_projector, preferred_element_type=jnp.float32
    ).astype(jnp.bfloat16)
    tokens, quarter, chans = first_factor_here.shape
    left_flat = first_factor_here.reshape(tokens, quarter * chans)
    right_flat = second_factor_here.reshape(tokens, quarter * chans)
    left_wide, right_wide = (
        lax.all_gather(left_flat, "cols", axis=1, tiled=True),
        lax.all_gather(right_flat, "cols", axis=1, tiled=True),
    )
    left_rows = left_wide.reshape(tokens, -1, chans)
    right_all = lax.all_gather(right_wide, "rows", axis=0, tiled=True)
    block = right_all.shape[0] // lax.axis_size("cols")
    right_cols = lax.dynamic_slice_in_dim(
        right_all, lax.axis_index("cols") * block, block, 0
    ).reshape(block, -1, chans)
    seqs = left_rows.shape[1]
    multiplier = 1.0 / seqs
    pair_ch = adjoint_update.shape[2]
    step_rows = 4
    rounds = tokens // step_rows
    first_tile_list = left_rows.reshape(rounds, step_rows, seqs, chans)
    cot_blocks = adjoint_update.reshape(rounds, step_rows, block, pair_ch)

    def advance(carry, inputs):
        right_acc, out_acc = carry
        left_slab, cot_slab = inputs
        outer = (
            jnp.einsum("isc,jsd->ijcd", left_slab, right_cols, preferred_element_type=jnp.float32)
            * multiplier
        ).astype(jnp.bfloat16)
        flat = outer.reshape(step_rows * block, chans * chans)
        cot_flat = cot_slab.reshape(step_rows * block, pair_ch)
        update = (
            jnp.dot(flat, final_projector, preferred_element_type=jnp.float32) + additive_term
        ).astype(jnp.bfloat16)
        outer_grad = jnp.dot(
            cot_flat, final_projector.T, preferred_element_type=jnp.float32
        ).astype(jnp.bfloat16)
        outer_grad = outer_grad.reshape(step_rows, block, chans, chans)
        left_piece = (
            jnp.einsum("ijcd,jsd->isc", outer_grad, right_cols, preferred_element_type=jnp.float32)
            * multiplier
        )
        right_acc = (
            right_acc
            + jnp.einsum("ijcd,isc->jsd", outer_grad, left_slab, preferred_element_type=jnp.float32)
            * multiplier
        )
        out_acc = out_acc + jnp.einsum(
            "fk,fe->ke", flat, cot_flat, preferred_element_type=jnp.float32
        )
        return ((right_acc, out_acc), (update.reshape(step_rows, block, pair_ch), left_piece))

    beginning_position = (
        jnp.zeros((block, seqs, chans), jnp.float32),
        jnp.zeros((chans * chans, pair_ch), jnp.float32),
    )
    (right_part, out_term), (updates, left_pieces) = lax.scan(
        advance, beginning_position, (first_tile_list, cot_blocks)
    )
    residue_update = updates.reshape(tokens, block, pair_ch)
    left_part = left_pieces.reshape(tokens, seqs * chans)
    first_adjoint = lax.psum_scatter(left_part, "cols", scatter_dimension=1, tiled=True).reshape(
        tokens, quarter, chans
    )
    moved = lax.all_to_all(
        right_part.reshape(block, seqs * chans), "cols", split_axis=1, concat_axis=0, tiled=True
    )
    right_back = lax.psum_scatter(moved, "rows", scatter_dimension=0, tiled=True).reshape(
        tokens, quarter, chans
    )
    final_projector_slope = lax.psum_scatter(
        out_term, ("rows", "cols"), scatter_dimension=0, tiled=True
    )
    unit_broadcast = unit_alignment.astype(jnp.float32)
    high = lax.Precision.HIGHEST
    left_term = jnp.einsum("tsk,tsc->kc", unit_broadcast, first_adjoint, precision=high)
    right_term = jnp.einsum("tsk,tsc->kc", unit_broadcast, right_back, precision=high)
    first_projector_slope, second_projector_slope = lax.psum(
        (left_term, right_term), ("rows", "cols")
    )
    unit_adjoint = jnp.einsum(
        "tsc,kc->tsk", first_adjoint, first_projector.astype(jnp.float32), precision=high
    )
    unit_adjoint = unit_adjoint + jnp.einsum(
        "tsc,kc->tsk", right_back, second_projector.astype(jnp.float32), precision=high
    )
    scaled_alignment = unit_adjoint * affine_factor
    alignment_slope = reciprocal_spread * (
        scaled_alignment
        - jnp.mean(scaled_alignment, axis=-1, keepdims=True)
        - zscored_alignment * jnp.mean(scaled_alignment * zscored_alignment, axis=-1, keepdims=True)
    )
    return (
        residue_update,
        alignment_slope,
        final_projector_slope,
        first_projector_slope,
        second_projector_slope,
    )


F32, BF16 = jnp.float32, jnp.bfloat16
LANES, SUBLANES = 128, 8


def dot(a, b, at=1, bt=0):
    return lax.dot_general(a, b, (((at,), (bt,)), ((), ())), preferred_element_type=F32)


def lane_group(shape, size):
    return lax.broadcasted_iota(jnp.int32, shape, len(shape) - 1) // size


def pick(parts, group):
    out = parts[-1]
    for b in range(len(parts) - 2, -1, -1):
        out = jnp.where(group == b, parts[b], out)
    return out


def normalise(x):
    centered = x - jnp.mean(x, axis=-1, keepdims=True)
    spread = lax.rsqrt(jnp.mean(centered * centered, axis=-1, keepdims=True) + 1e-05)
    return centered * spread, spread


def call(kernel, out_shape, scratch=(), flops=0, space=pltpu.VMEM):
    place = pl.BlockSpec(memory_space=space)
    on_chip = pl.BlockSpec(memory_space=pltpu.VMEM)

    def run(*args):
        return pl.pallas_call(
            kernel,
            out_shape=out_shape,
            in_specs=[place] * len(args),
            out_specs=jax.tree.map(lambda _: on_chip, out_shape),
            scratch_shapes=list(scratch),
            cost_estimate=pl.CostEstimate(flops=flops, bytes_accessed=0, transcendentals=0),
            compiler_params=pltpu.CompilerParams(vmem_limit_bytes=16 * 2**20),
        )(*args)

    return run


def norm_kernel(*refs):
    x_ref, offset_ref, sems = refs[-3:]
    count = sems.shape[0]
    sources, (out_ref, xhat_ref, spread_ref) = refs[:count], refs[count : count + 3]
    kept = (x_ref, offset_ref) + refs[count + 3 : -3]
    copies = [
        pltpu.make_async_copy(source, ref, sems.at[n])
        for n, (source, ref) in enumerate(zip(sources, kept))
    ]
    for copy in copies:
        copy.start()
    for copy in copies[:3]:
        copy.wait()
    tokens, quarter, width = x_ref.shape
    xhat, spread = normalise(x_ref[...].reshape(tokens * quarter, width))
    xhat_ref[...] = xhat
    spread_ref[...] = jnp.broadcast_to(spread, xhat.shape)
    unit = xhat * kept[2][...] + offset_ref[...]
    half = tokens * quarter // 2
    out_ref[...] = jnp.concatenate([unit[:half], unit[half:]], axis=1).astype(BF16)
    for copy in copies[3:]:
        copy.wait()


def grad_kernel(
    cot_ref, final_ref, first_ref, second_ref,
    by_col_ref, by_row_ref, cot_cols_ref, weight_ref, order_ref,
    cot_f, final_f,
    *, chans,
):
    tokens, block, _ = cot_ref.shape
    steps = by_col_ref.shape[0] // tokens
    per = LANES // chans
    cot = cot_ref[...]
    final = final_ref[...]
    cot_f[...] = cot.astype(F32)
    final_f[...] = final.astype(F32)
    for j in range(block):
        cot_cols_ref[j * tokens : (j + 1) * tokens, :] = cot_f[:, j, :].astype(BF16)
    cot_cols = cot_cols_ref[...]
    cot_rows = cot.reshape(tokens * block, cot.shape[2])
    for a in range(steps):
        got = dot(cot_cols, final[a * LANES : (a + 1) * LANES], 1, 1).astype(BF16)
        for j in range(block):
            by_col_ref[a * tokens : (a + 1) * tokens, j * LANES : (j + 1) * LANES] = got[
                j * tokens : (j + 1) * tokens
            ]
        lanes_dc = jnp.concatenate(
            [final_f[pl.ds(a * per + b, chans, stride=chans), :] for b in range(per)], axis=0
        ).astype(BF16)
        got = dot(cot_rows, lanes_dc, 1, 1).astype(BF16)
        for i in range(tokens):
            by_row_ref[a * block : (a + 1) * block, i * LANES : (i + 1) * LANES] = got[
                i * block : (i + 1) * block
            ]
    for x, ref in enumerate((first_ref, second_ref)):
        projector = ref[...]
        zero = jnp.zeros_like(projector)
        halves = [
            jnp.concatenate([projector, zero], axis=1),
            jnp.concatenate([zero, projector], axis=1),
        ]
        empty = jnp.concatenate([zero, zero], axis=1)
        for b in range(per):
            for h in range(2):
                for other in range(per):
                    at = (((x * 2) + h) * per + other) * chans
                    weight_ref[b, at : at + chans, :] = halves[h] if other == b else empty
    size = tokens * chans
    for b in range(per):
        row = lax.broadcasted_iota(jnp.int32, (size, LANES), 0)
        lane = lax.broadcasted_iota(jnp.int32, (size, LANES), 1)
        wanted = lane % tokens * chans + lane // tokens * per + b
        order_ref[:, b * LANES : (b + 1) * LANES] = jnp.where(row == wanted, 1.0, 0.0).astype(BF16)


def half_kernel(own_ref, other_ref, out_ref, unit_f):
    low = lax.axis_index("cols") % 2
    half, seqs, lanes = unit_f.shape
    quarter = seqs // 2
    for k, ref in enumerate((own_ref, other_ref)):
        at = pl.multiple_of((low ^ k) * quarter, quarter)
        unit_f[:, pl.ds(at, quarter), :] = ref[...].astype(F32).reshape(half, quarter, lanes)
    out_ref[...] = unit_f[...].reshape(half * seqs, lanes).astype(BF16)


def join(first_half, refs, unit_ref):
    half, seqs, lanes = unit_ref.shape
    for k, ref in enumerate(refs):
        at = pl.multiple_of((first_half ^ k) * (seqs // 2), seqs // 2)
        unit_ref[:, pl.ds(at, seqs // 2), :] = ref[...].reshape(half, seqs // 2, lanes)
    return unit_ref[...].reshape(half * seqs, lanes)


def project(unit, weight_ref, x, seqs, per):
    half = unit.shape[0] // seqs
    by_group = unit.reshape(half // per, per, seqs, unit.shape[1])
    size = weight_ref.shape[1] // 2
    total = None
    for b in range(per):
        part = by_group[:, b].reshape(half // per * seqs, unit.shape[1])
        got = dot(part, weight_ref[b, x * size : (x + 1) * size, :], 1, 1)
        total = got if total is None else total + got
    total = total.astype(BF16)
    count = half // per
    return [
        total[p % count * seqs : (p % count + 1) * seqs, p // count * LANES : (p // count + 1) * LANES]
        for p in range(2 * count)
    ]


def reorder(tiles, order_ref):
    wide = dot(jnp.concatenate(tiles, axis=1), order_ref[...])
    count = wide.shape[1] // LANES
    return jnp.concatenate([wide[:, b * LANES : (b + 1) * LANES] for b in range(count)], axis=0)


def fold(spread_ref, seqs, chans, tokens):
    per = LANES // chans
    group = lane_group((seqs, LANES), chans)
    out = []
    for p in range(tokens // per):
        total = None
        for shift in range(per):
            parts = []
            for b in range(per):
                t = p * per + (b + shift) % per
                parts.append(spread_ref[b * seqs : (b + 1) * seqs, t * LANES : (t + 1) * LANES])
            part = pick(parts, group)
            if shift:
                part = pltpu.roll(part, shift * chans, 1)
            total = part if total is None else total + part
        out.append(total)
    return out


def slope(unit_turned, tiles, per, chans):
    seqs = tiles[0].shape[0]
    count = len(tiles) // 2
    group = lane_group((seqs, LANES), chans)
    rows = []
    for p in range(count):
        for b in range(per):
            rows.append(
                jnp.concatenate(
                    [jnp.where(group == b, tiles[h * count + p], 0.0) for h in range(2)], axis=1
                )
            )
    got = dot(unit_turned, jnp.concatenate(rows, axis=0).astype(BF16))
    width = unit_turned.shape[0] // 2
    return got[:width, :LANES] + got[width:, LANES:]


def left_kernel(
    u0, u1, weight_ref, order_ref, by_col_ref, left_ref, turned_ref, part_ref, unit_ref, spread_f,
    *, chans,
):
    per = LANES // chans
    half, seqs, _ = unit_ref.shape
    tokens = 2 * half
    unit = join(lax.axis_index("cols") // 2, (u0, u1), unit_ref)
    turned_ref[...] = unit.astype(F32).T.astype(BF16)
    turned = reorder(project(unit, weight_ref, 0, seqs, per), order_ref)
    left_ref[...] = turned.T.astype(BF16)
    spread_f[...] = dot(turned.astype(BF16), by_col_ref[...])
    for p, tile in enumerate(fold(spread_f, seqs, chans, tokens)):
        part_ref[p] = tile * (1.0 / seqs)


def pair_kernel(
    u0, u1, left_ref, turned_ref, part_ref, weight_ref, order_ref, by_row_ref, cot_cols_ref,
    outer_ref, own_ref, m3, m2, m1,
    block_ref, slope_f, spread_f, both_f, unit_ref,
    *, chans, sizes, first_halves,
):
    per, steps = LANES // chans, chans // (LANES // chans)
    rows, cols = sizes
    half, seqs, _ = unit_ref.shape
    tokens = 2 * half
    groups = tokens // per
    quarter = seqs // cols
    share = slope_f.shape[0] // (rows * cols)
    mine = lax.axis_index("cols")
    group = lane_group((seqs, LANES), chans)
    place = lax.axis_index("rows") * cols + mine
    unit = join((first_halves >> place) & 1, (u0, u1), unit_ref)
    right = project(unit, weight_ref, 1, seqs, per)
    for p, tile in enumerate(right):
        tile = tile.astype(F32)
        rolled = [pltpu.roll(tile, s * chans, 1) if s else tile for s in range(per)]
        for own in range(per):
            j = p * per + own
            for b in range(per):
                block_ref[b * seqs : (b + 1) * seqs, j * LANES : (j + 1) * LANES] = jnp.where(
                    group == b, rolled[(b - own) % per], 0.0
                ).astype(BF16)
    left = left_ref[...]
    for p in range(groups):
        span = per * LANES
        got = dot(left, block_ref[:, p * span : (p + 1) * span])
        got = (got * (1.0 / seqs)).astype(BF16)
        for own in range(per):
            j = p * per + own
            for a in range(steps):
                outer_ref[j * tokens : (j + 1) * tokens, a * LANES : (a + 1) * LANES] = got[
                    a * tokens : (a + 1) * tokens, own * LANES : (own + 1) * LANES
                ]
    spread_f[...] = dot(reorder(right, order_ref).astype(BF16), by_row_ref[...])
    slope_f[...] = dot(outer_ref[...], cot_cols_ref[...], 0, 0)
    lefts = [tile * (1.0 / seqs) for tile in fold(spread_f, seqs, chans, tokens)]
    rights = [part_ref[p] for p in range(groups)]
    for p in range(groups):
        both_f[p, 0] = lefts[p]
        both_f[p, 1] = rights[p]
    sides = [
        slope(turned_ref[...], lefts, per, chans),
        slope(unit.astype(F32).T.astype(BF16), rights, per, chans),
    ]
    sides = [s + pltpu.roll(s, LANES // 2, 1) for s in sides]
    sides = [s + pltpu.roll(s, LANES // 4, 1) for s in sides]
    width = sides[0].shape[0] // 2
    slopes = pick(
        [side[h * width : (h + 1) * width] for h in range(2) for side in sides],
        lane_group((width, LANES), chans),
    )
    for k, ref in enumerate((own_ref, m1, m2, m3)):
        peer = mine ^ k
        kind = ref.dtype
        for r in range(rows):
            at = pl.multiple_of((r * cols + peer) * share, share)
            ref[r * share : (r + 1) * share, :] = slope_f[pl.ds(at, share), :].astype(kind)
        base = rows * share
        at = pl.multiple_of(peer * quarter, quarter)
        span = groups * quarter
        for x in range(2):
            ref[base + x * span : base + (x + 1) * span, :] = (
                both_f[:, x, pl.ds(at, quarter), :].reshape(span, LANES).astype(kind)
            )
        base += 2 * span
        ref[base : base + width, :] = slopes.astype(kind)


def update_kernel(outer_ref, final_ref, bias_ref, update_ref, update_f):
    tokens = update_ref.shape[0]
    update = dot(outer_ref[...], final_ref[...]) + bias_ref[...]
    for j in range(update_ref.shape[1]):
        update_f[:, j, :] = update[j * tokens : (j + 1) * tokens]
    update_ref[...] = update_f[...].astype(BF16)


def between_kernel(
    own_ref, r3, r2, r1, left_ref, next_ref, m3, m2, m1, total_f, right_f, *, rows, share
):
    refs = (own_ref, r1, r2, r3)
    span = left_ref.shape[0]
    first = rows * share
    last = first + 2 * span
    mine, column = lax.axis_index("rows"), lax.axis_index("cols")
    for k, ref in enumerate(refs):
        right_f[column ^ k] = ref[first + span : last, :].astype(F32)
    for start, stop in ((0, first + span), (last, total_f.shape[0])):
        total = own_ref[start:stop, :]
        for ref in refs[1:]:
            total = total + ref[start:stop, :].astype(F32)
        total_f[start:stop, :] = total
    left_ref[...] = total_f[first : first + span, :]
    slopes = total_f[last:, :]
    for k, ref in enumerate((next_ref, m1, m2, m3)):
        place = (mine ^ (mine >> 1)) + k
        place = place % rows
        peer = place ^ (place >> 1)
        at = pl.multiple_of(peer * share, share)
        ref[0:share, :] = total_f[pl.ds(at, share), :].astype(ref.dtype)
        ref[share : share + span, :] = right_f[peer].astype(ref.dtype)
        ref[share + span :, :] = slopes.astype(ref.dtype)


def to_unit(back, projector_ref, unit_ref, quarter):
    back = back[...]
    projector = projector_ref[...]
    chans = projector.shape[0]
    high = back.astype(BF16)
    low = (back - high.astype(F32)).astype(BF16)
    zero = jnp.zeros_like(projector)
    per = LANES // chans
    for b in range(per):
        weights = jnp.concatenate([projector if i == b else zero for i in range(per)], axis=0)
        got = dot(high, weights) + dot(low, weights)
        for p in range(back.shape[0] // quarter):
            unit_ref[p * per + b] = got[p * quarter : (p + 1) * quarter]


def last_kernel(
    own_ref, r3, r2, r1, unit_ref, xhat_ref, spread_ref, gain_ref, second_ref,
    final_ref, first_slope_ref, second_slope_ref, out_ref, unit_f,
):
    total = own_ref[...] + r1[...].astype(F32) + r2[...].astype(F32) + r3[...].astype(F32)
    share = final_ref.shape[0]
    final_ref[...] = total[:share]
    tokens, quarter, width = out_ref.shape
    span = tokens * quarter * second_ref.shape[0] // LANES
    to_unit(total[share : share + span], second_ref, unit_f, quarter)
    g = (unit_ref[...] + unit_f[...]).reshape(tokens * quarter, width) * gain_ref[...]
    xhat = xhat_ref[...]
    out = spread_ref[...] * (
        g
        - jnp.mean(g, axis=-1, keepdims=True)
        - xhat * jnp.mean(g * xhat, axis=-1, keepdims=True)
    )
    out_ref[...] = out.reshape(tokens, quarter, width)
    slopes = total[share + span :].T
    chans = second_ref.shape[0]
    for x, ref in enumerate((first_slope_ref, second_slope_ref)):
        ref[...] = jnp.concatenate(
            [slopes[(2 * h + x) * chans : (2 * h + x + 1) * chans] for h in range(2)], axis=1
        )


def exchange(messages, axis, order):
    size = lax.axis_size(axis)
    got = {}
    for k in order:
        if axis == "cols":
            pairs = [(p, p ^ k) for p in range(size)]
        else:
            cycle = [p ^ (p >> 1) for p in range(size)]
            pairs = [(cycle[p], cycle[(p + k) % size]) for p in range(size)]
        got[k] = lax.ppermute(messages[k], axis, pairs)
    return [got[k] for k in sorted(got)]


ROUTES = (
    ((3, 2, 0, 1), (1, 0, 2, 3)),
    ((0, 3, 2, 1), (1, 2, 0, 3)),
    ((0, 3, 1, 2), (2, 1, 0, 3)),
    ((1, 0, 3, 2), (2, 3, 0, 1)),
)


def holders(cols):
    first, second, mask = [], [], 0
    for r, (a, b) in enumerate(ROUTES):
        assert all(a.index(z) // 2 != b.index(z) // 2 for z in a)
        first += [(r * cols + q, z * cols + r) for q, z in enumerate(a)]
        second += [(r * cols + q, z * cols + r) for q, z in enumerate(b)]
        for q, z in enumerate(a):
            mask |= q // 2 << (z * cols + r)
    return first, second, mask


def local_square(*args):
    return local_square_(*args)


def local_square_(
    alignment_features,
    affine_factor,
    affine_offset,
    first_projector,
    second_projector,
    final_projector,
    additive_term,
    adjoint_update,
):
    rows, cols = lax.axis_size("rows"), lax.axis_size("cols")
    tokens, quarter, width = alignment_features.shape
    chans = first_projector.shape[1]
    total, pair_ch = final_projector.shape
    seqs = quarter * cols
    per, steps = LANES // chans, chans // (LANES // chans)
    share = total // (rows * cols)
    shape = jax.ShapeDtypeStruct
    wide, tall = tokens * LANES, steps * tokens
    groups = tokens // per
    half = tokens // 2
    aligned = shape((tokens, quarter, width), F32)
    flat = shape((tokens * quarter, width), F32)
    inputs = [
        alignment_features,
        affine_offset.reshape(1, width),
        affine_factor.reshape(1, width),
        adjoint_update,
        final_projector,
        first_projector.T,
        second_projector.T,
        additive_term.reshape(1, pair_ch),
    ]
    unit, xhat, spread, gain, cot, final, first, second, bias = call(
        norm_kernel,
        [shape((half * quarter, 2 * width), BF16), flat, flat]
        + [shape(i.shape, i.dtype) for i in inputs[2:]],
        [pltpu.VMEM(i.shape, i.dtype) for i in inputs[:2]]
        + [pltpu.SemaphoreType.DMA((len(inputs),))],
        space=pltpu.HBM,
    )(*[pltpu.with_memory_space_constraint(i, pltpu.HBM) for i in inputs])
    partner = lax.ppermute(unit, "cols", [(p, p ^ 1) for p in range(cols)])
    halves = call(
        half_kernel,
        shape((half * seqs // 2, 2 * width), BF16),
        [pltpu.VMEM((half, seqs // 2, 2 * width), F32)],
    )(unit, partner)
    from_first, from_second, first_halves = holders(cols)
    cols_a = lax.ppermute(halves, ("rows", "cols"), from_first)
    cols_b = lax.ppermute(halves, ("rows", "cols"), from_second)
    across = lax.ppermute(halves, "cols", [(p, p ^ 2) for p in range(cols)])
    grad = call(
        functools.partial(grad_kernel, chans=chans),
        (
            shape((tall, wide), BF16),
            shape((tall, wide), BF16),
            shape((tokens * tokens, pair_ch), BF16),
            shape((per, 4 * LANES, 2 * width), BF16),
            shape((tokens * chans, per * LANES), BF16),
        ),
        [pltpu.VMEM(adjoint_update.shape, F32), pltpu.VMEM((total, pair_ch), F32)],
        flops=8 * tokens * tokens * total * pair_ch,
    )
    by_col, by_row, cot_cols, weight, order = grad(cot, final, first, second)
    left, turned, part = call(
        functools.partial(left_kernel, chans=chans),
        (
            shape((tall, LANES), BF16),
            shape((2 * width, half * seqs), BF16),
            shape((groups, seqs, LANES), F32),
        ),
        [pltpu.VMEM((half, seqs, 2 * width), BF16), pltpu.VMEM((LANES, wide), F32)],
        flops=10**8,
    )(halves, across, weight, order, by_col)
    span = groups * quarter
    message = rows * share + 2 * span + width // 2
    outer, own, *messages = call(
        functools.partial(
            pair_kernel, chans=chans, sizes=(rows, cols), first_halves=first_halves
        ),
        (
            shape((tokens * tokens, total), BF16),
            shape((message, LANES), F32),
            *[shape((message, LANES), BF16)] * (cols - 1),
        ),
        [
            pltpu.VMEM((LANES, wide), BF16),
            pltpu.VMEM((total, pair_ch), F32),
            pltpu.VMEM((LANES, wide), F32),
            pltpu.VMEM((groups, 2, seqs, LANES), F32),
            pltpu.VMEM((half, seqs, 2 * width), BF16),
        ],
    )(cols_a, cols_b, left, turned, part, weight, order, by_row, cot_cols)
    got = exchange([own] + messages[::-1], "cols", (1, 2, 3))
    update = call(
        update_kernel,
        shape((tokens, tokens, pair_ch), BF16),
        [pltpu.VMEM((tokens, tokens, pair_ch), F32)],
        flops=10**8,
    )(outer, final, bias)
    message = share + span + width // 2
    back, own, *messages = call(
        functools.partial(between_kernel, rows=rows, share=share),
        (
            shape((span, LANES), F32),
            shape((message, LANES), F32),
            *[shape((message, LANES), BF16)] * (rows - 1),
        ),
        [
            pltpu.VMEM((rows * share + 2 * span + width // 2, LANES), F32),
            pltpu.VMEM((cols, span, LANES), F32),
        ],
    )(own, *got[::-1])
    got = exchange([own] + messages[::-1], "rows", (1, 2, 3))
    from_left = call(functools.partial(to_unit, quarter=quarter), aligned, flops=10**8)(back, first)
    final_slope, first_slope, second_slope, alignment_slope = call(
        last_kernel,
        (
            shape((share, pair_ch), F32),
            shape((chans, width), F32),
            shape((chans, width), F32),
            aligned,
        ),
        [pltpu.VMEM((tokens, quarter, width), F32)],
    )(own, *got[::-1], from_left, xhat, spread, gain, second)
    return update, alignment_slope, final_slope, first_slope.T, second_slope.T


def fits(mesh, alignment_features, first_projector, final_projector):
    rows, cols = mesh.shape["rows"], mesh.shape["cols"]
    tokens = alignment_features.shape[0] // (mesh.shape["groups"] * rows)
    quarter = alignment_features.shape[1] // cols
    width, chans = first_projector.shape
    per = LANES // chans
    return (
        rows == cols == len(ROUTES)
        and chans * per == LANES
        and chans % per == 0
        and chans // per == SUBLANES
        and 2 * width == LANES
        and final_projector.shape[1] == LANES
        and quarter == SUBLANES
        and tokens % (2 * SUBLANES) == 0
        and quarter * cols == chans
        and chans // per * tokens == LANES
    )


def solution(mesh):
    in_specs = (
        P(("groups", "rows"), "cols", None),
        P(),
        P(),
        P(),
        P(),
        P(),
        P(),
        P(("groups", "rows"), "cols", None),
    )
    out_specs = (
        P(("groups", "rows"), "cols", None),
        P(("groups", "rows"), "cols", None),
        P(("groups", "rows", "cols"), None),
        P("groups", None),
        P("groups", None),
    )

    def whole(*args):
        square = fits(mesh, args[0], args[3], args[5])
        step = jax.shard_map(
            local_square if square else local_general,
            mesh=mesh,
            in_specs=in_specs,
            out_specs=out_specs,
            check_vma=False,
        )
        return step(*args)

    return whole
```

```python
import functools

import jax
import jax.numpy as jnp
from jax import lax
from jax.experimental import pallas as pl
from jax.experimental.pallas import tpu as pltpu
from jax.sharding import PartitionSpec as P


def layernorm_parts(alignment_features, affine_factor, affine_offset):
    centered_alignment = alignment_features - jnp.mean(alignment_features, axis=-1, keepdims=True)
    reciprocal_spread = lax.rsqrt(
        jnp.mean(centered_alignment * centered_alignment, axis=-1, keepdims=True) + 1e-05
    )
    zscored_alignment = centered_alignment * reciprocal_spread
    return (
        zscored_alignment,
        reciprocal_spread,
        (zscored_alignment * affine_factor + affine_offset).astype(jnp.bfloat16),
    )


def local_general(
    alignment_features,
    affine_factor,
    affine_offset,
    first_projector,
    second_projector,
    final_projector,
    additive_term,
    adjoint_update,
):
    zscored_alignment, reciprocal_spread, unit_alignment = layernorm_parts(
        alignment_features, affine_factor, affine_offset
    )
    first_factor_here = jnp.dot(
        unit_alignment, first_projector, preferred_element_type=jnp.float32
    ).astype(jnp.bfloat16)
    second_factor_here = jnp.dot(
        unit_alignment, second_projector, preferred_element_type=jnp.float32
    ).astype(jnp.bfloat16)
    tokens, quarter, chans = first_factor_here.shape
    left_flat = first_factor_here.reshape(tokens, quarter * chans)
    right_flat = second_factor_here.reshape(tokens, quarter * chans)
    left_wide, right_wide = (
        lax.all_gather(left_flat, "cols", axis=1, tiled=True),
        lax.all_gather(right_flat, "cols", axis=1, tiled=True),
    )
    left_rows = left_wide.reshape(tokens, -1, chans)
    right_all = lax.all_gather(right_wide, "rows", axis=0, tiled=True)
    block = right_all.shape[0] // lax.axis_size("cols")
    right_cols = lax.dynamic_slice_in_dim(
        right_all, lax.axis_index("cols") * block, block, 0
    ).reshape(block, -1, chans)
    seqs = left_rows.shape[1]
    multiplier = 1.0 / seqs
    pair_ch = adjoint_update.shape[2]
    step_rows = 4
    rounds = tokens // step_rows
    first_tile_list = left_rows.reshape(rounds, step_rows, seqs, chans)
    cot_blocks = adjoint_update.reshape(rounds, step_rows, block, pair_ch)

    def advance(carry, inputs):
        right_acc, out_acc = carry
        left_slab, cot_slab = inputs
        outer = (
            jnp.einsum("isc,jsd->ijcd", left_slab, right_cols, preferred_element_type=jnp.float32)
            * multiplier
        ).astype(jnp.bfloat16)
        flat = outer.reshape(step_rows * block, chans * chans)
        cot_flat = cot_slab.reshape(step_rows * block, pair_ch)
        update = (
            jnp.dot(flat, final_projector, preferred_element_type=jnp.float32) + additive_term
        ).astype(jnp.bfloat16)
        outer_grad = jnp.dot(
            cot_flat, final_projector.T, preferred_element_type=jnp.float32
        ).astype(jnp.bfloat16)
        outer_grad = outer_grad.reshape(step_rows, block, chans, chans)
        left_piece = (
            jnp.einsum("ijcd,jsd->isc", outer_grad, right_cols, preferred_element_type=jnp.float32)
            * multiplier
        )
        right_acc = (
            right_acc
            + jnp.einsum("ijcd,isc->jsd", outer_grad, left_slab, preferred_element_type=jnp.float32)
            * multiplier
        )
        out_acc = out_acc + jnp.einsum(
            "fk,fe->ke", flat, cot_flat, preferred_element_type=jnp.float32
        )
        return ((right_acc, out_acc), (update.reshape(step_rows, block, pair_ch), left_piece))

    beginning_position = (
        jnp.zeros((block, seqs, chans), jnp.float32),
        jnp.zeros((chans * chans, pair_ch), jnp.float32),
    )
    (right_part, out_term), (updates, left_pieces) = lax.scan(
        advance, beginning_position, (first_tile_list, cot_blocks)
    )
    residue_update = updates.reshape(tokens, block, pair_ch)
    left_part = left_pieces.reshape(tokens, seqs * chans)
    first_adjoint = lax.psum_scatter(left_part, "cols", scatter_dimension=1, tiled=True).reshape(
        tokens, quarter, chans
    )
    moved = lax.all_to_all(
        right_part.reshape(block, seqs * chans), "cols", split_axis=1, concat_axis=0, tiled=True
    )
    right_back = lax.psum_scatter(moved, "rows", scatter_dimension=0, tiled=True).reshape(
        tokens, quarter, chans
    )
    final_projector_slope = lax.psum_scatter(
        out_term, ("rows", "cols"), scatter_dimension=0, tiled=True
    )
    unit_broadcast = unit_alignment.astype(jnp.float32)
    high = lax.Precision.HIGHEST
    left_term = jnp.einsum("tsk,tsc->kc", unit_broadcast, first_adjoint, precision=high)
    right_term = jnp.einsum("tsk,tsc->kc", unit_broadcast, right_back, precision=high)
    first_projector_slope, second_projector_slope = lax.psum(
        (left_term, right_term), ("rows", "cols")
    )
    unit_adjoint = jnp.einsum(
        "tsc,kc->tsk", first_adjoint, first_projector.astype(jnp.float32), precision=high
    )
    unit_adjoint = unit_adjoint + jnp.einsum(
        "tsc,kc->tsk", right_back, second_projector.astype(jnp.float32), precision=high
    )
    scaled_alignment = unit_adjoint * affine_factor
    alignment_slope = reciprocal_spread * (
        scaled_alignment
        - jnp.mean(scaled_alignment, axis=-1, keepdims=True)
        - zscored_alignment * jnp.mean(scaled_alignment * zscored_alignment, axis=-1, keepdims=True)
    )
    return (
        residue_update,
        alignment_slope,
        final_projector_slope,
        first_projector_slope,
        second_projector_slope,
    )


F32, BF16 = jnp.float32, jnp.bfloat16
LANES, SUBLANES = 128, 8


def dot(a, b, at=1, bt=0):
    return lax.dot_general(a, b, (((at,), (bt,)), ((), ())), preferred_element_type=F32)


def along(mine, step, size):
    place = ((mine ^ (mine >> 1)) + step + size) % size
    return place ^ (place >> 1)


def lane_group(shape, size):
    return lax.broadcasted_iota(jnp.int32, shape, len(shape) - 1) // size


def pick(parts, group):
    out = parts[-1]
    for b in range(len(parts) - 2, -1, -1):
        out = jnp.where(group == b, parts[b], out)
    return out


def normalise(x):
    centered = x - jnp.mean(x, axis=-1, keepdims=True)
    spread = lax.rsqrt(jnp.mean(centered * centered, axis=-1, keepdims=True) + 1e-05)
    return centered * spread, spread


def call(kernel, out_shape, scratch=(), flops=0, space=pltpu.VMEM):
    place = pl.BlockSpec(memory_space=space)
    on_chip = pl.BlockSpec(memory_space=pltpu.VMEM)

    def run(*args):
        return pl.pallas_call(
            kernel,
            out_shape=out_shape,
            in_specs=[place] * len(args),
            out_specs=jax.tree.map(lambda _: on_chip, out_shape),
            scratch_shapes=list(scratch),
            cost_estimate=pl.CostEstimate(flops=flops, bytes_accessed=0, transcendentals=0),
            compiler_params=pltpu.CompilerParams(vmem_limit_bytes=16 * 2**20),
        )(*args)

    return run


def norm_kernel(*refs):
    x_ref, offset_ref, sems = refs[-3:]
    count = sems.shape[0]
    sources, (out_ref, xhat_ref, spread_ref) = refs[:count], refs[count : count + 3]
    kept = (x_ref, offset_ref) + refs[count + 3 : -3]
    copies = [
        pltpu.make_async_copy(source, ref, sems.at[n])
        for n, (source, ref) in enumerate(zip(sources, kept))
    ]
    for copy in copies:
        copy.start()
    for copy in copies[:3]:
        copy.wait()
    tokens, quarter, width = x_ref.shape
    xhat, spread = normalise(x_ref[...].reshape(tokens * quarter, width))
    xhat_ref[...] = xhat
    spread_ref[...] = jnp.broadcast_to(spread, xhat.shape)
    unit = xhat * kept[2][...] + offset_ref[...]
    half = tokens * quarter // 2
    out_ref[...] = jnp.concatenate([unit[:half], unit[half:]], axis=1).astype(BF16)
    for copy in copies[3:]:
        copy.wait()


def grad_kernel(
    cot_ref, final_ref, first_ref, second_ref,
    by_col_ref, by_row_ref, cot_cols_ref, weight_ref, order_ref,
    cot_f, final_f,
    *, chans,
):
    tokens, block, _ = cot_ref.shape
    steps = by_col_ref.shape[0] // tokens
    per = LANES // chans
    cot = cot_ref[...]
    final = final_ref[...]
    cot_f[...] = cot.astype(F32)
    final_f[...] = final.astype(F32)
    for j in range(block):
        cot_cols_ref[j * tokens : (j + 1) * tokens, :] = cot_f[:, j, :].astype(BF16)
    cot_cols = cot_cols_ref[...]
    cot_rows = cot.reshape(tokens * block, cot.shape[2])
    for a in range(steps):
        got = dot(cot_cols, final[a * LANES : (a + 1) * LANES], 1, 1).astype(BF16)
        for j in range(block):
            by_col_ref[a * tokens : (a + 1) * tokens, j * LANES : (j + 1) * LANES] = got[
                j * tokens : (j + 1) * tokens
            ]
        lanes_dc = jnp.concatenate(
            [final_f[pl.ds(a * per + b, chans, stride=chans), :] for b in range(per)], axis=0
        ).astype(BF16)
        got = dot(cot_rows, lanes_dc, 1, 1).astype(BF16)
        for i in range(tokens):
            by_row_ref[a * block : (a + 1) * block, i * LANES : (i + 1) * LANES] = got[
                i * block : (i + 1) * block
            ]
    for x, ref in enumerate((first_ref, second_ref)):
        projector = ref[...]
        zero = jnp.zeros_like(projector)
        halves = [
            jnp.concatenate([projector, zero], axis=1),
            jnp.concatenate([zero, projector], axis=1),
        ]
        empty = jnp.concatenate([zero, zero], axis=1)
        for b in range(per):
            for h in range(2):
                for other in range(per):
                    at = (((x * 2) + h) * per + other) * chans
                    weight_ref[b, at : at + chans, :] = halves[h] if other == b else empty
    size = tokens * chans
    for b in range(per):
        row = lax.broadcasted_iota(jnp.int32, (size, LANES), 0)
        lane = lax.broadcasted_iota(jnp.int32, (size, LANES), 1)
        wanted = lane % tokens * chans + lane // tokens * per + b
        order_ref[:, b * LANES : (b + 1) * LANES] = jnp.where(row == wanted, 1.0, 0.0).astype(BF16)


def half_kernel(own_ref, other_ref, out_ref, unit_f):
    low = lax.axis_index("cols") % 2
    half, seqs, lanes = unit_f.shape
    quarter = seqs // 2
    for k, ref in enumerate((own_ref, other_ref)):
        at = pl.multiple_of((low ^ k) * quarter, quarter)
        unit_f[:, pl.ds(at, quarter), :] = ref[...].astype(F32).reshape(half, quarter, lanes)
    out_ref[...] = unit_f[...].reshape(half * seqs, lanes).astype(BF16)


def join(first_half, refs, unit_ref):
    half, seqs, lanes = unit_ref.shape
    for k, ref in enumerate(refs):
        at = pl.multiple_of((first_half ^ k) * (seqs // 2), seqs // 2)
        unit_ref[:, pl.ds(at, seqs // 2), :] = ref[...].reshape(half, seqs // 2, lanes)
    return unit_ref[...].reshape(half * seqs, lanes)


def project(unit, weight_ref, x, seqs, per):
    half = unit.shape[0] // seqs
    by_group = unit.reshape(half // per, per, seqs, unit.shape[1])
    size = weight_ref.shape[1] // 2
    wide = jnp.concatenate(
        [by_group[:, b].reshape(half // per * seqs, unit.shape[1]) for b in range(per)], axis=1
    )
    weights = jnp.concatenate(
        [weight_ref[b, x * size : (x + 1) * size, :] for b in range(per)], axis=1
    )
    total = dot(wide, weights, 1, 1).astype(BF16)
    count = half // per
    return [
        total[p % count * seqs : (p % count + 1) * seqs, p // count * LANES : (p // count + 1) * LANES]
        for p in range(2 * count)
    ]


def reorder(tiles, order_ref):
    wide = dot(jnp.concatenate(tiles, axis=1), order_ref[...])
    count = wide.shape[1] // LANES
    return jnp.concatenate([wide[:, b * LANES : (b + 1) * LANES] for b in range(count)], axis=0)


def fold(spread_ref, seqs, chans, tokens):
    per = LANES // chans
    group = lane_group((seqs, LANES), chans)
    out = []
    for p in range(tokens // per):
        total = None
        for shift in range(per):
            parts = []
            for b in range(per):
                t = p * per + (b + shift) % per
                parts.append(spread_ref[b * seqs : (b + 1) * seqs, t * LANES : (t + 1) * LANES])
            part = pick(parts, group)
            if shift:
                part = pltpu.roll(part, shift * chans, 1)
            total = part if total is None else total + part
        out.append(total)
    return out


def slope(unit_turned, tiles, per, chans):
    seqs = tiles[0].shape[0]
    count = len(tiles) // 2
    group = lane_group((seqs, LANES), chans)
    rows = []
    for p in range(count):
        for b in range(per):
            rows.append(
                jnp.concatenate(
                    [jnp.where(group == b, tiles[h * count + p], 0.0) for h in range(2)], axis=1
                )
            )
    got = dot(unit_turned, jnp.concatenate(rows, axis=0).astype(BF16))
    width = unit_turned.shape[0] // 2
    return got[:width, :LANES] + got[width:, LANES:]


def left_kernel(
    u0, u1, weight_ref, order_ref, by_col_ref, left_ref, turned_ref, part_ref, unit_ref, spread_f,
    *, chans,
):
    per = LANES // chans
    half, seqs, _ = unit_ref.shape
    tokens = 2 * half
    unit = join(lax.axis_index("cols") // 2, (u0, u1), unit_ref)
    turned_ref[...] = unit.astype(F32).T.astype(BF16)
    turned = reorder(project(unit, weight_ref, 0, seqs, per), order_ref)
    left_ref[...] = turned.T.astype(BF16)
    spread_f[...] = dot(turned.astype(BF16), by_col_ref[...])
    for p, tile in enumerate(fold(spread_f, seqs, chans, tokens)):
        part_ref[p] = tile * (1.0 / seqs)


def pair_kernel(
    u0, u1, left_ref, turned_ref, part_ref, weight_ref, order_ref, by_row_ref, cot_cols_ref,
    outer_ref, own_ref, m3, m2, m1,
    block_ref, slope_f, spread_f, both_f, unit_ref,
    *, chans, sizes, first_halves,
):
    per, steps = LANES // chans, chans // (LANES // chans)
    rows, cols = sizes
    half, seqs, _ = unit_ref.shape
    tokens = 2 * half
    groups = tokens // per
    quarter = seqs // cols
    share = slope_f.shape[0] // (rows * cols)
    mine = lax.axis_index("cols")
    group = lane_group((seqs, LANES), chans)
    place = lax.axis_index("rows") * cols + mine
    unit = join((first_halves >> place) & 1, (u0, u1), unit_ref)
    right = project(unit, weight_ref, 1, seqs, per)
    spread_f[...] = dot(reorder(right, order_ref).astype(BF16), by_row_ref[...])
    for p, tile in enumerate(right):
        tile = tile.astype(F32)
        rolled = [pltpu.roll(tile, s * chans, 1) if s else tile for s in range(per)]
        for own in range(per):
            j = p * per + own
            for b in range(per):
                block_ref[b * seqs : (b + 1) * seqs, j * LANES : (j + 1) * LANES] = jnp.where(
                    group == b, rolled[(b - own) % per], 0.0
                ).astype(BF16)
    left = left_ref[...]
    for p in range(groups):
        span = per * LANES
        got = dot(left, block_ref[:, p * span : (p + 1) * span])
        got = (got * (1.0 / seqs)).astype(BF16)
        for own in range(per):
            j = p * per + own
            for a in range(steps):
                outer_ref[j * tokens : (j + 1) * tokens, a * LANES : (a + 1) * LANES] = got[
                    a * tokens : (a + 1) * tokens, own * LANES : (own + 1) * LANES
                ]
    lefts = [tile * (1.0 / seqs) for tile in fold(spread_f, seqs, chans, tokens)]
    rights = [part_ref[p] for p in range(groups)]
    for p in range(groups):
        both_f[p, 0] = lefts[p]
        both_f[p, 1] = rights[p]
    sides = [
        slope(turned_ref[...], lefts, per, chans),
        slope(unit.astype(F32).T.astype(BF16), rights, per, chans),
    ]
    sides = [s + pltpu.roll(s, LANES // 2, 1) for s in sides]
    sides = [s + pltpu.roll(s, LANES // 4, 1) for s in sides]
    width = sides[0].shape[0] // 2
    slopes = pick(
        [side[h * width : (h + 1) * width] for h in range(2) for side in sides],
        lane_group((width, LANES), chans),
    )
    slope_f[...] = dot(outer_ref[...], cot_cols_ref[...], 0, 0).astype(BF16)
    for k, ref in enumerate((own_ref, m1, m2, m3)):
        peer = along(mine, k, cols)
        kind = ref.dtype
        for r in range(rows):
            at = pl.multiple_of((r * cols + peer) * share, share)
            ref[r * share : (r + 1) * share, :] = slope_f[pl.ds(at, share), :].astype(kind)
        base = rows * share
        at = pl.multiple_of(peer * quarter, quarter)
        span = groups * quarter
        for x in range(2):
            ref[base + x * span : base + (x + 1) * span, :] = (
                both_f[:, x, pl.ds(at, quarter), :].reshape(span, LANES).astype(kind)
            )
        base += 2 * span
        ref[base : base + width, :] = slopes.astype(kind)


def update_kernel(outer_ref, final_ref, bias_ref, update_ref, update_f):
    tokens = update_ref.shape[0]
    update = dot(outer_ref[...], final_ref[...]) + bias_ref[...]
    for j in range(update_ref.shape[1]):
        update_f[:, j, :] = update[j * tokens : (j + 1) * tokens]
    update_ref[...] = update_f[...].astype(BF16)


def between_kernel(
    own_ref, r3, r2, r1, left_ref, next_ref, m3, m2, m1, total_f, right_f, *, rows, share
):
    refs = (own_ref, r1, r2, r3)
    span = left_ref.shape[0]
    first = rows * share
    last = first + 2 * span
    mine, column = lax.axis_index("rows"), lax.axis_index("cols")
    for k, ref in enumerate(refs):
        right_f[along(column, -k, right_f.shape[0])] = ref[first + span : last, :].astype(F32)
    for start, stop in ((0, first + span), (last, total_f.shape[0])):
        total = own_ref[start:stop, :]
        for ref in refs[1:]:
            total = total + ref[start:stop, :].astype(F32)
        total_f[start:stop, :] = total
    left_ref[...] = total_f[first : first + span, :]
    slopes = total_f[last:, :]
    for k, ref in enumerate((next_ref, m1, m2, m3)):
        peer = along(mine, k, rows)
        at = pl.multiple_of(peer * share, share)
        ref[0:share, :] = total_f[pl.ds(at, share), :].astype(ref.dtype)
        ref[share : share + span, :] = right_f[peer].astype(ref.dtype)
        ref[share + span :, :] = slopes.astype(ref.dtype)


def to_unit(back, projector_ref, unit_ref, quarter):
    back = back[...]
    projector = projector_ref[...]
    chans = projector.shape[0]
    high = back.astype(BF16)
    low = (back - high.astype(F32)).astype(BF16)
    zero = jnp.zeros_like(projector)
    per = LANES // chans
    for b in range(per):
        weights = jnp.concatenate([projector if i == b else zero for i in range(per)], axis=0)
        got = dot(high, weights) + dot(low, weights)
        for p in range(back.shape[0] // quarter):
            unit_ref[p * per + b] = got[p * quarter : (p + 1) * quarter]


def last_kernel(
    own_ref, r3, r2, r1, unit_ref, xhat_ref, spread_ref, gain_ref, second_ref,
    final_ref, first_slope_ref, second_slope_ref, out_ref, unit_f,
):
    total = own_ref[...] + r1[...].astype(F32) + r2[...].astype(F32) + r3[...].astype(F32)
    share = final_ref.shape[0]
    final_ref[...] = total[:share]
    tokens, quarter, width = out_ref.shape
    span = tokens * quarter * second_ref.shape[0] // LANES
    to_unit(total[share : share + span], second_ref, unit_f, quarter)
    g = (unit_ref[...] + unit_f[...]).reshape(tokens * quarter, width) * gain_ref[...]
    xhat = xhat_ref[...]
    out = spread_ref[...] * (
        g
        - jnp.mean(g, axis=-1, keepdims=True)
        - xhat * jnp.mean(g * xhat, axis=-1, keepdims=True)
    )
    out_ref[...] = out.reshape(tokens, quarter, width)
    slopes = total[share + span :].T
    chans = second_ref.shape[0]
    for x, ref in enumerate((first_slope_ref, second_slope_ref)):
        ref[...] = jnp.concatenate(
            [slopes[(2 * h + x) * chans : (2 * h + x + 1) * chans] for h in range(2)], axis=1
        )


def exchange(messages, axis, order):
    size = lax.axis_size(axis)
    got = {}
    for k in order:
        got[k] = lax.ppermute(messages[k], axis, [(p, along(p, k, size)) for p in range(size)])
    return [got[k] for k in sorted(got)]


ROUTES = (
    ((3, 2, 0, 1), (1, 0, 2, 3)),
    ((0, 3, 2, 1), (1, 2, 0, 3)),
    ((0, 3, 1, 2), (2, 1, 0, 3)),
    ((1, 0, 3, 2), (2, 3, 0, 1)),
)


def holders(cols):
    first, second, mask = [], [], 0
    for r, (a, b) in enumerate(ROUTES):
        assert all(a.index(z) // 2 != b.index(z) // 2 for z in a)
        first += [(r * cols + q, z * cols + r) for q, z in enumerate(a)]
        second += [(r * cols + q, z * cols + r) for q, z in enumerate(b)]
        for q, z in enumerate(a):
            mask |= q // 2 << (z * cols + r)
    return first, second, mask


def local_square(*args):
    return local_square_(*args)


def local_square_(
    alignment_features,
    affine_factor,
    affine_offset,
    first_projector,
    second_projector,
    final_projector,
    additive_term,
    adjoint_update,
):
    rows, cols = lax.axis_size("rows"), lax.axis_size("cols")
    tokens, quarter, width = alignment_features.shape
    chans = first_projector.shape[1]
    total, pair_ch = final_projector.shape
    seqs = quarter * cols
    per, steps = LANES // chans, chans // (LANES // chans)
    share = total // (rows * cols)
    shape = jax.ShapeDtypeStruct
    wide, tall = tokens * LANES, steps * tokens
    groups = tokens // per
    half = tokens // 2
    aligned = shape((tokens, quarter, width), F32)
    flat = shape((tokens * quarter, width), F32)
    inputs = [
        alignment_features,
        affine_offset.reshape(1, width),
        affine_factor.reshape(1, width),
        adjoint_update,
        final_projector,
        first_projector.T,
        second_projector.T,
        additive_term.reshape(1, pair_ch),
    ]
    unit, xhat, spread, gain, cot, final, first, second, bias = call(
        norm_kernel,
        [shape((half * quarter, 2 * width), BF16), flat, flat]
        + [shape(i.shape, i.dtype) for i in inputs[2:]],
        [pltpu.VMEM(i.shape, i.dtype) for i in inputs[:2]]
        + [pltpu.SemaphoreType.DMA((len(inputs),))],
        space=pltpu.HBM,
    )(*[pltpu.with_memory_space_constraint(i, pltpu.HBM) for i in inputs])
    partner = lax.ppermute(unit, "cols", [(p, p ^ 1) for p in range(cols)])
    halves = call(
        half_kernel,
        shape((half * seqs // 2, 2 * width), BF16),
        [pltpu.VMEM((half, seqs // 2, 2 * width), F32)],
    )(unit, partner)
    from_first, from_second, first_halves = holders(cols)
    cols_a = lax.ppermute(halves, ("rows", "cols"), from_first)
    cols_b = lax.ppermute(halves, ("rows", "cols"), from_second)
    across = lax.ppermute(halves, "cols", [(p, p ^ 2) for p in range(cols)])
    grad = call(
        functools.partial(grad_kernel, chans=chans),
        (
            shape((tall, wide), BF16),
            shape((tall, wide), BF16),
            shape((tokens * tokens, pair_ch), BF16),
            shape((per, 4 * LANES, 2 * width), BF16),
            shape((tokens * chans, per * LANES), BF16),
        ),
        [pltpu.VMEM(adjoint_update.shape, F32), pltpu.VMEM((total, pair_ch), F32)],
        flops=8 * tokens * tokens * total * pair_ch,
    )
    by_col, by_row, cot_cols, weight, order = grad(cot, final, first, second)
    left, turned, part = call(
        functools.partial(left_kernel, chans=chans),
        (
            shape((tall, LANES), BF16),
            shape((2 * width, half * seqs), BF16),
            shape((groups, seqs, LANES), F32),
        ),
        [pltpu.VMEM((half, seqs, 2 * width), BF16), pltpu.VMEM((LANES, wide), F32)],
        flops=10**8,
    )(halves, across, weight, order, by_col)
    span = groups * quarter
    message = rows * share + 2 * span + width // 2
    outer, own, *messages = call(
        functools.partial(
            pair_kernel, chans=chans, sizes=(rows, cols), first_halves=first_halves
        ),
        (
            shape((tokens * tokens, total), BF16),
            shape((message, LANES), F32),
            *[shape((message, LANES), BF16)] * (cols - 1),
        ),
        [
            pltpu.VMEM((LANES, wide), BF16),
            pltpu.VMEM((total, pair_ch), BF16),
            pltpu.VMEM((LANES, wide), F32),
            pltpu.VMEM((groups, 2, seqs, LANES), F32),
            pltpu.VMEM((half, seqs, 2 * width), BF16),
        ],
    )(cols_a, cols_b, left, turned, part, weight, order, by_row, cot_cols)
    got = exchange([own] + messages[::-1], "cols", (1, 2, 3))
    update = call(
        update_kernel,
        shape((tokens, tokens, pair_ch), BF16),
        [pltpu.VMEM((tokens, tokens, pair_ch), F32)],
        flops=10**8,
    )(outer, final, bias)
    message = share + span + width // 2
    back, own, *messages = call(
        functools.partial(between_kernel, rows=rows, share=share),
        (
            shape((span, LANES), F32),
            shape((message, LANES), F32),
            *[shape((message, LANES), BF16)] * (rows - 1),
        ),
        [
            pltpu.VMEM((rows * share + 2 * span + width // 2, LANES), F32),
            pltpu.VMEM((cols, span, LANES), F32),
        ],
    )(own, *got[::-1])
    got = exchange([own] + messages[::-1], "rows", (1, 2, 3))
    from_left = call(functools.partial(to_unit, quarter=quarter), aligned, flops=10**8)(back, first)
    final_slope, first_slope, second_slope, alignment_slope = call(
        last_kernel,
        (
            shape((share, pair_ch), F32),
            shape((chans, width), F32),
            shape((chans, width), F32),
            aligned,
        ),
        [pltpu.VMEM((tokens, quarter, width), F32)],
    )(own, *got[::-1], from_left, xhat, spread, gain, second)
    return update, alignment_slope, final_slope, first_slope.T, second_slope.T


def fits(mesh, alignment_features, first_projector, final_projector):
    rows, cols = mesh.shape["rows"], mesh.shape["cols"]
    tokens = alignment_features.shape[0] // (mesh.shape["groups"] * rows)
    quarter = alignment_features.shape[1] // cols
    width, chans = first_projector.shape
    per = LANES // chans
    return (
        rows == cols == len(ROUTES)
        and chans * per == LANES
        and chans % per == 0
        and chans // per == SUBLANES
        and 2 * width == LANES
        and final_projector.shape[1] == LANES
        and quarter == SUBLANES
        and tokens % (2 * SUBLANES) == 0
        and quarter * cols == chans
        and chans // per * tokens == LANES
    )


def solution(mesh):
    in_specs = (
        P(("groups", "rows"), "cols", None),
        P(),
        P(),
        P(),
        P(),
        P(),
        P(),
        P(("groups", "rows"), "cols", None),
    )
    out_specs = (
        P(("groups", "rows"), "cols", None),
        P(("groups", "rows"), "cols", None),
        P(("groups", "rows", "cols"), None),
        P("groups", None),
        P("groups", None),
    )

    def whole(*args):
        square = fits(mesh, args[0], args[3], args[5])
        step = jax.shard_map(
            local_square if square else local_general,
            mesh=mesh,
            in_specs=in_specs,
            out_specs=out_specs,
            check_vma=False,
        )
        return step(*args)

    return whole
```
